8 devices in a mesh: batch: 1 (over z), row: 2 (over y), col: 4 (over x, core).
Axes of the slice: x: 2, y: 2, z: 1, core: 2. Of those that a mesh axis runs over, the one named last changes fastest.
Arguments:
- a_mat: bfloat16 [16384, 512], P(('batch', 'row'), 'col')
Outputs:
- output: bfloat16 [16384, 16384], P(('batch', 'row'), 'col')
All inputs are finite; a program needn't handle non-finite values.
Results may differ from the reference program's by a relative error of at most 0.001.
Values are sent between devices in bfloat16 or wider.
A program may use at most 1 GiB of HBM per device.

```python
import jax
import jax.numpy as jnp
from jax import lax

N = 16384
BLOCK = 256
M_COLS = 512
ROW_GROUPS = 2
COL_GROUPS = 4


def setup_inputs(seed: int = 0, part: int = 0) -> dict:
    base_key = jax.random.fold_in(jax.random.key(seed), part)
    values = jax.random.normal(base_key, (N, M_COLS), jnp.float32) * (M_COLS ** -0.25)
    return {"a_mat": values.astype(jnp.bfloat16)}


def global_index(size, groups):
    stored = jnp.arange(size)
    per_group = size // groups
    group_id = stored // per_group
    within = stored % per_group
    return ((within // BLOCK) * groups + group_id) * BLOCK + within % BLOCK


def reference(a_mat):
    blocks = N // BLOCK
    natural = a_mat.reshape(ROW_GROUPS, blocks // ROW_GROUPS, BLOCK, M_COLS).transpose(1, 0, 2, 3)
    col_order = natural.reshape(blocks // COL_GROUPS, COL_GROUPS, BLOCK, M_COLS).transpose(1, 0, 2, 3).reshape(N, M_COLS)
    col_trans = col_order.T
    row_index = global_index(N, ROW_GROUPS).reshape(blocks, BLOCK)
    col_index = global_index(N, COL_GROUPS)

    def one_block(block_item):
        row_blk, idx_blk = block_item
        product = jnp.dot(row_blk, col_trans, preferred_element_type=jnp.float32)
        return jnp.where(idx_blk[:, None] >= col_index[None, :], product, 0.0).astype(jnp.bfloat16)

    result = lax.map(one_block, (a_mat.reshape(blocks, BLOCK, M_COLS), row_index))
    return result.reshape(N, N)
```

```python
import functools
import jax
import jax.numpy as jnp
from jax import lax
from jax.experimental import pallas as pl
from jax.experimental.pallas import tpu as pltpu
from jax.sharding import PartitionSpec as P

BLOCK = 256
K_DIM = 512
PIECE = 128
NM = 16
CH = 4
NC = NM // CH
NBUF = 3
AXES = ('row', 'col')


def flat(y, x, k):
    return y * 4 + x * 2 + k


ALL = [(y, x, k) for y in range(2) for x in range(2) for k in range(2)]
PERM_PARTNER = [(flat(y, x, k), flat(y, x, 1 - k)) for y, x, k in ALL]
PERM_X = [(flat(y, x, k), flat(y, 1 - x, k)) for y, x, k in ALL]
PERM_YA = [(flat(y, x, y), flat(1 - y, x, y)) for y in range(2) for x in range(2)]
PERM_YB = [(flat(y, x, 1 - y), flat(1 - y, x, y)) for y in range(2) for x in range(2)]


def positions():
    y = lax.axis_index('row')
    col = lax.axis_index('col')
    return y, col // 2, col % 2, col


def zero_kernel(c_ref, zbuf, sem):
    zbuf[...] = jnp.zeros_like(zbuf)
    copies = []
    for i in range(NC):
        for j in range(i + 1, NC):
            cp = pltpu.make_async_copy(zbuf, c_ref.at[pl.ds(CH * i, CH), :, :, pl.ds(j * CH * BLOCK, CH * BLOCK)], sem)
            cp.start()
            copies.append(cp)
    for cp in copies:
        cp.wait()


def lookup(job, values):
    out = jnp.int32(values[-1]) if values else jnp.int32(0)
    for n in range(len(values) - 2, -1, -1):
        out = jnp.where(job == n, jnp.int32(values[n]), out)
    return out


def stage_kernel(jobs_m, jobs_u, n_in, srcs, *refs):
    ins = refs[:n_in]
    c_ref = refs[n_in + 1]
    panels, obuf, lsem, osem, seen = refs[n_in + 2:]
    y, x, k, col = positions()
    matched = k == y
    cp = jnp.where(matched, 0, 2)

    def load(panel, chunk, start):
        for p in range(4):
            ref, kind = ins[srcs[(panel, chunk, p)][0]], srcs[(panel, chunk, p)][1]
            if kind == 'local':
                s = x if panel == 0 else 1 - x
                src = ref.at[pl.ds(CH * chunk, CH), s]
            elif kind == 'full':
                src = ref.at[pl.ds(CH * chunk, CH)]
            else:
                src = ref
            pltpu.make_async_copy(src, panels.at[panel, pl.ds(CH * chunk, CH), :, pl.ds(p * PIECE, PIECE)], lsem.at[panel * NC + chunk]).start()

    def need(jobs, is_matched):
        order = []
        for rp, i, j in jobs:
            for item in ((rp, i), (0 if is_matched else 2, j)):
                if item not in order:
                    order.append(item)
        return order

    for n in range(3 * NC):
        seen[n] = 0

    @pl.when(matched)
    def _():
        for panel, chunk in need(jobs_m, True):
            load(panel, chunk, True)

    @pl.when(jnp.logical_not(matched))
    def _():
        for panel, chunk in need(jobs_u, False):
            load(panel, chunk, True)

    n_jobs = jnp.where(matched, len(jobs_m), len(jobs_u))

    def ensure(panel, chunk):
        idx = panel * NC + chunk

        @pl.when(seen[idx] == 0)
        def _():
            ref = panels.at[panel, pl.ds(CH * chunk, CH)]
            pltpu.make_async_copy(ref, ref, lsem.at[idx]).wait()
            seen[idx] = 1

    def out_copy(b, rp, i, j):
        s = jnp.where(rp == 0, x, 1 - x)
        return pltpu.make_async_copy(obuf.at[b], c_ref.at[pl.ds(CH * i, CH), s, :, pl.ds(pl.multiple_of(j * CH * BLOCK, CH * BLOCK), CH * BLOCK)], osem.at[b])

    def body(job, _):
        def pick(f):
            vm = lookup(job, [f(v) for v in jobs_m])
            vu = lookup(job, [f(v) for v in jobs_u])
            return jnp.where(matched, vm, vu)
        rp = pick(lambda v: v[0])
        i = pick(lambda v: v[1])
        j = pick(lambda v: v[2])
        b = lax.rem(job, NBUF)
        ensure(rp, i)
        ensure(cp, j)

        @pl.when(job >= NBUF)
        def _():
            out_copy(b, rp, i, j).wait()

        @pl.when(i != j)
        def _():
            rows = panels[rp, pl.ds(CH * i, CH)].reshape(CH * BLOCK, K_DIM)
            cols = panels[cp, pl.ds(CH * j, CH)].reshape(CH * BLOCK, K_DIM)
            prod = lax.dot_general(rows, cols, (((1,), (1,)), ((), ())), preferred_element_type=jnp.float32)
            obuf[b] = prod.astype(jnp.bfloat16).reshape(CH, BLOCK, CH * BLOCK)

        @pl.when(i == j)
        def _():
            s = jnp.where(rp == 0, x, 1 - x)
            for q in range(CH):
                rows = panels[rp, pl.ds(CH * i + q, CH - q)].reshape((CH - q) * BLOCK, K_DIM)
                cols = panels[cp, CH * j + q]
                prod = lax.dot_general(rows, cols, (((1,), (1,)), ((), ())), preferred_element_type=jnp.float32)
                row_id = lax.broadcasted_iota(jnp.int32, (BLOCK, BLOCK), 0) + (2 * s + y) * BLOCK
                col_id = lax.broadcasted_iota(jnp.int32, (BLOCK, BLOCK), 1) + col * BLOCK
                head = jnp.where(row_id >= col_id, prod[:BLOCK], 0.0)
                obuf[b, q, :, q * BLOCK:(q + 1) * BLOCK] = head.astype(jnp.bfloat16)
                if q + 1 < CH:
                    obuf[b, q + 1:, :, q * BLOCK:(q + 1) * BLOCK] = prod[BLOCK:].astype(jnp.bfloat16).reshape(CH - q - 1, BLOCK, BLOCK)
                if q:
                    obuf[b, :q, :, q * BLOCK:(q + 1) * BLOCK] = jnp.zeros((q, BLOCK, BLOCK), jnp.bfloat16)
        out_copy(b, rp, i, j).start()
        return 0

    lax.fori_loop(0, n_jobs, body, 0)
    for b in range(NBUF):
        @pl.when(n_jobs > b)
        def _():
            out_copy(b, 0, 0, 0).wait()


def run_stage(c, jobs_m, jobs_u, arrays, srcs):
    any_spec = pl.BlockSpec(memory_space=pl.ANY)
    tiles = max(sum(10 if i == j else 16 for _, i, j in jobs) for jobs in (jobs_m, jobs_u))
    flops = tiles * 2 * BLOCK * BLOCK * K_DIM
    return pl.pallas_call(
        functools.partial(stage_kernel, jobs_m, jobs_u, len(arrays), srcs),
        out_shape=jax.ShapeDtypeStruct(c.shape, c.dtype),
        in_specs=[any_spec] * (len(arrays) + 1),
        out_specs=any_spec,
        input_output_aliases={len(arrays): 0},
        scratch_shapes=[
            pltpu.VMEM((3, NM, BLOCK, K_DIM), jnp.bfloat16),
            pltpu.VMEM((NBUF, CH, BLOCK, CH * BLOCK), jnp.bfloat16),
            pltpu.SemaphoreType.DMA((3 * NC,)),
            pltpu.SemaphoreType.DMA((NBUF,)),
            pltpu.SMEM((3 * NC,), jnp.int32),
        ],
        compiler_params=pltpu.CompilerParams(vmem_limit_bytes=48 * 1024 * 1024),
        cost_estimate=pl.CostEstimate(flops=flops, bytes_accessed=tiles * BLOCK * BLOCK * 2, transcendentals=0),
    )(*arrays, c)


def solution(mesh):
    def local_fn(a):
        y, x, k, col = positions()
        a4 = a.reshape(NM, 2, BLOCK, PIECE)
        same = lax.dynamic_index_in_dim(a4, x, 1, keepdims=False)
        other = lax.dynamic_index_in_dim(a4, 1 - x, 1, keepdims=False)
        part = lax.ppermute(a, AXES, PERM_PARTNER).reshape(NM, 2, BLOCK, PIECE)
        xa = lax.ppermute(other, AXES, PERM_X)
        y0a = lax.ppermute(same, AXES, PERM_YA)
        y0b = lax.ppermute(same, AXES, PERM_YB)
        xb = [None] * NC
        for u in range(NC):
            i = NC - 1 - u
            xb[i] = lax.ppermute(same[CH * i:CH * (i + 1)], AXES, PERM_X)
        xap = lax.ppermute(xa, AXES, PERM_PARTNER)
        y2a, y2b, xbp = [None] * NC, [None] * NC, [None] * NC
        for u in range(NC):
            y2a[u] = lax.ppermute(xa[CH * u:CH * (u + 1)], AXES, PERM_YA)
            y2b[u] = lax.ppermute(xa[CH * u:CH * (u + 1)], AXES, PERM_YB)
            i = NC - 1 - u
            xbp[i] = lax.ppermute(xb[i], AXES, PERM_PARTNER)

        any_spec = pl.BlockSpec(memory_space=pl.ANY)
        c = pl.pallas_call(
            zero_kernel,
            out_shape=jax.ShapeDtypeStruct((NM, 2, BLOCK, NM * BLOCK), jnp.bfloat16),
            out_specs=any_spec,
            scratch_shapes=[pltpu.VMEM((CH, 2, BLOCK, CH * BLOCK), jnp.bfloat16), pltpu.SemaphoreType.DMA],
            cost_estimate=pl.CostEstimate(flops=9_000_000_000, bytes_accessed=24 << 20, transcendentals=0),
        )()

        def sources(arrays):
            srcs = {}
            names = {id(v): n for n, v in enumerate(arrays)}

            def put(key, arr, kind):
                if id(arr) in names:
                    srcs[key] = (names[id(arr)], kind)
            for ch in range(NC):
                for panel in (0, 1):
                    put((panel, ch, 0), a4, 'local')
                    put((panel, ch, 1), part, 'local')
                put((0, ch, 2), xa, 'full')
                put((0, ch, 3), xap, 'full')
                put((1, ch, 2), xb[ch], 'chunk')
                put((1, ch, 3), xbp[ch], 'chunk')
                put((2, ch, 0), y0a, 'full')
                put((2, ch, 1), y0b, 'full')
                put((2, ch, 2), y2a[ch], 'chunk')
                put((2, ch, 3), y2b[ch], 'chunk')
            return srcs

        base = [a4, part, xa, xap]
        jobs0 = [(0, i, j) for i in range(NC) for j in range(i + 1)]
        c = run_stage(c, jobs0, [], base, sources(base))
        for u in range(NC):
            i_new = NC - 1 - u
            jobs_m = [(1, i_new, j) for j in range(i_new + 1)]
            jobs_u = [(0, i, u) for i in range(u, NC)]
            for i in range(i_new, NC):
                js = range(min(u, i) + 1) if i == i_new else ([u] if u <= i else [])
                jobs_u += [(1, i, j) for j in js]
            arrays = base + [y0a, y0b] + xb[i_new:] + xbp[i_new:] + y2a[:u + 1] + y2b[:u + 1]
            c = run_stage(c, jobs_m, jobs_u, arrays, sources(arrays))
        return c.reshape(2 * NM * BLOCK, NM * BLOCK)

    spec = P(('batch', 'row'), 'col')
    return jax.shard_map(local_fn, mesh=mesh, in_specs=(spec,), out_specs=spec, check_vma=False)
```

```python
import functools
import jax
import jax.numpy as jnp
from jax import lax
from jax.experimental import pallas as pl
from jax.experimental.pallas import tpu as pltpu
from jax.sharding import PartitionSpec as P

BLOCK = 256
K_DIM = 512
PIECE = 128
PIECES = K_DIM // PIECE
NM = 16
CH = 4
NC = NM // CH
NBUF = 3
TILE = CH * BLOCK
JOBS = [(i, j) for j in range(NC) for i in range(j, NC)]


def positions():
    y = lax.axis_index('row')
    col = lax.axis_index('col')
    return y, col // 2, col % 2, col


def chunk(c):
    return pl.ds(c * CH, CH)


def panel(ref, lead, first, count):
    parts = [ref[(*lead, p, pl.ds(first, count))].reshape(count * BLOCK, PIECE) for p in range(PIECES)]
    return jnp.concatenate(parts, axis=1)


def dot_t(rows, cols):
    return lax.dot_general(rows, cols, (((1,), (1,)), ((), ())), preferred_element_type=jnp.float32)


def full_tile(out, row_ref, row_lead, i, col_ref, col_lead, j):
    prod = dot_t(panel(row_ref, row_lead, i * CH, CH), panel(col_ref, col_lead, j * CH, CH))
    out[...] = prod.astype(jnp.bfloat16).reshape(CH, BLOCK, TILE)


def diag_tile(out, row_ref, row_lead, col_ref, col_lead, j, row_blk, col_blk):
    for q in range(CH):
        prod = dot_t(panel(row_ref, row_lead, j * CH + q, CH - q), panel(col_ref, col_lead, j * CH + q, 1))
        row_id = lax.broadcasted_iota(jnp.int32, (BLOCK, BLOCK), 0) + row_blk * BLOCK
        col_id = lax.broadcasted_iota(jnp.int32, (BLOCK, BLOCK), 1) + col_blk * BLOCK
        lanes = slice(q * BLOCK, (q + 1) * BLOCK)
        out[q, :, lanes] = jnp.where(row_id >= col_id, prod[:BLOCK], 0.0).astype(jnp.bfloat16)
        if q + 1 < CH:
            out[q + 1:, :, lanes] = prod[BLOCK:].astype(jnp.bfloat16).reshape(CH - q - 1, BLOCK, BLOCK)
        if q:
            out[:q, :, lanes] = jnp.zeros((q, BLOCK, BLOCK), jnp.bfloat16)


def gather_kernel(a_ref, sc_ref, o_ref, t_ref, lsem, d_send, d_recv, x_send, x_recv, r_send, r_recv, y_send, y_recv):
    y, x, k, col = positions()
    other_parity = k != y
    side = jnp.where(other_parity, 1, 0)
    slot = jnp.where(k == y, 0, 1)
    partner = (0, y, 2 * x + 1 - k)
    x_peer = (0, y, 2 * (1 - x) + k)
    y_peer = (0, 1 - y, 2 * x + y)

    barrier = pltpu.get_barrier_semaphore()
    for dev in (partner, x_peer, (0, 1 - y, 2 * x), (0, 1 - y, 2 * x + 1)):
        pl.semaphore_signal(barrier, inc=1, device_id=dev, device_id_type=pl.DeviceIdType.MESH)
    pl.semaphore_wait(barrier, 4)

    def remote(src, dst, send, recv, dev):
        return pltpu.make_async_remote_copy(src, dst, send, recv, device_id=dev, device_id_type=pl.DeviceIdType.MESH)

    def x_copy(n):
        c = n % NC
        if n < NC:
            return remote(a_ref.at[chunk(c), 1 - x], sc_ref.at[0, 2, chunk(c)], x_send.at[n], x_recv.at[n], x_peer)
        return remote(a_ref.at[chunk(c), x], o_ref.at[2, chunk(c)], x_send.at[n], x_recv.at[n], x_peer)

    def relay_copy(n):
        c = n % NC
        if n < NC:
            return remote(sc_ref.at[0, 2, chunk(c)], sc_ref.at[0, 3, chunk(c)], r_send.at[n], r_recv.at[n], partner)
        return remote(o_ref.at[2, chunk(c)], o_ref.at[3, chunk(c)], r_send.at[n], r_recv.at[n], partner)

    def y0_copy(s):
        return remote(a_ref.at[:, x], sc_ref.at[1, s], y_send.at[0], y_recv.at[s, 0], y_peer)

    def y2_copy(s, c):
        return remote(sc_ref.at[0, 2, chunk(c)], sc_ref.at[1, 2 + s, chunk(c)], y_send.at[1 + c], y_recv.at[s, 1 + c], y_peer)

    d_copies = [remote(a_ref.at[:, x], sc_ref.at[0, 1], d_send.at[0], d_recv.at[0], partner),
                remote(a_ref.at[:, 1 - x], o_ref.at[1], d_send.at[1], d_recv.at[1], partner)]
    l_copies = [pltpu.make_async_copy(a_ref.at[:, x], sc_ref.at[0, 0], lsem.at[0]),
                pltpu.make_async_copy(a_ref.at[:, 1 - x], o_ref.at[0], lsem.at[1])]

    for n in range(2 * NC):
        x_copy(n).start()
    y0_copy(slot).start()
    for cp in d_copies + l_copies:
        cp.start()

    for c in range(NC):
        x_copy(c).wait_recv()
        relay_copy(c).start()
        y2_copy(slot, c).start()
    l_copies[0].wait()
    d_copies[0].wait_recv()
    for c in range(NC):
        relay_copy(c).wait_recv()

    row_blk = 2 * x + y
    for c in range(NC):
        x_copy(NC + c).wait_recv()
        relay_copy(NC + c).start()

        @pl.when(other_parity)
        def _():
            for s in range(2):
                if c == 0:
                    y0_copy(s).wait_recv()
                y2_copy(s, c).wait_recv()

        base = JOBS.index((c, c))
        diag_tile(t_ref.at[base], sc_ref, (0,), sc_ref, (side,), c, row_blk, col)

        def body(i, _):
            full_tile(t_ref.at[base + i - c], sc_ref, (0,), i, sc_ref, (side,), c)
            return 0
        if c + 1 < NC:
            lax.fori_loop(c + 1, NC, body, 0)

    l_copies[1].wait()
    d_copies[1].wait_recv()
    for c in range(NC):
        relay_copy(NC + c).wait_recv()
    for n in range(2 * NC):
        x_copy(n).wait_send()
        relay_copy(n).wait_send()
    for cp in d_copies:
        cp.wait_send()
    y0_copy(slot).wait_send()
    for c in range(NC):
        y2_copy(slot, c).wait_send()


def lookup(n, values):
    out = jnp.int32(values[-1])
    for m in range(len(values) - 2, -1, -1):
        out = jnp.where(n == m, jnp.int32(values[m]), out)
    return out


def write_kernel(sc_ref, o_ref, t_ref, c_ref, zbuf, obuf, tsem, zsem, osem):
    y, x, k, col = positions()
    side = jnp.where(k != y, 1, 0)

    def dest(i, j, s):
        return c_ref.at[pl.ds(i * CH, CH), s, :, pl.ds(pl.multiple_of(j * TILE, TILE), TILE)]

    t_copies = [pltpu.make_async_copy(t_ref.at[n], dest(i, j, x), tsem) for n, (i, j) in enumerate(JOBS)]
    for cp in t_copies:
        cp.start()
    zbuf[...] = jnp.zeros_like(zbuf)
    z_copies = [pltpu.make_async_copy(zbuf, dest(i, j, s), zsem) for i in range(NC) for j in range(i + 1, NC) for s in range(2)]
    for cp in z_copies:
        cp.start()

    def out_copy(b, i, j):
        return pltpu.make_async_copy(obuf.at[b], dest(i, j, 1 - x), osem.at[b])

    def body(n, _):
        i = lookup(n, [v[0] for v in JOBS])
        j = lookup(n, [v[1] for v in JOBS])
        b = lax.rem(n, NBUF)

        @pl.when(n >= NBUF)
        def _():
            out_copy(b, i, j).wait()

        @pl.when(i != j)
        def _():
            full_tile(obuf.at[b], o_ref, (), i, sc_ref, (side,), j)

        @pl.when(i == j)
        def _():
            diag_tile(obuf.at[b], o_ref, (), sc_ref, (side,), j, 2 * (1 - x) + y, col)
        out_copy(b, i, j).start()
        return 0

    lax.fori_loop(0, len(JOBS), body, 0)
    for b in range(NBUF):
        out_copy(b, 0, 0).wait()
    for cp in t_copies + z_copies:
        cp.wait()


def solution(mesh):
    def local_fn(a):
        a4 = pltpu.with_memory_space_constraint(a.reshape(NM, 2, BLOCK, PIECE), pltpu.HBM)
        any_spec = pl.BlockSpec(memory_space=pl.ANY)
        vmem = pl.BlockSpec(memory_space=pltpu.VMEM)
        dma = pltpu.SemaphoreType.DMA
        half_flops = 136 * 2 * BLOCK * BLOCK * K_DIM
        sc, o, t = pl.pallas_call(
            gather_kernel,
            out_shape=[pltpu.VMEM((2, PIECES, NM, BLOCK, PIECE), jnp.bfloat16),
                       pltpu.VMEM((PIECES, NM, BLOCK, PIECE), jnp.bfloat16),
                       pltpu.VMEM((len(JOBS), CH, BLOCK, TILE), jnp.bfloat16)],
            in_specs=[pl.BlockSpec(memory_space=pltpu.HBM)],
            out_specs=[vmem] * 3,
            scratch_shapes=[dma((2,)), dma((2,)), dma((2,)), dma((2 * NC,)), dma((2 * NC,)), dma((2 * NC,)), dma((2 * NC,)),
                            dma((1 + NC,)), dma((2, 1 + NC))],
            compiler_params=pltpu.CompilerParams(collective_id=0, has_side_effects=True, vmem_limit_bytes=8 * 1024 * 1024),
            cost_estimate=pl.CostEstimate(flops=half_flops, bytes_accessed=2 << 20, transcendentals=0),
        )(a4)
        c = pl.pallas_call(
            write_kernel,
            out_shape=jax.ShapeDtypeStruct((NM, 2, BLOCK, NM * BLOCK), jnp.bfloat16),
            in_specs=[vmem] * 3,
            out_specs=any_spec,
            scratch_shapes=[pltpu.VMEM((CH, BLOCK, TILE), jnp.bfloat16),
                            pltpu.VMEM((NBUF, CH, BLOCK, TILE), jnp.bfloat16),
                            dma(()), dma(()), dma((NBUF,))],
            compiler_params=pltpu.CompilerParams(vmem_limit_bytes=20 * 1024 * 1024),
            cost_estimate=pl.CostEstimate(flops=half_flops, bytes_accessed=64 << 20, transcendentals=0),
        )(sc, o, t)
        return c.reshape(2 * NM * BLOCK, NM * BLOCK)

    spec = P(('batch', 'row'), 'col')
    return jax.shard_map(local_fn, mesh=mesh, in_specs=(spec,), out_specs=spec, check_vma=False)
```

```python
import functools
import jax
import jax.numpy as jnp
from jax import lax
from jax.experimental import pallas as pl
from jax.experimental.pallas import tpu as pltpu
from jax.sharding import PartitionSpec as P

BLOCK = 256
K_DIM = 512
PIECE = 128
PIECES = K_DIM // PIECE
NM = 16
CH = 4
NC = NM // CH
NBUF = 5
LEAD = 3
TILE = CH * BLOCK
JOBS = [(i, j) for j in range(NC) for i in range(j, NC)]


def positions():
    y = lax.axis_index('row')
    col = lax.axis_index('col')
    return y, col // 2, col % 2, col


def chunk(c):
    return pl.ds(c * CH, CH)


def panel(ref, lead, first, count):
    parts = [ref[(*lead, p, pl.ds(first, count))].reshape(count * BLOCK, PIECE) for p in range(PIECES)]
    return jnp.concatenate(parts, axis=1)


def dot_t(rows, cols):
    return lax.dot_general(rows, cols, (((1,), (1,)), ((), ())), preferred_element_type=jnp.float32)


def full_tile(out, row_ref, row_lead, i, col_ref, col_lead, j):
    prod = dot_t(panel(row_ref, row_lead, i * CH, CH), panel(col_ref, col_lead, j * CH, CH))
    out[...] = prod.astype(jnp.bfloat16).reshape(CH, BLOCK, TILE)


def diag_tile(out, row_ref, row_lead, col_ref, col_lead, j, row_blk, col_blk):
    for q in range(CH):
        prod = dot_t(panel(row_ref, row_lead, j * CH + q, CH - q), panel(col_ref, col_lead, j * CH + q, 1))
        row_id = lax.broadcasted_iota(jnp.int32, (BLOCK, BLOCK), 0) + row_blk * BLOCK
        col_id = lax.broadcasted_iota(jnp.int32, (BLOCK, BLOCK), 1) + col_blk * BLOCK
        lanes = slice(q * BLOCK, (q + 1) * BLOCK)
        out[q, :, lanes] = jnp.where(row_id >= col_id, prod[:BLOCK], 0.0).astype(jnp.bfloat16)
        if q + 1 < CH:
            out[q + 1:, :, lanes] = prod[BLOCK:].astype(jnp.bfloat16).reshape(CH - q - 1, BLOCK, BLOCK)
        if q:
            out[:q, :, lanes] = jnp.zeros((q, BLOCK, BLOCK), jnp.bfloat16)


def gather_kernel(a_ref, sc_ref, o_ref, t_ref, lsem, d_send, d_recv, x_send, x_recv, r_send, r_recv, y_send, y_recv):
    y, x, k, col = positions()
    other_parity = k != y
    side = jnp.where(other_parity, 1, 0)
    slot = jnp.where(k == y, 0, 1)
    partner = (0, y, 2 * x + 1 - k)
    x_peer = (0, y, 2 * (1 - x) + k)
    y_peer = (0, 1 - y, 2 * x + y)

    barrier = pltpu.get_barrier_semaphore()
    for dev in (partner, x_peer, (0, 1 - y, 2 * x), (0, 1 - y, 2 * x + 1)):
        pl.semaphore_signal(barrier, inc=1, device_id=dev, device_id_type=pl.DeviceIdType.MESH)
    pl.semaphore_wait(barrier, 4)

    def remote(src, dst, send, recv, dev):
        return pltpu.make_async_remote_copy(src, dst, send, recv, device_id=dev, device_id_type=pl.DeviceIdType.MESH)

    def x_copy(n):
        c = n % NC
        if n < NC:
            return remote(a_ref.at[chunk(c), 1 - x], sc_ref.at[0, 2, chunk(c)], x_send.at[n], x_recv.at[n], x_peer)
        return remote(a_ref.at[chunk(c), x], o_ref.at[2, chunk(c)], x_send.at[n], x_recv.at[n], x_peer)

    def relay_copy(n):
        c = n % NC
        if n < NC:
            return remote(sc_ref.at[0, 2, chunk(c)], sc_ref.at[0, 3, chunk(c)], r_send.at[n], r_recv.at[n], partner)
        return remote(o_ref.at[2, chunk(c)], o_ref.at[3, chunk(c)], r_send.at[n], r_recv.at[n], partner)

    def y0_copy(s):
        return remote(a_ref.at[:, x], sc_ref.at[1, s], y_send.at[0], y_recv.at[s, 0], y_peer)

    def y2_copy(s, c):
        return remote(sc_ref.at[0, 2, chunk(c)], sc_ref.at[1, 2 + s, chunk(c)], y_send.at[1 + c], y_recv.at[s, 1 + c], y_peer)

    d_copies = [remote(a_ref.at[:, x], sc_ref.at[0, 1], d_send.at[0], d_recv.at[0], partner),
                remote(a_ref.at[:, 1 - x], o_ref.at[1], d_send.at[1], d_recv.at[1], partner)]
    l_copies = [pltpu.make_async_copy(a_ref.at[:, x], sc_ref.at[0, 0], lsem.at[0]),
                pltpu.make_async_copy(a_ref.at[:, 1 - x], o_ref.at[0], lsem.at[1])]

    for n in range(2 * NC):
        x_copy(n).start()
    y0_copy(slot).start()
    for cp in d_copies + l_copies:
        cp.start()

    for c in range(NC):
        x_copy(c).wait_recv()
        relay_copy(c).start()
        y2_copy(slot, c).start()
    l_copies[0].wait()
    d_copies[0].wait_recv()
    for c in range(NC):
        relay_copy(c).wait_recv()

    row_blk = 2 * x + y
    for c in range(NC):
        x_copy(NC + c).wait_recv()
        relay_copy(NC + c).start()

        @pl.when(other_parity)
        def _():
            for s in range(2):
                if c == 0:
                    y0_copy(s).wait_recv()
                y2_copy(s, c).wait_recv()

        base = JOBS.index((c, c))
        diag_tile(t_ref.at[base], sc_ref, (0,), sc_ref, (side,), c, row_blk, col)

        def body(i, _):
            full_tile(t_ref.at[base + i - c], sc_ref, (0,), i, sc_ref, (side,), c)
            return 0
        if c + 1 < NC:
            lax.fori_loop(c + 1, NC, body, 0)

    l_copies[1].wait()
    d_copies[1].wait_recv()
    for c in range(NC):
        relay_copy(NC + c).wait_recv()
    for n in range(2 * NC):
        x_copy(n).wait_send()
        relay_copy(n).wait_send()
    for cp in d_copies:
        cp.wait_send()
    y0_copy(slot).wait_send()
    for c in range(NC):
        y2_copy(slot, c).wait_send()


def lookup(n, values):
    out = jnp.int32(values[-1])
    for m in range(len(values) - 2, -1, -1):
        out = jnp.where(n == m, jnp.int32(values[m]), out)
    return out


def write_kernel(sc_ref, o_ref, t_ref, c_ref, zbuf, obuf, tsem, zsem, osem):
    y, x, k, col = positions()
    side = jnp.where(k != y, 1, 0)

    def dest(i, j, s):
        return c_ref.at[pl.ds(i * CH, CH), s, :, pl.ds(pl.multiple_of(j * TILE, TILE), TILE)]

    t_copies = [pltpu.make_async_copy(t_ref.at[n], dest(i, j, x), tsem) for n, (i, j) in enumerate(JOBS)]
    for cp in t_copies[:LEAD]:
        cp.start()
    zbuf[...] = jnp.zeros_like(zbuf)
    z_copies = [pltpu.make_async_copy(zbuf, dest(i, j, s), zsem) for i in range(NC) for j in range(i + 1, NC) for s in range(2)]

    def out_copy(b, i, j):
        return pltpu.make_async_copy(obuf.at[b], dest(i, j, 1 - x), osem.at[b])

    def body(n, _):
        i = lookup(n, [v[0] for v in JOBS])
        j = lookup(n, [v[1] for v in JOBS])
        b = lax.rem(n, NBUF)

        @pl.when(n >= NBUF)
        def _():
            out_copy(b, i, j).wait()

        @pl.when(i != j)
        def _():
            full_tile(obuf.at[b], o_ref, (), i, sc_ref, (side,), j)

        @pl.when(i == j)
        def _():
            diag_tile(obuf.at[b], o_ref, (), sc_ref, (side,), j, 2 * (1 - x) + y, col)
        out_copy(b, i, j).start()

        @pl.when(n + LEAD < len(JOBS))
        def _():
            m = jnp.minimum(n + LEAD, len(JOBS) - 1)
            ti = lookup(m, [v[0] for v in JOBS])
            tj = lookup(m, [v[1] for v in JOBS])
            pltpu.make_async_copy(t_ref.at[m], dest(ti, tj, x), tsem).start()
        return 0

    lax.fori_loop(0, len(JOBS), body, 0)
    for cp in z_copies:
        cp.start()
    for b in range(NBUF):
        out_copy(b, 0, 0).wait()
    for cp in t_copies + z_copies:
        cp.wait()


def solution(mesh):
    def local_fn(a):
        a4 = pltpu.with_memory_space_constraint(a.reshape(NM, 2, BLOCK, PIECE), pltpu.HBM)
        any_spec = pl.BlockSpec(memory_space=pl.ANY)
        vmem = pl.BlockSpec(memory_space=pltpu.VMEM)
        dma = pltpu.SemaphoreType.DMA
        half_flops = 136 * 2 * BLOCK * BLOCK * K_DIM
        sc, o, t = pl.pallas_call(
            gather_kernel,
            out_shape=[pltpu.VMEM((2, PIECES, NM, BLOCK, PIECE), jnp.bfloat16),
                       pltpu.VMEM((PIECES, NM, BLOCK, PIECE), jnp.bfloat16),
                       pltpu.VMEM((len(JOBS), CH, BLOCK, TILE), jnp.bfloat16)],
            in_specs=[pl.BlockSpec(memory_space=pltpu.HBM)],
            out_specs=[vmem] * 3,
            scratch_shapes=[dma((2,)), dma((2,)), dma((2,)), dma((2 * NC,)), dma((2 * NC,)), dma((2 * NC,)), dma((2 * NC,)),
                            dma((1 + NC,)), dma((2, 1 + NC))],
            compiler_params=pltpu.CompilerParams(collective_id=0, has_side_effects=True, vmem_limit_bytes=8 * 1024 * 1024),
            cost_estimate=pl.CostEstimate(flops=half_flops, bytes_accessed=2 << 20, transcendentals=0),
        )(a4)
        c = pl.pallas_call(
            write_kernel,
            out_shape=jax.ShapeDtypeStruct((NM, 2, BLOCK, NM * BLOCK), jnp.bfloat16),
            in_specs=[vmem] * 3,
            out_specs=any_spec,
            scratch_shapes=[pltpu.VMEM((CH, BLOCK, TILE), jnp.bfloat16),
                            pltpu.VMEM((NBUF, CH, BLOCK, TILE), jnp.bfloat16),
                            dma(()), dma(()), dma((NBUF,))],
            compiler_params=pltpu.CompilerParams(vmem_limit_bytes=20 * 1024 * 1024),
            cost_estimate=pl.CostEstimate(flops=half_flops, bytes_accessed=64 << 20, transcendentals=0),
        )(sc, o, t)
        return c.reshape(2 * NM * BLOCK, NM * BLOCK)

    spec = P(('batch', 'row'), 'col')
    return jax.shard_map(local_fn, mesh=mesh, in_specs=(spec,), out_specs=spec, check_vma=False)
```

```python
import functools
import jax
import jax.numpy as jnp
from jax import lax
from jax.experimental import pallas as pl
from jax.experimental.pallas import tpu as pltpu
from jax.sharding import PartitionSpec as P

BLOCK = 256
K_DIM = 512
PIECE = 128
PIECES = K_DIM // PIECE
NM = 16
CH = 4
NC = NM // CH
NBUF = 5
LEAD = 3
TILE = CH * BLOCK
JOBS = [(i, j) for j in range(NC) for i in range(j, NC)]


def positions():
    y = lax.axis_index('row')
    col = lax.axis_index('col')
    return y, col // 2, col % 2, col


def chunk(c):
    return pl.ds(c * CH, CH)


def panel(ref, lead, first, count):
    parts = [ref[(*lead, p, pl.ds(first, count))].reshape(count * BLOCK, PIECE) for p in range(PIECES)]
    return jnp.concatenate(parts, axis=1)


def dot_t(rows, cols):
    return lax.dot_general(rows, cols, (((1,), (1,)), ((), ())), preferred_element_type=jnp.float32)


def full_tile(out, row_ref, row_lead, i, col_ref, col_lead, j):
    prod = dot_t(panel(row_ref, row_lead, i * CH, CH), panel(col_ref, col_lead, j * CH, CH))
    out[...] = prod.astype(jnp.bfloat16).reshape(CH, BLOCK, TILE)


def diag_tile(out, row_ref, row_lead, col_ref, col_lead, j, row_blk, col_blk):
    for q in range(CH):
        prod = dot_t(panel(row_ref, row_lead, j * CH + q, CH - q), panel(col_ref, col_lead, j * CH + q, 1))
        row_id = lax.broadcasted_iota(jnp.int32, (BLOCK, BLOCK), 0) + row_blk * BLOCK
        col_id = lax.broadcasted_iota(jnp.int32, (BLOCK, BLOCK), 1) + col_blk * BLOCK
        lanes = slice(q * BLOCK, (q + 1) * BLOCK)
        out[q, :, lanes] = jnp.where(row_id >= col_id, prod[:BLOCK], 0.0).astype(jnp.bfloat16)
        if q + 1 < CH:
            out[q + 1:, :, lanes] = prod[BLOCK:].astype(jnp.bfloat16).reshape(CH - q - 1, BLOCK, BLOCK)


MESH_ID = pl.DeviceIdType.MESH


def remote(src, dst, send, recv, dev):
    return pltpu.make_async_remote_copy(src, dst, send, recv, device_id=dev, device_id_type=MESH_ID)


def signal(sem, devices):
    for dev in devices:
        pl.semaphore_signal(sem, inc=1, device_id=dev, device_id_type=MESH_ID)


def first_kernel(a_ref, sc_ref, token_ref, x_send, x_recv, y_send, y_recv):
    y, x, k, _ = positions()
    token_ref[...] = jnp.zeros_like(token_ref)

    @pl.when(k != y)
    def _():
        x_peer = (0, y, 2 * (1 - x) + k)
        y_peer = (0, 1 - y, 2 * x + y)
        barrier = pltpu.get_barrier_semaphore()
        signal(barrier, (x_peer, y_peer))
        pl.semaphore_wait(barrier, 2)
        xc = remote(a_ref.at[:, 1 - x], sc_ref.at[0, 2], x_send, x_recv, x_peer)
        yc = remote(a_ref.at[:, x], sc_ref.at[1, 1], y_send, y_recv, y_peer)
        xc.start()
        yc.start()
        xc.wait()
        yc.wait()


def zero_kernel(token_ref, c_ref, done_ref, zbuf, sem):
    zbuf[...] = jnp.zeros_like(zbuf)
    done_ref[...] = jnp.zeros_like(done_ref)
    copies = []
    for s in range(2):
        for i in range(NC):
            for j in range(i + 1, NC):
                copies.append(pltpu.make_async_copy(zbuf, c_ref.at[chunk(i), s, :, pl.ds(j * TILE, TILE)], sem))
            for q in range(1, CH):
                copies.append(pltpu.make_async_copy(
                    zbuf.at[pl.ds(0, q), :, pl.ds(0, BLOCK)],
                    c_ref.at[pl.ds(i * CH, q), s, :, pl.ds((i * CH + q) * BLOCK, BLOCK)], sem))
    for cp in copies:
        cp.start()
    for cp in copies:
        cp.wait()


def gather_kernel(a_ref, sc_in, token_ref, sc_ref, o_ref, t_ref, yb, join, lsem, d_send, d_recv, x_send, x_recv, r_send, r_recv,
                  y_send, y_recv, b_send, b_recv):
    y, x, k, col = positions()
    late = k != y
    side = jnp.where(late, 1, 0)
    partner = (0, y, 2 * x + 1 - k)
    x_peer = (0, y, 2 * (1 - x) + k)
    y_early = (0, 1 - y, 2 * x + 1 - y)
    y_late = (0, 1 - y, 2 * x + y)

    def x_copy(n):
        c = n % NC
        if n < NC:
            return remote(a_ref.at[chunk(c), 1 - x], sc_ref.at[0, 2, chunk(c)], x_send.at[n], x_recv.at[n], x_peer)
        return remote(a_ref.at[chunk(c), x], o_ref.at[2, chunk(c)], x_send.at[n], x_recv.at[n], x_peer)

    def relay_copy(n):
        c = n % NC
        if n < NC:
            return remote(sc_ref.at[0, 2, chunk(c)], sc_ref.at[0, 3, chunk(c)], r_send.at[n], r_recv.at[n], partner)
        return remote(o_ref.at[2, chunk(c)], o_ref.at[3, chunk(c)], r_send.at[n], r_recv.at[n], partner)

    def y_copy(s, c):
        return remote(sc_ref.at[0, 2, chunk(c)], sc_ref.at[1, 2 + s, chunk(c)], y_send.at[c], y_recv.at[s, c], y_late)

    yb_copy = remote(a_ref.at[:, x], yb, b_send.at[0], b_recv.at[0], y_early)
    yb_relay = remote(yb, sc_ref.at[1, 0], b_send.at[1], b_recv.at[1], partner)
    d_copies = [remote(a_ref.at[:, x], sc_ref.at[0, 1], d_send.at[0], d_recv.at[0], partner),
                remote(a_ref.at[:, 1 - x], o_ref.at[1], d_send.at[1], d_recv.at[1], partner)]
    l_copies = [pltpu.make_async_copy(a_ref.at[:, x], sc_ref.at[0, 0], lsem.at[0]),
                pltpu.make_async_copy(a_ref.at[:, 1 - x], o_ref.at[0], lsem.at[1])]
    for cp in l_copies:
        cp.start()
    barrier = pltpu.get_barrier_semaphore()

    @pl.when(jnp.logical_not(late))
    def _():
        signal(barrier, (x_peer, y_early, partner, y_late))
        pl.semaphore_wait(barrier, 2)
        for n in range(2 * NC):
            x_copy(n).start()
        yb_copy.start()
        pl.semaphore_wait(join, 2)
        d_copies[0].start()
        for c in range(NC):
            x_copy(c).wait_recv()
            y_copy(0, c).start()
            relay_copy(c).start()
        yb_copy.wait_recv()
        yb_relay.start()
        d_copies[1].start()

    @pl.when(late)
    def _():
        signal(barrier, (x_peer, y_late))
        pl.semaphore_wait(barrier, 4)
        signal(join, (partner, y_early))
        for n in range(NC, 2 * NC):
            x_copy(n).start()
        for c in range(NC):
            y_copy(1, c).start()
        for c in range(NC):
            relay_copy(c).start()
        for cp in d_copies:
            cp.start()

    l_copies[0].wait()
    d_copies[0].wait_recv()
    for c in range(NC):
        relay_copy(c).wait_recv()

    row_blk = 2 * x + y
    for c in range(NC):
        x_copy(NC + c).wait_recv()
        relay_copy(NC + c).start()

        @pl.when(late)
        def _():
            if c == 0:
                yb_relay.wait_recv()
            for s in range(2):
                y_copy(s, c).wait_recv()

        base = JOBS.index((c, c))
        diag_tile(t_ref.at[base], sc_ref, (0,), sc_ref, (side,), c, row_blk, col)

        def body(i, _):
            full_tile(t_ref.at[base + i - c], sc_ref, (0,), i, sc_ref, (side,), c)
            return 0
        if c + 1 < NC:
            lax.fori_loop(c + 1, NC, body, 0)

    l_copies[1].wait()
    d_copies[1].wait_recv()
    for c in range(NC):
        relay_copy(NC + c).wait_recv()
    for n in range(2 * NC):
        relay_copy(n).wait_send()
    for n in range(NC, 2 * NC):
        x_copy(n).wait_send()
    for cp in d_copies:
        cp.wait_send()
    for c in range(NC):
        y_copy(0, c).wait_send()

    @pl.when(jnp.logical_not(late))
    def _():
        for n in range(NC):
            x_copy(n).wait_send()
        yb_copy.wait_send()
        yb_relay.wait_send()


def lookup(n, values):
    out = jnp.int32(values[-1])
    for m in range(len(values) - 2, -1, -1):
        out = jnp.where(n == m, jnp.int32(values[m]), out)
    return out


def write_kernel(sc_ref, o_ref, t_ref, c_in, c_ref, obuf, tsem, osem):
    y, x, k, col = positions()
    side = jnp.where(k != y, 1, 0)

    def job(n):
        return lookup(n, [v[0] for v in JOBS]), lookup(n, [v[1] for v in JOBS])

    def put(src, i, j, s, sem, act):
        @pl.when(i != j)
        def _():
            act(pltpu.make_async_copy(src, c_ref.at[pl.ds(i * CH, CH), s, :, pl.ds(pl.multiple_of(j * TILE, TILE), TILE)], sem))

        @pl.when(i == j)
        def _():
            for q in range(CH):
                act(pltpu.make_async_copy(
                    src.at[pl.ds(q, CH - q), :, pl.ds(q * BLOCK, BLOCK)],
                    c_ref.at[pl.ds(i * CH + q, CH - q), s, :, pl.ds(pl.multiple_of(j * TILE + q * BLOCK, BLOCK), BLOCK)], sem))

    def put_panel(n, act):
        i, j = job(n)
        put(t_ref.at[n], i, j, x, tsem, act)

    def put_job(n, act):
        i, j = job(n)
        b = lax.rem(n, NBUF)
        put(obuf.at[b], i, j, 1 - x, osem.at[b], act)

    def start(cp):
        cp.start()

    def wait(cp):
        cp.wait()

    for n in range(LEAD):
        put_panel(jnp.int32(n), start)

    def body(n, _):
        i, j = job(n)
        b = lax.rem(n, NBUF)

        @pl.when(n >= NBUF)
        def _():
            put_job(n - NBUF, wait)

        @pl.when(i != j)
        def _():
            full_tile(obuf.at[b], o_ref, (), i, sc_ref, (side,), j)

        @pl.when(i == j)
        def _():
            diag_tile(obuf.at[b], o_ref, (), sc_ref, (side,), j, 2 * (1 - x) + y, col)
        put_job(n, start)

        @pl.when(n + LEAD < len(JOBS))
        def _():
            put_panel(jnp.minimum(n + LEAD, len(JOBS) - 1), start)
        return 0

    lax.fori_loop(0, len(JOBS), body, 0)

    def drain(n, _):
        put_panel(n, wait)

        @pl.when(n >= len(JOBS) - NBUF)
        def _():
            put_job(n, wait)
        return 0
    lax.fori_loop(0, len(JOBS), drain, 0)


def solution(mesh):
    def local_fn(a):
        a4 = pltpu.with_memory_space_constraint(a.reshape(NM, 2, BLOCK, PIECE), pltpu.HBM)
        any_spec = pl.BlockSpec(memory_space=pl.ANY)
        hbm = pl.BlockSpec(memory_space=pltpu.HBM)
        vmem = pl.BlockSpec(memory_space=pltpu.VMEM)
        dma = pltpu.SemaphoreType.DMA
        half_flops = 136 * 2 * BLOCK * BLOCK * K_DIM
        panels = pltpu.VMEM((2, PIECES, NM, BLOCK, PIECE), jnp.bfloat16)
        token = jax.ShapeDtypeStruct((8, 128), jnp.float32)
        sc, first = pl.pallas_call(
            first_kernel,
            out_shape=[panels, token],
            in_specs=[hbm],
            out_specs=[vmem, vmem],
            scratch_shapes=[dma(())] * 4,
            compiler_params=pltpu.CompilerParams(collective_id=0, has_side_effects=True, vmem_limit_bytes=2 * 1024 * 1024),
        )(a4)
        c, zeroed = pl.pallas_call(
            zero_kernel,
            out_shape=[jax.ShapeDtypeStruct((NM, 2, BLOCK, NM * BLOCK), jnp.bfloat16), token],
            in_specs=[any_spec],
            out_specs=[any_spec, vmem],
            scratch_shapes=[pltpu.VMEM((CH, BLOCK, TILE), jnp.bfloat16), dma(())],
            compiler_params=pltpu.CompilerParams(vmem_limit_bytes=4 * 1024 * 1024),
            cost_estimate=pl.CostEstimate(flops=half_flops, bytes_accessed=30 << 20, transcendentals=0),
        )(first)
        sc, o, t = pl.pallas_call(
            gather_kernel,
            out_shape=[panels,
                       pltpu.VMEM((PIECES, NM, BLOCK, PIECE), jnp.bfloat16),
                       pltpu.VMEM((len(JOBS), CH, BLOCK, TILE), jnp.bfloat16)],
            in_specs=[hbm, vmem, any_spec],
            out_specs=[vmem] * 3,
            input_output_aliases={1: 0},
            scratch_shapes=[pltpu.VMEM((NM, BLOCK, PIECE), jnp.bfloat16), pltpu.SemaphoreType.REGULAR,
                            dma((2,)), dma((2,)), dma((2,)), dma((2 * NC,)), dma((2 * NC,)), dma((2 * NC,)), dma((2 * NC,)),
                            dma((NC,)), dma((2, NC)), dma((2,)), dma((2,))],
            compiler_params=pltpu.CompilerParams(collective_id=1, has_side_effects=True, vmem_limit_bytes=8 * 1024 * 1024),
            cost_estimate=pl.CostEstimate(flops=half_flops, bytes_accessed=2 << 20, transcendentals=0),
        )(a4, sc, zeroed)
        c = pl.pallas_call(
            write_kernel,
            out_shape=jax.ShapeDtypeStruct((NM, 2, BLOCK, NM * BLOCK), jnp.bfloat16),
            in_specs=[vmem] * 3 + [any_spec],
            out_specs=any_spec,
            input_output_aliases={3: 0},
            scratch_shapes=[pltpu.VMEM((NBUF, CH, BLOCK, TILE), jnp.bfloat16), dma(()), dma((NBUF,))],
            compiler_params=pltpu.CompilerParams(vmem_limit_bytes=20 * 1024 * 1024),
            cost_estimate=pl.CostEstimate(flops=half_flops, bytes_accessed=34 << 20, transcendentals=0),
        )(sc, o, t, c)
        return c.reshape(2 * NM * BLOCK, NM * BLOCK)

    spec = P(('batch', 'row'), 'col')
    return jax.shard_map(local_fn, mesh=mesh, in_specs=(spec,), out_specs=spec, check_vma=False)
```

```python
import functools
import jax
import jax.numpy as jnp
from jax import lax
from jax.experimental import pallas as pl
from jax.experimental.pallas import tpu as pltpu
from jax.sharding import PartitionSpec as P

BLOCK = 256
K_DIM = 512
PIECE = 128
PIECES = K_DIM // PIECE
NM = 16
CH = 4
NC = NM // CH
NBUF = 5
LEAD = 4
TILE = CH * BLOCK
JOBS = [(i, j) for j in range(NC) for i in range(j, NC)]
NA = 3
NR = 2
O_ORDER = (3, 0, 1, 2)
EXTRA = [(3, 0), (3, 1)]
LATER = [job for job in JOBS if job not in EXTRA]
PANELS = [(i, j, 0) for i, j in JOBS] + [(i, j, 1) for i, j in EXTRA]


def positions():
    y = lax.axis_index('row')
    col = lax.axis_index('col')
    return y, col // 2, col % 2, col


def chunk(c):
    return pl.ds(c * CH, CH)


def panel(ref, lead, first, count):
    parts = [ref[(*lead, p, pl.ds(first, count))].reshape(count * BLOCK, PIECE) for p in range(PIECES)]
    return jnp.concatenate(parts, axis=1)


def dot_t(rows, cols):
    return lax.dot_general(rows, cols, (((1,), (1,)), ((), ())), preferred_element_type=jnp.float32)


def full_tile(out, row_ref, row_lead, i, col_ref, col_lead, j):
    prod = dot_t(panel(row_ref, row_lead, i * CH, CH), panel(col_ref, col_lead, j * CH, CH))
    out[...] = prod.astype(jnp.bfloat16).reshape(CH, BLOCK, TILE)


def diag_tile(out, row_ref, row_lead, col_ref, col_lead, j, row_blk, col_blk):
    for q in range(CH):
        prod = dot_t(panel(row_ref, row_lead, j * CH + q, CH - q), panel(col_ref, col_lead, j * CH + q, 1))
        row_id = lax.broadcasted_iota(jnp.int32, (BLOCK, BLOCK), 0) + row_blk * BLOCK
        col_id = lax.broadcasted_iota(jnp.int32, (BLOCK, BLOCK), 1) + col_blk * BLOCK
        lanes = slice(q * BLOCK, (q + 1) * BLOCK)
        out[q, :, lanes] = jnp.where(row_id >= col_id, prod[:BLOCK], 0.0).astype(jnp.bfloat16)
        if q + 1 < CH:
            out[q + 1:, :, lanes] = prod[BLOCK:].astype(jnp.bfloat16).reshape(CH - q - 1, BLOCK, BLOCK)


MESH_ID = pl.DeviceIdType.MESH


def remote(src, dst, send, recv, dev):
    return pltpu.make_async_remote_copy(src, dst, send, recv, device_id=dev, device_id_type=MESH_ID)


def signal(sem, devices):
    for dev in devices:
        pl.semaphore_signal(sem, inc=1, device_id=dev, device_id_type=MESH_ID)


def first_kernel(a_ref, sc_ref, token_ref, x_send, x_recv, y_send, y_recv):
    y, x, k, _ = positions()
    token_ref[...] = jnp.zeros_like(token_ref)

    @pl.when(k != y)
    def _():
        x_peer = (0, y, 2 * (1 - x) + k)
        y_peer = (0, 1 - y, 2 * x + y)
        barrier = pltpu.get_barrier_semaphore()
        signal(barrier, (x_peer, y_peer))
        pl.semaphore_wait(barrier, 2)
        part = pl.ds(0, NA * CH)
        xc = remote(a_ref.at[part, 1 - x], sc_ref.at[0, 2, part], x_send, x_recv, x_peer)
        yc = remote(a_ref.at[part, x], sc_ref.at[1, 1, part], y_send, y_recv, y_peer)
        xc.start()
        yc.start()
        xc.wait()
        yc.wait()


def zero_kernel(token_ref, c_ref, done_ref, zbuf, sem):
    zbuf[...] = jnp.zeros_like(zbuf)
    done_ref[...] = jnp.zeros_like(done_ref)
    copies = []
    for s in range(2):
        for i in range(NC):
            for j in range(i + 1, NC):
                copies.append(pltpu.make_async_copy(zbuf, c_ref.at[chunk(i), s, :, pl.ds(j * TILE, TILE)], sem))
            for q in range(1, CH):
                copies.append(pltpu.make_async_copy(
                    zbuf.at[pl.ds(0, q), :, pl.ds(0, BLOCK)],
                    c_ref.at[pl.ds(i * CH, q), s, :, pl.ds((i * CH + q) * BLOCK, BLOCK)], sem))
    for cp in copies:
        cp.start()
    for cp in copies:
        cp.wait()


def gather_kernel(a_ref, sc_in, token_ref, sc_ref, o_ref, t_ref, yb, yr, join, lsem, d_send, d_recv, x_send, x_recv, r_send, r_recv,
                  y_send, y_recv, b_send, b_recv, q_send, q_recv, u_send, u_recv):
    y, x, k, col = positions()
    late = k != y
    early = k == y
    side = jnp.where(late, 1, 0)
    partner = (0, y, 2 * x + 1 - k)
    x_peer = (0, y, 2 * (1 - x) + k)
    y_early = (0, 1 - y, 2 * x + 1 - y)
    y_late = (0, 1 - y, 2 * x + y)
    tail = pl.ds(NA * CH, (NC - NA) * CH)

    def x_copy(n):
        c = n % NC
        if n < NC:
            return remote(a_ref.at[chunk(c), 1 - x], sc_ref.at[0, 2, chunk(c)], x_send.at[n], x_recv.at[n], x_peer)
        return remote(a_ref.at[chunk(c), x], o_ref.at[2, chunk(c)], x_send.at[n], x_recv.at[n], x_peer)

    def relay_copy(n):
        c = n % NC
        if n < NC:
            return remote(sc_ref.at[0, 2, chunk(c)], sc_ref.at[0, 3, chunk(c)], r_send.at[n], r_recv.at[n], partner)
        return remote(o_ref.at[2, chunk(c)], o_ref.at[3, chunk(c)], r_send.at[n], r_recv.at[n], partner)

    def y_copy(s, c):
        return remote(sc_ref.at[0, 2, chunk(c)], sc_ref.at[1, 2 + s, chunk(c)], y_send.at[c], y_recv.at[s, c], y_late)

    def yr_copy(c):
        return remote(sc_ref.at[0, 2, chunk(c)], yr.at[chunk(c)], q_send.at[c], q_recv.at[c], y_early)

    def yr_relay(c):
        return remote(yr.at[chunk(c)], sc_ref.at[1, 2, chunk(c)], y_send.at[c], y_recv.at[0, c], partner)

    yb_copy = remote(a_ref.at[:, x], yb, b_send.at[0], b_recv.at[0], y_early)
    yb_relay = remote(yb, sc_ref.at[1, 0], b_send.at[1], b_recv.at[1], partner)
    u_copy = remote(a_ref.at[tail, x], sc_ref.at[1, 1, tail], u_send, u_recv, y_late)
    d_copies = [remote(a_ref.at[:, x], sc_ref.at[0, 1], d_send.at[0], d_recv.at[0], partner),
                remote(a_ref.at[:, 1 - x], o_ref.at[1], d_send.at[1], d_recv.at[1], partner)]
    l_copies = [pltpu.make_async_copy(a_ref.at[:, x], sc_ref.at[0, 0], lsem.at[0]),
                pltpu.make_async_copy(a_ref.at[:, 1 - x], o_ref.at[0], lsem.at[1])]
    for cp in l_copies:
        cp.start()
    barrier = pltpu.get_barrier_semaphore()

    @pl.when(early)
    def _():
        signal(barrier, (x_peer, y_early, partner, y_late))
        pl.semaphore_wait(barrier, 2)
        for n in list(range(NC)) + [NC + c for c in O_ORDER]:
            x_copy(n).start()
        yb_copy.start()
        for c in range(NR):
            x_copy(c).wait_recv()
            yr_copy(c).start()
        pl.semaphore_wait(join, 2)
        d_copies[0].start()
        for c in range(NC):
            if c >= NR:
                x_copy(c).wait_recv()
                y_copy(0, c).start()
            relay_copy(c).start()
        yb_copy.wait_recv()
        yb_relay.start()
        for c in range(NR):
            yr_copy(c).wait_recv()
            yr_relay(c).start()
        d_copies[1].start()

    @pl.when(late)
    def _():
        signal(barrier, (x_peer, y_late))
        pl.semaphore_wait(barrier, 4)
        signal(join, (partner, y_early))
        for n in list(range(NA, NC)) + [NC + c for c in O_ORDER]:
            x_copy(n).start()
        for c in range(NA):
            y_copy(1, c).start()
        u_copy.start()
        for c in range(NA):
            relay_copy(c).start()
        for cp in d_copies:
            cp.start()
        for c in range(NA, NC):
            x_copy(c).wait_recv()
            relay_copy(c).start()
            y_copy(1, c).start()

    l_copies[0].wait()
    d_copies[0].wait_recv()
    for c in range(NC):
        relay_copy(c).wait_recv()

    row_blk = 2 * x + y
    for c in range(NC):
        x_copy(NC + O_ORDER[c]).wait_recv()
        relay_copy(NC + O_ORDER[c]).start()
        if c == NC - 2:
            l_copies[1].wait()
            d_copies[1].wait_recv()
            relay_copy(NC + O_ORDER[0]).wait_recv()
        if c >= NC - 2:
            m = c - (NC - 2)
            full_tile(t_ref.at[len(JOBS) + m], o_ref, (), EXTRA[m][0], sc_ref, (side,), EXTRA[m][1])

        @pl.when(late)
        def _():
            if c == 0:
                yb_relay.wait_recv()
            if c == NA:
                u_copy.wait_recv()
            for s in range(2):
                y_copy(s, c).wait_recv()

        base = JOBS.index((c, c))
        diag_tile(t_ref.at[base], sc_ref, (0,), sc_ref, (side,), c, row_blk, col)

        def body(i, _):
            full_tile(t_ref.at[base + i - c], sc_ref, (0,), i, sc_ref, (side,), c)
            return 0
        if c + 1 < NC:
            lax.fori_loop(c + 1, NC, body, 0)

    for c in O_ORDER[1:]:
        relay_copy(NC + c).wait_recv()
    for n in range(2 * NC):
        relay_copy(n).wait_send()
    for n in range(NA, 2 * NC):
        x_copy(n).wait_send()
    for cp in d_copies:
        cp.wait_send()
    for c in range(NC):
        y_copy(0, c).wait_send()

    @pl.when(late)
    def _():
        u_copy.wait_send()

    @pl.when(early)
    def _():
        for n in range(NA):
            x_copy(n).wait_send()
        for c in range(NR):
            yr_copy(c).wait_send()
        yb_copy.wait_send()
        yb_relay.wait_send()


def lookup(n, values):
    out = jnp.int32(values[-1])
    for m in range(len(values) - 2, -1, -1):
        out = jnp.where(n == m, jnp.int32(values[m]), out)
    return out


def write_kernel(sc_ref, o_ref, t_ref, c_in, c_ref, obuf, tsem, osem):
    y, x, k, col = positions()
    side = jnp.where(k != y, 1, 0)

    def pick(n, values):
        return [lookup(n, column) for column in zip(*values)]

    def put(src, i, j, s, sem, act):
        @pl.when(i != j)
        def _():
            act(pltpu.make_async_copy(src, c_ref.at[pl.ds(i * CH, CH), s, :, pl.ds(pl.multiple_of(j * TILE, TILE), TILE)], sem))

        @pl.when(i == j)
        def _():
            for q in range(CH):
                act(pltpu.make_async_copy(
                    src.at[pl.ds(q, CH - q), :, pl.ds(q * BLOCK, BLOCK)],
                    c_ref.at[pl.ds(i * CH + q, CH - q), s, :, pl.ds(pl.multiple_of(j * TILE + q * BLOCK, BLOCK), BLOCK)], sem))

    def put_panel(n, act):
        i, j, cls = pick(n, PANELS)
        put(t_ref.at[n], i, j, jnp.where(cls == 0, x, 1 - x), tsem, act)

    def put_job(n, act):
        i, j = pick(n, LATER)
        b = lax.rem(n, NBUF)
        put(obuf.at[b], i, j, 1 - x, osem.at[b], act)

    def start(cp):
        cp.start()

    def wait(cp):
        cp.wait()

    for n in range(LEAD):
        put_panel(jnp.int32(n), start)

    def body(n, _):
        i, j = pick(n, LATER)
        b = lax.rem(n, NBUF)

        @pl.when(n >= NBUF)
        def _():
            put_job(n - NBUF, wait)

        @pl.when(i != j)
        def _():
            full_tile(obuf.at[b], o_ref, (), i, sc_ref, (side,), j)

        @pl.when(i == j)
        def _():
            diag_tile(obuf.at[b], o_ref, (), sc_ref, (side,), j, 2 * (1 - x) + y, col)
        put_job(n, start)

        @pl.when(n + LEAD < len(PANELS))
        def _():
            put_panel(jnp.minimum(n + LEAD, len(PANELS) - 1), start)
        return 0

    lax.fori_loop(0, len(LATER), body, 0)

    def drain(n, _):
        put_panel(n, wait)

        @pl.when(jnp.logical_and(n >= len(LATER) - NBUF, n < len(LATER)))
        def _():
            put_job(jnp.minimum(n, len(LATER) - 1), wait)
        return 0
    lax.fori_loop(0, len(PANELS), drain, 0)


def solution(mesh):
    def local_fn(a):
        a4 = pltpu.with_memory_space_constraint(a.reshape(NM, 2, BLOCK, PIECE), pltpu.HBM)
        any_spec = pl.BlockSpec(memory_space=pl.ANY)
        hbm = pl.BlockSpec(memory_space=pltpu.HBM)
        vmem = pl.BlockSpec(memory_space=pltpu.VMEM)
        dma = pltpu.SemaphoreType.DMA
        half_flops = 136 * 2 * BLOCK * BLOCK * K_DIM
        panels = pltpu.VMEM((2, PIECES, NM, BLOCK, PIECE), jnp.bfloat16)
        token = jax.ShapeDtypeStruct((8, 128), jnp.float32)
        sc, first = pl.pallas_call(
            first_kernel,
            out_shape=[panels, token],
            in_specs=[hbm],
            out_specs=[vmem, vmem],
            scratch_shapes=[dma(())] * 4,
            compiler_params=pltpu.CompilerParams(collective_id=0, has_side_effects=True, vmem_limit_bytes=2 * 1024 * 1024),
        )(a4)
        c, zeroed = pl.pallas_call(
            zero_kernel,
            out_shape=[jax.ShapeDtypeStruct((NM, 2, BLOCK, NM * BLOCK), jnp.bfloat16), token],
            in_specs=[any_spec],
            out_specs=[any_spec, vmem],
            scratch_shapes=[pltpu.VMEM((CH, BLOCK, TILE), jnp.bfloat16), dma(())],
            compiler_params=pltpu.CompilerParams(vmem_limit_bytes=4 * 1024 * 1024),
            cost_estimate=pl.CostEstimate(flops=half_flops, bytes_accessed=30 << 20, transcendentals=0),
        )(first)
        sc, o, t = pl.pallas_call(
            gather_kernel,
            out_shape=[panels,
                       pltpu.VMEM((PIECES, NM, BLOCK, PIECE), jnp.bfloat16),
                       pltpu.VMEM((len(PANELS), CH, BLOCK, TILE), jnp.bfloat16)],
            in_specs=[hbm, vmem, any_spec],
            out_specs=[vmem] * 3,
            input_output_aliases={1: 0},
            scratch_shapes=[pltpu.VMEM((NM, BLOCK, PIECE), jnp.bfloat16), pltpu.VMEM((NR * CH, BLOCK, PIECE), jnp.bfloat16),
                            pltpu.SemaphoreType.REGULAR,
                            dma((2,)), dma((2,)), dma((2,)), dma((2 * NC,)), dma((2 * NC,)), dma((2 * NC,)), dma((2 * NC,)),
                            dma((NC,)), dma((2, NC)), dma((2,)), dma((2,)), dma((NR,)), dma((NR,)), dma(()), dma(())],
            compiler_params=pltpu.CompilerParams(collective_id=1, has_side_effects=True, vmem_limit_bytes=8 * 1024 * 1024),
            cost_estimate=pl.CostEstimate(flops=half_flops, bytes_accessed=2 << 20, transcendentals=0),
        )(a4, sc, zeroed)
        c = pl.pallas_call(
            write_kernel,
            out_shape=jax.ShapeDtypeStruct((NM, 2, BLOCK, NM * BLOCK), jnp.bfloat16),
            in_specs=[vmem] * 3 + [any_spec],
            out_specs=any_spec,
            input_output_aliases={3: 0},
            scratch_shapes=[pltpu.VMEM((NBUF, CH, BLOCK, TILE), jnp.bfloat16), dma(()), dma((NBUF,))],
            compiler_params=pltpu.CompilerParams(vmem_limit_bytes=15 * 1024 * 1024),
            cost_estimate=pl.CostEstimate(flops=half_flops, bytes_accessed=34 << 20, transcendentals=0),
        )(sc, o, t, c)
        return c.reshape(2 * NM * BLOCK, NM * BLOCK)

    spec = P(('batch', 'row'), 'col')
    return jax.shard_map(local_fn, mesh=mesh, in_specs=(spec,), out_specs=spec, check_vma=False)
```

```python
import functools
import jax
import jax.numpy as jnp
from jax import lax
from jax.experimental import pallas as pl
from jax.experimental.pallas import tpu as pltpu
from jax.sharding import PartitionSpec as P

BLOCK = 256
K_DIM = 512
PIECE = 128
PIECES = K_DIM // PIECE
NM = 16
CH = 4
NC = NM // CH
NBUF = 5
LEAD = 4
TILE = CH * BLOCK
JOBS = [(i, j) for j in range(NC) for i in range(j, NC)]
NA = 14
NR = 2
O_ORDER = (3, 0, 1, 2)
EXTRA = [(3, 0), (3, 1)]
LATER = [job for job in JOBS if job not in EXTRA]
PANELS = [(i, j, 0) for i, j in JOBS] + [(i, j, 1) for i, j in EXTRA]


def positions():
    y = lax.axis_index('row')
    col = lax.axis_index('col')
    return y, col // 2, col % 2, col


def chunk(c):
    return pl.ds(c * CH, CH)


def panel(ref, lead, first, count):
    parts = [ref[(*lead, p, pl.ds(first, count))].reshape(count * BLOCK, PIECE) for p in range(PIECES)]
    return jnp.concatenate(parts, axis=1)


def dot_t(rows, cols):
    return lax.dot_general(rows, cols, (((1,), (1,)), ((), ())), preferred_element_type=jnp.float32)


def full_tile(out, row_ref, row_lead, i, col_ref, col_lead, j):
    prod = dot_t(panel(row_ref, row_lead, i * CH, CH), panel(col_ref, col_lead, j * CH, CH))
    out[...] = prod.astype(jnp.bfloat16).reshape(CH, BLOCK, TILE)


def diag_tile(out, row_ref, row_lead, col_ref, col_lead, j, row_blk, col_blk):
    for q in range(CH):
        prod = dot_t(panel(row_ref, row_lead, j * CH + q, CH - q), panel(col_ref, col_lead, j * CH + q, 1))
        row_id = lax.broadcasted_iota(jnp.int32, (BLOCK, BLOCK), 0) + row_blk * BLOCK
        col_id = lax.broadcasted_iota(jnp.int32, (BLOCK, BLOCK), 1) + col_blk * BLOCK
        lanes = slice(q * BLOCK, (q + 1) * BLOCK)
        out[q, :, lanes] = jnp.where(row_id >= col_id, prod[:BLOCK], 0.0).astype(jnp.bfloat16)
        if q + 1 < CH:
            out[q + 1:, :, lanes] = prod[BLOCK:].astype(jnp.bfloat16).reshape(CH - q - 1, BLOCK, BLOCK)


MESH_ID = pl.DeviceIdType.MESH


def remote(src, dst, send, recv, dev):
    return pltpu.make_async_remote_copy(src, dst, send, recv, device_id=dev, device_id_type=MESH_ID)


def signal(sem, devices):
    for dev in devices:
        pl.semaphore_signal(sem, inc=1, device_id=dev, device_id_type=MESH_ID)


def first_kernel(a_ref, sc_ref, token_ref, x_send, x_recv, y_send, y_recv):
    y, x, k, _ = positions()
    token_ref[...] = jnp.zeros_like(token_ref)

    @pl.when(k != y)
    def _():
        x_peer = (0, y, 2 * (1 - x) + k)
        y_peer = (0, 1 - y, 2 * x + y)
        barrier = pltpu.get_barrier_semaphore()
        signal(barrier, (x_peer, y_peer))
        pl.semaphore_wait(barrier, 2)
        part = pl.ds(0, NA)
        xc = remote(a_ref.at[part, 1 - x], sc_ref.at[0, 2, part], x_send, x_recv, x_peer)
        yc = remote(a_ref.at[part, x], sc_ref.at[1, 1, part], y_send, y_recv, y_peer)
        xc.start()
        yc.start()
        xc.wait()
        yc.wait()


def zero_kernel(token_ref, c_ref, done_ref, zbuf, sem):
    zbuf[...] = jnp.zeros_like(zbuf)
    done_ref[...] = jnp.zeros_like(done_ref)
    copies = []
    for s in range(2):
        for i in range(NC):
            for j in range(i + 1, NC):
                copies.append(pltpu.make_async_copy(zbuf, c_ref.at[chunk(i), s, :, pl.ds(j * TILE, TILE)], sem))
            for q in range(1, CH):
                copies.append(pltpu.make_async_copy(
                    zbuf.at[pl.ds(0, q), :, pl.ds(0, BLOCK)],
                    c_ref.at[pl.ds(i * CH, q), s, :, pl.ds((i * CH + q) * BLOCK, BLOCK)], sem))
    for cp in copies:
        cp.start()
    for cp in copies:
        cp.wait()


def gather_kernel(a_ref, sc_in, token_ref, sc_ref, o_ref, t_ref, yb, yr, join, lsem, d_send, d_recv, x_send, x_recv, r_send, r_recv,
                  y_send, y_recv, b_send, b_recv, q_send, q_recv, u_send, u_recv, v_send, v_recv):
    y, x, k, col = positions()
    late = k != y
    early = k == y
    side = jnp.where(late, 1, 0)
    partner = (0, y, 2 * x + 1 - k)
    x_peer = (0, y, 2 * (1 - x) + k)
    y_early = (0, 1 - y, 2 * x + 1 - y)
    y_late = (0, 1 - y, 2 * x + y)
    tail = pl.ds(NA, NM - NA)

    def x_copy(n):
        c = n % NC
        if n < NC:
            return remote(a_ref.at[chunk(c), 1 - x], sc_ref.at[0, 2, chunk(c)], x_send.at[n], x_recv.at[n], x_peer)
        return remote(a_ref.at[chunk(c), x], o_ref.at[2, chunk(c)], x_send.at[n], x_recv.at[n], x_peer)

    def relay_copy(n):
        c = n % NC
        if n < NC:
            return remote(sc_ref.at[0, 2, chunk(c)], sc_ref.at[0, 3, chunk(c)], r_send.at[n], r_recv.at[n], partner)
        return remote(o_ref.at[2, chunk(c)], o_ref.at[3, chunk(c)], r_send.at[n], r_recv.at[n], partner)

    def y_copy(s, c):
        return remote(sc_ref.at[0, 2, chunk(c)], sc_ref.at[1, 2 + s, chunk(c)], y_send.at[c], y_recv.at[s, c], y_late)

    def yr_copy(c):
        return remote(sc_ref.at[0, 2, chunk(c)], yr.at[chunk(c)], q_send.at[c], q_recv.at[c], y_early)

    def yr_relay(c):
        return remote(yr.at[chunk(c)], sc_ref.at[1, 2, chunk(c)], y_send.at[c], y_recv.at[0, c], partner)

    yb_copy = remote(a_ref.at[:, x], yb, b_send.at[0], b_recv.at[0], y_early)
    yb_relay = remote(yb, sc_ref.at[1, 0], b_send.at[1], b_recv.at[1], partner)
    x_tail = remote(a_ref.at[tail, 1 - x], sc_ref.at[0, 2, tail], v_send, v_recv, x_peer)
    u_copy = remote(a_ref.at[tail, x], sc_ref.at[1, 1, tail], u_send, u_recv, y_late)
    d_copies = [remote(a_ref.at[:, x], sc_ref.at[0, 1], d_send.at[0], d_recv.at[0], partner),
                remote(a_ref.at[:, 1 - x], o_ref.at[1], d_send.at[1], d_recv.at[1], partner)]
    l_copies = [pltpu.make_async_copy(a_ref.at[:, x], sc_ref.at[0, 0], lsem.at[0]),
                pltpu.make_async_copy(a_ref.at[:, 1 - x], o_ref.at[0], lsem.at[1])]
    for cp in l_copies:
        cp.start()
    barrier = pltpu.get_barrier_semaphore()

    @pl.when(early)
    def _():
        signal(barrier, (x_peer, y_early, partner, y_late))
        pl.semaphore_wait(barrier, 2)
        for n in list(range(NC)) + [NC + c for c in O_ORDER]:
            x_copy(n).start()
        yb_copy.start()
        for c in range(NR):
            x_copy(c).wait_recv()
            yr_copy(c).start()
        pl.semaphore_wait(join, 2)
        d_copies[0].start()
        for c in range(NC):
            if c >= NR:
                x_copy(c).wait_recv()
                y_copy(0, c).start()
            relay_copy(c).start()
        yb_copy.wait_recv()
        yb_relay.start()
        for c in range(NR):
            yr_copy(c).wait_recv()
            yr_relay(c).start()
        d_copies[1].start()

    @pl.when(late)
    def _():
        signal(barrier, (x_peer, y_late))
        pl.semaphore_wait(barrier, 4)
        signal(join, (partner, y_early))
        x_tail.start()
        for c in O_ORDER:
            x_copy(NC + c).start()
        for c in range(NC - 1):
            y_copy(1, c).start()
        u_copy.start()
        for c in range(NC - 1):
            relay_copy(c).start()
        for cp in d_copies:
            cp.start()
        x_tail.wait_recv()
        relay_copy(NC - 1).start()
        y_copy(1, NC - 1).start()

    l_copies[0].wait()
    d_copies[0].wait_recv()
    for c in range(NC):
        relay_copy(c).wait_recv()

    row_blk = 2 * x + y
    for c in range(NC):
        x_copy(NC + O_ORDER[c]).wait_recv()
        relay_copy(NC + O_ORDER[c]).start()
        if c == NC - 2:
            l_copies[1].wait()
            d_copies[1].wait_recv()
            relay_copy(NC + O_ORDER[0]).wait_recv()
        if c >= NC - 2:
            m = c - (NC - 2)
            full_tile(t_ref.at[len(JOBS) + m], o_ref, (), EXTRA[m][0], sc_ref, (side,), EXTRA[m][1])

        @pl.when(late)
        def _():
            if c == 0:
                yb_relay.wait_recv()
            if c == NC - 1:
                u_copy.wait_recv()
            for s in range(2):
                y_copy(s, c).wait_recv()

        base = JOBS.index((c, c))
        diag_tile(t_ref.at[base], sc_ref, (0,), sc_ref, (side,), c, row_blk, col)

        def body(i, _):
            full_tile(t_ref.at[base + i - c], sc_ref, (0,), i, sc_ref, (side,), c)
            return 0
        if c + 1 < NC:
            lax.fori_loop(c + 1, NC, body, 0)

    for c in O_ORDER[1:]:
        relay_copy(NC + c).wait_recv()
    for n in range(2 * NC):
        relay_copy(n).wait_send()
    for n in range(NC, 2 * NC):
        x_copy(n).wait_send()
    for cp in d_copies:
        cp.wait_send()
    for c in range(NC):
        y_copy(0, c).wait_send()

    @pl.when(late)
    def _():
        u_copy.wait_send()
        x_tail.wait_send()

    @pl.when(early)
    def _():
        for n in range(NC):
            x_copy(n).wait_send()
        for c in range(NR):
            yr_copy(c).wait_send()
        yb_copy.wait_send()
        yb_relay.wait_send()


def lookup(n, values):
    out = jnp.int32(values[-1])
    for m in range(len(values) - 2, -1, -1):
        out = jnp.where(n == m, jnp.int32(values[m]), out)
    return out


def write_kernel(sc_ref, o_ref, t_ref, c_in, c_ref, obuf, tsem, osem):
    y, x, k, col = positions()
    side = jnp.where(k != y, 1, 0)

    def pick(n, values):
        return [lookup(n, column) for column in zip(*values)]

    def put(src, i, j, s, sem, act):
        @pl.when(i != j)
        def _():
            act(pltpu.make_async_copy(src, c_ref.at[pl.ds(i * CH, CH), s, :, pl.ds(pl.multiple_of(j * TILE, TILE), TILE)], sem))

        @pl.when(i == j)
        def _():
            for q in range(CH):
                act(pltpu.make_async_copy(
                    src.at[pl.ds(q, CH - q), :, pl.ds(q * BLOCK, BLOCK)],
                    c_ref.at[pl.ds(i * CH + q, CH - q), s, :, pl.ds(pl.multiple_of(j * TILE + q * BLOCK, BLOCK), BLOCK)], sem))

    def put_panel(n, act):
        i, j, cls = pick(n, PANELS)
        put(t_ref.at[n], i, j, jnp.where(cls == 0, x, 1 - x), tsem, act)

    def put_job(n, act):
        i, j = pick(n, LATER)
        b = lax.rem(n, NBUF)
        put(obuf.at[b], i, j, 1 - x, osem.at[b], act)

    def start(cp):
        cp.start()

    def wait(cp):
        cp.wait()

    for n in range(LEAD):
        put_panel(jnp.int32(n), start)

    def body(n, _):
        i, j = pick(n, LATER)
        b = lax.rem(n, NBUF)

        @pl.when(n >= NBUF)
        def _():
            put_job(n - NBUF, wait)

        @pl.when(i != j)
        def _():
            full_tile(obuf.at[b], o_ref, (), i, sc_ref, (side,), j)

        @pl.when(i == j)
        def _():
            diag_tile(obuf.at[b], o_ref, (), sc_ref, (side,), j, 2 * (1 - x) + y, col)
        put_job(n, start)

        @pl.when(n + LEAD < len(PANELS))
        def _():
            put_panel(jnp.minimum(n + LEAD, len(PANELS) - 1), start)
        return 0

    lax.fori_loop(0, len(LATER), body, 0)

    def drain(n, _):
        put_panel(n, wait)

        @pl.when(jnp.logical_and(n >= len(LATER) - NBUF, n < len(LATER)))
        def _():
            put_job(jnp.minimum(n, len(LATER) - 1), wait)
        return 0
    lax.fori_loop(0, len(PANELS), drain, 0)


def solution(mesh):
    def local_fn(a):
        a4 = pltpu.with_memory_space_constraint(a.reshape(NM, 2, BLOCK, PIECE), pltpu.HBM)
        any_spec = pl.BlockSpec(memory_space=pl.ANY)
        hbm = pl.BlockSpec(memory_space=pltpu.HBM)
        vmem = pl.BlockSpec(memory_space=pltpu.VMEM)
        dma = pltpu.SemaphoreType.DMA
        half_flops = 136 * 2 * BLOCK * BLOCK * K_DIM
        panels = pltpu.VMEM((2, PIECES, NM, BLOCK, PIECE), jnp.bfloat16)
        token = jax.ShapeDtypeStruct((8, 128), jnp.float32)
        sc, first = pl.pallas_call(
            first_kernel,
            out_shape=[panels, token],
            in_specs=[hbm],
            out_specs=[vmem, vmem],
            scratch_shapes=[dma(())] * 4,
            compiler_params=pltpu.CompilerParams(collective_id=0, has_side_effects=True, vmem_limit_bytes=2 * 1024 * 1024),
        )(a4)
        c, zeroed = pl.pallas_call(
            zero_kernel,
            out_shape=[jax.ShapeDtypeStruct((NM, 2, BLOCK, NM * BLOCK), jnp.bfloat16), token],
            in_specs=[any_spec],
            out_specs=[any_spec, vmem],
            scratch_shapes=[pltpu.VMEM((CH, BLOCK, TILE), jnp.bfloat16), dma(())],
            compiler_params=pltpu.CompilerParams(vmem_limit_bytes=4 * 1024 * 1024),
            cost_estimate=pl.CostEstimate(flops=half_flops, bytes_accessed=30 << 20, transcendentals=0),
        )(first)
        sc, o, t = pl.pallas_call(
            gather_kernel,
            out_shape=[panels,
                       pltpu.VMEM((PIECES, NM, BLOCK, PIECE), jnp.bfloat16),
                       pltpu.VMEM((len(PANELS), CH, BLOCK, TILE), jnp.bfloat16)],
            in_specs=[hbm, vmem, any_spec],
            out_specs=[vmem] * 3,
            input_output_aliases={1: 0},
            scratch_shapes=[pltpu.VMEM((NM, BLOCK, PIECE), jnp.bfloat16), pltpu.VMEM((NR * CH, BLOCK, PIECE), jnp.bfloat16),
                            pltpu.SemaphoreType.REGULAR,
                            dma((2,)), dma((2,)), dma((2,)), dma((2 * NC,)), dma((2 * NC,)), dma((2 * NC,)), dma((2 * NC,)),
                            dma((NC,)), dma((2, NC)), dma((2,)), dma((2,)), dma((NR,)), dma((NR,))] + [dma(())] * 4,
            compiler_params=pltpu.CompilerParams(collective_id=1, has_side_effects=True, vmem_limit_bytes=8 * 1024 * 1024),
            cost_estimate=pl.CostEstimate(flops=half_flops, bytes_accessed=2 << 20, transcendentals=0),
        )(a4, sc, zeroed)
        c = pl.pallas_call(
            write_kernel,
            out_shape=jax.ShapeDtypeStruct((NM, 2, BLOCK, NM * BLOCK), jnp.bfloat16),
            in_specs=[vmem] * 3 + [any_spec],
            out_specs=any_spec,
            input_output_aliases={3: 0},
            scratch_shapes=[pltpu.VMEM((NBUF, CH, BLOCK, TILE), jnp.bfloat16), dma(()), dma((NBUF,))],
            compiler_params=pltpu.CompilerParams(vmem_limit_bytes=15 * 1024 * 1024),
            cost_estimate=pl.CostEstimate(flops=half_flops, bytes_accessed=34 << 20, transcendentals=0),
        )(sc, o, t, c)
        return c.reshape(2 * NM * BLOCK, NM * BLOCK)

    spec = P(('batch', 'row'), 'col')
    return jax.shard_map(local_fn, mesh=mesh, in_specs=(spec,), out_specs=spec, check_vma=False)
```

```python
import functools
import jax
import jax.numpy as jnp
from jax import lax
from jax.experimental import pallas as pl
from jax.experimental.pallas import tpu as pltpu
from jax.sharding import PartitionSpec as P

BLOCK = 256
K_DIM = 512
PIECE = 128
PIECES = K_DIM // PIECE
NM = 16
CH = 4
NC = NM // CH
NBUF = 5
LEAD = 4
TILE = CH * BLOCK
JOBS = [(i, j) for j in range(NC) for i in range(j, NC)]
LAST = (NC - 1, NC - 1)
NOW = [job for job in JOBS if job != LAST]
NAX, NAY = 15, 14
NR = 2
O_PARTS = ((12, 4), (0, 4), (4, 4), (8, 3), (11, 1))
NX = NC + len(O_PARTS)
EXTRA = [(3, 0), (3, 1)]
LATER = [job for job in JOBS if job not in EXTRA]
PANELS = [(i, j, 0) for i, j in NOW] + [(i, j, 1) for i, j in EXTRA]


def positions():
    y = lax.axis_index('row')
    col = lax.axis_index('col')
    return y, col // 2, col % 2, col


def chunk(c):
    return pl.ds(c * CH, CH)


def panel(ref, lead, first, count):
    parts = [ref[(*lead, p, pl.ds(first, count))].reshape(count * BLOCK, PIECE) for p in range(PIECES)]
    return jnp.concatenate(parts, axis=1)


def dot_t(rows, cols):
    return lax.dot_general(rows, cols, (((1,), (1,)), ((), ())), preferred_element_type=jnp.float32)


def full_tile(out, row_ref, row_lead, i, col_ref, col_lead, j):
    prod = dot_t(panel(row_ref, row_lead, i * CH, CH), panel(col_ref, col_lead, j * CH, CH))
    out[...] = prod.astype(jnp.bfloat16).reshape(CH, BLOCK, TILE)


def diag_tile(out, row_ref, row_lead, col_ref, col_lead, j, row_blk, col_blk):
    for q in range(CH):
        prod = dot_t(panel(row_ref, row_lead, j * CH + q, CH - q), panel(col_ref, col_lead, j * CH + q, 1))
        row_id = lax.broadcasted_iota(jnp.int32, (BLOCK, BLOCK), 0) + row_blk * BLOCK
        col_id = lax.broadcasted_iota(jnp.int32, (BLOCK, BLOCK), 1) + col_blk * BLOCK
        lanes = slice(q * BLOCK, (q + 1) * BLOCK)
        out[q, :, lanes] = jnp.where(row_id >= col_id, prod[:BLOCK], 0.0).astype(jnp.bfloat16)
        if q + 1 < CH:
            out[q + 1:, :, lanes] = prod[BLOCK:].astype(jnp.bfloat16).reshape(CH - q - 1, BLOCK, BLOCK)


MESH_ID = pl.DeviceIdType.MESH


def remote(src, dst, send, recv, dev):
    return pltpu.make_async_remote_copy(src, dst, send, recv, device_id=dev, device_id_type=MESH_ID)


def signal(sem, devices):
    for dev in devices:
        pl.semaphore_signal(sem, inc=1, device_id=dev, device_id_type=MESH_ID)


def first_kernel(a_ref, sc_ref, token_ref, x_send, x_recv, y_send, y_recv):
    y, x, k, _ = positions()
    token_ref[...] = jnp.zeros_like(token_ref)

    @pl.when(k != y)
    def _():
        x_peer = (0, y, 2 * (1 - x) + k)
        y_peer = (0, 1 - y, 2 * x + y)
        barrier = pltpu.get_barrier_semaphore()
        signal(barrier, (x_peer, y_peer))
        pl.semaphore_wait(barrier, 2)
        px, py = pl.ds(0, NAX), pl.ds(0, NAY)
        xc = remote(a_ref.at[px, 1 - x], sc_ref.at[0, 2, px], x_send, x_recv, x_peer)
        yc = remote(a_ref.at[py, x], sc_ref.at[1, 1, py], y_send, y_recv, y_peer)
        xc.start()
        yc.start()
        xc.wait()
        yc.wait()


def zero_kernel(token_ref, c_ref, done_ref, zbuf, sem):
    zbuf[...] = jnp.zeros_like(zbuf)
    done_ref[...] = jnp.zeros_like(done_ref)
    copies = []
    for s in range(2):
        for i in range(NC):
            for j in range(i + 1, NC):
                copies.append(pltpu.make_async_copy(zbuf, c_ref.at[chunk(i), s, :, pl.ds(j * TILE, TILE)], sem))
            for q in range(1, CH):
                copies.append(pltpu.make_async_copy(
                    zbuf.at[pl.ds(0, q), :, pl.ds(0, BLOCK)],
                    c_ref.at[pl.ds(i * CH, q), s, :, pl.ds((i * CH + q) * BLOCK, BLOCK)], sem))
    for cp in copies:
        cp.start()
    for cp in copies:
        cp.wait()


def gather_kernel(a_ref, sc_in, token_ref, sc_ref, o_ref, t_ref, yb, yr, join, lsem, d_send, d_recv, x_send, x_recv, r_send, r_recv,
                  y_send, y_recv, b_send, b_recv, q_send, q_recv, u_send, u_recv, v_send, v_recv):
    y, x, k, col = positions()
    late = k != y
    early = k == y
    side = jnp.where(late, 1, 0)
    partner = (0, y, 2 * x + 1 - k)
    x_peer = (0, y, 2 * (1 - x) + k)
    y_early = (0, 1 - y, 2 * x + 1 - y)
    y_late = (0, 1 - y, 2 * x + y)
    tx, ty = pl.ds(NAX, NM - NAX), pl.ds(NAY, NM - NAY)

    def x_copy(n):
        if n < NC:
            return remote(a_ref.at[chunk(n), 1 - x], sc_ref.at[0, 2, chunk(n)], x_send.at[n], x_recv.at[n], x_peer)
        part = pl.ds(*O_PARTS[n - NC])
        return remote(a_ref.at[part, x], o_ref.at[2, part], x_send.at[n], x_recv.at[n], x_peer)

    def relay_copy(n):
        if n < NC:
            return remote(sc_ref.at[0, 2, chunk(n)], sc_ref.at[0, 3, chunk(n)], r_send.at[n], r_recv.at[n], partner)
        part = pl.ds(*O_PARTS[n - NC])
        return remote(o_ref.at[2, part], o_ref.at[3, part], r_send.at[n], r_recv.at[n], partner)

    def y_copy(s, c):
        return remote(sc_ref.at[0, 2, chunk(c)], sc_ref.at[1, 2 + s, chunk(c)], y_send.at[c], y_recv.at[s, c], y_late)

    def yr_copy(c):
        return remote(sc_ref.at[0, 2, chunk(c)], yr.at[chunk(c)], q_send.at[c], q_recv.at[c], y_early)

    def yr_relay(c):
        return remote(yr.at[chunk(c)], sc_ref.at[1, 2, chunk(c)], y_send.at[c], y_recv.at[0, c], partner)

    yb_copy = remote(a_ref.at[:, x], yb, b_send.at[0], b_recv.at[0], y_early)
    yb_relay = remote(yb, sc_ref.at[1, 0], b_send.at[1], b_recv.at[1], partner)
    x_tail = remote(a_ref.at[tx, 1 - x], sc_ref.at[0, 2, tx], v_send, v_recv, x_peer)
    u_copy = remote(a_ref.at[ty, x], sc_ref.at[1, 1, ty], u_send, u_recv, y_late)
    d_copies = [remote(a_ref.at[:, x], sc_ref.at[0, 1], d_send.at[0], d_recv.at[0], partner),
                remote(a_ref.at[:, 1 - x], o_ref.at[1], d_send.at[1], d_recv.at[1], partner)]
    l_copies = [pltpu.make_async_copy(a_ref.at[:, x], sc_ref.at[0, 0], lsem.at[0]),
                pltpu.make_async_copy(a_ref.at[:, 1 - x], o_ref.at[0], lsem.at[1])]
    for cp in l_copies:
        cp.start()
    barrier = pltpu.get_barrier_semaphore()

    @pl.when(early)
    def _():
        signal(barrier, (x_peer, y_early, partner, y_late))
        pl.semaphore_wait(barrier, 2)
        for n in range(NX):
            x_copy(n).start()
        yb_copy.start()
        for c in range(NR):
            x_copy(c).wait_recv()
            yr_copy(c).start()
        pl.semaphore_wait(join, 2)
        d_copies[0].start()
        for c in range(NC):
            if c >= NR:
                x_copy(c).wait_recv()
                y_copy(0, c).start()
            relay_copy(c).start()
        yb_copy.wait_recv()
        yb_relay.start()
        for c in range(NR):
            yr_copy(c).wait_recv()
            yr_relay(c).start()
        d_copies[1].start()

    @pl.when(late)
    def _():
        signal(barrier, (x_peer, y_late))
        pl.semaphore_wait(barrier, 4)
        signal(join, (partner, y_early))
        x_tail.start()
        for n in range(NC, NX):
            x_copy(n).start()
        for c in range(NC - 1):
            y_copy(1, c).start()
        u_copy.start()
        for c in range(NC - 1):
            relay_copy(c).start()
        for cp in d_copies:
            cp.start()
        x_tail.wait_recv()
        relay_copy(NC - 1).start()
        y_copy(1, NC - 1).start()

    l_copies[0].wait()
    d_copies[0].wait_recv()
    for c in range(NC):
        relay_copy(c).wait_recv()

    row_blk = 2 * x + y
    for c in range(NC):
        for n in ([c] if c < NC - 1 else range(c, len(O_PARTS))):
            x_copy(NC + n).wait_recv()
            relay_copy(NC + n).start()

        @pl.when(late)
        def _():
            if c == 0:
                yb_relay.wait_recv()
            if c == NC - 1:
                u_copy.wait_recv()
            for s in range(2):
                y_copy(s, c).wait_recv()

        if c < NC - 1:
            base = NOW.index((c, c))
            diag_tile(t_ref.at[base], sc_ref, (0,), sc_ref, (side,), c, row_blk, col)

            def body(i, _):
                full_tile(t_ref.at[base + i - c], sc_ref, (0,), i, sc_ref, (side,), c)
                return 0
            lax.fori_loop(c + 1, NC, body, 0)
        if c == 1:
            l_copies[1].wait()
            d_copies[1].wait_recv()
            relay_copy(NC).wait_recv()
        if c in (1, 2):
            i, j = EXTRA[c - 1]
            full_tile(t_ref.at[len(NOW) + c - 1], o_ref, (), i, sc_ref, (side,), j)

    for n in range(1, len(O_PARTS)):
        relay_copy(NC + n).wait_recv()
    for n in range(NX):
        relay_copy(n).wait_send()
    for n in range(NC, NX):
        x_copy(n).wait_send()
    for cp in d_copies:
        cp.wait_send()
    for c in range(NC):
        y_copy(0, c).wait_send()

    @pl.when(late)
    def _():
        u_copy.wait_send()
        x_tail.wait_send()

    @pl.when(early)
    def _():
        for n in range(NC):
            x_copy(n).wait_send()
        for c in range(NR):
            yr_copy(c).wait_send()
        yb_copy.wait_send()
        yb_relay.wait_send()


def lookup(n, values):
    out = jnp.int32(values[-1])
    for m in range(len(values) - 2, -1, -1):
        out = jnp.where(n == m, jnp.int32(values[m]), out)
    return out


def write_kernel(sc_ref, o_ref, t_ref, c_in, c_ref, obuf, tsem, osem):
    y, x, k, col = positions()
    side = jnp.where(k != y, 1, 0)

    def pick(n, values):
        return [lookup(n, column) for column in zip(*values)]

    def put(src, i, j, s, sem, act):
        @pl.when(i != j)
        def _():
            act(pltpu.make_async_copy(src, c_ref.at[pl.ds(i * CH, CH), s, :, pl.ds(pl.multiple_of(j * TILE, TILE), TILE)], sem))

        @pl.when(i == j)
        def _():
            for q in range(CH):
                act(pltpu.make_async_copy(
                    src.at[pl.ds(q, CH - q), :, pl.ds(q * BLOCK, BLOCK)],
                    c_ref.at[pl.ds(i * CH + q, CH - q), s, :, pl.ds(pl.multiple_of(j * TILE + q * BLOCK, BLOCK), BLOCK)], sem))

    def put_panel(n, act):
        i, j, cls = pick(n, PANELS)
        put(t_ref.at[n], i, j, jnp.where(cls == 0, x, 1 - x), tsem, act)

    def put_job(n, act):
        i, j = pick(n, LATER)
        b = lax.rem(n, NBUF)
        put(obuf.at[b], i, j, 1 - x, osem.at[b], act)

    def start(cp):
        cp.start()

    def wait(cp):
        cp.wait()

    for n in range(LEAD):
        put_panel(jnp.int32(n), start)

    def body(n, _):
        i, j = pick(n, LATER)
        b = lax.rem(n, NBUF)

        @pl.when(n >= NBUF)
        def _():
            put_job(n - NBUF, wait)

        @pl.when(i != j)
        def _():
            full_tile(obuf.at[b], o_ref, (), i, sc_ref, (side,), j)

        @pl.when(i == j)
        def _():
            diag_tile(obuf.at[b], o_ref, (), sc_ref, (side,), j, 2 * (1 - x) + y, col)
        put_job(n, start)

        @pl.when(n + LEAD < len(PANELS))
        def _():
            put_panel(jnp.minimum(n + LEAD, len(PANELS) - 1), start)
        return 0

    lax.fori_loop(0, len(LATER), body, 0)
    last_slot = len(LATER) % NBUF
    put_job(jnp.int32(len(LATER) - NBUF), wait)
    diag_tile(obuf.at[last_slot], sc_ref, (0,), sc_ref, (side,), LAST[1], 2 * x + y, col)
    put(obuf.at[last_slot], jnp.int32(LAST[0]), jnp.int32(LAST[1]), x, osem.at[last_slot], start)

    def drain(n, _):
        put_panel(n, wait)

        @pl.when(jnp.logical_and(n > len(LATER) - NBUF, n < len(LATER)))
        def _():
            put_job(jnp.minimum(n, len(LATER) - 1), wait)
        return 0
    lax.fori_loop(0, len(PANELS), drain, 0)
    put(obuf.at[last_slot], jnp.int32(LAST[0]), jnp.int32(LAST[1]), x, osem.at[last_slot], wait)


def solution(mesh):
    def local_fn(a):
        a4 = pltpu.with_memory_space_constraint(a.reshape(NM, 2, BLOCK, PIECE), pltpu.HBM)
        any_spec = pl.BlockSpec(memory_space=pl.ANY)
        hbm = pl.BlockSpec(memory_space=pltpu.HBM)
        vmem = pl.BlockSpec(memory_space=pltpu.VMEM)
        dma = pltpu.SemaphoreType.DMA
        half_flops = 136 * 2 * BLOCK * BLOCK * K_DIM
        panels = pltpu.VMEM((2, PIECES, NM, BLOCK, PIECE), jnp.bfloat16)
        token = jax.ShapeDtypeStruct((8, 128), jnp.float32)
        sc, first = pl.pallas_call(
            first_kernel,
            out_shape=[panels, token],
            in_specs=[hbm],
            out_specs=[vmem, vmem],
            scratch_shapes=[dma(())] * 4,
            compiler_params=pltpu.CompilerParams(collective_id=0, has_side_effects=True, vmem_limit_bytes=2 * 1024 * 1024),
        )(a4)
        c, zeroed = pl.pallas_call(
            zero_kernel,
            out_shape=[jax.ShapeDtypeStruct((NM, 2, BLOCK, NM * BLOCK), jnp.bfloat16), token],
            in_specs=[any_spec],
            out_specs=[any_spec, vmem],
            scratch_shapes=[pltpu.VMEM((CH, BLOCK, TILE), jnp.bfloat16), dma(())],
            compiler_params=pltpu.CompilerParams(vmem_limit_bytes=4 * 1024 * 1024),
            cost_estimate=pl.CostEstimate(flops=half_flops, bytes_accessed=30 << 20, transcendentals=0),
        )(first)
        sc, o, t = pl.pallas_call(
            gather_kernel,
            out_shape=[panels,
                       pltpu.VMEM((PIECES, NM, BLOCK, PIECE), jnp.bfloat16),
                       pltpu.VMEM((len(PANELS), CH, BLOCK, TILE), jnp.bfloat16)],
            in_specs=[hbm, vmem, any_spec],
            out_specs=[vmem] * 3,
            input_output_aliases={1: 0},
            scratch_shapes=[pltpu.VMEM((NM, BLOCK, PIECE), jnp.bfloat16), pltpu.VMEM((NR * CH, BLOCK, PIECE), jnp.bfloat16),
                            pltpu.SemaphoreType.REGULAR,
                            dma((2,)), dma((2,)), dma((2,)), dma((NX,)), dma((NX,)), dma((NX,)), dma((NX,)),
                            dma((NC,)), dma((2, NC)), dma((2,)), dma((2,)), dma((NR,)), dma((NR,))] + [dma(())] * 4,
            compiler_params=pltpu.CompilerParams(collective_id=1, has_side_effects=True, vmem_limit_bytes=8 * 1024 * 1024),
            cost_estimate=pl.CostEstimate(flops=half_flops, bytes_accessed=2 << 20, transcendentals=0),
        )(a4, sc, zeroed)
        c = pl.pallas_call(
            write_kernel,
            out_shape=jax.ShapeDtypeStruct((NM, 2, BLOCK, NM * BLOCK), jnp.bfloat16),
            in_specs=[vmem] * 3 + [any_spec],
            out_specs=any_spec,
            input_output_aliases={3: 0},
            scratch_shapes=[pltpu.VMEM((NBUF, CH, BLOCK, TILE), jnp.bfloat16), dma(()), dma((NBUF,))],
            compiler_params=pltpu.CompilerParams(vmem_limit_bytes=15 * 1024 * 1024),
            cost_estimate=pl.CostEstimate(flops=half_flops, bytes_accessed=34 << 20, transcendentals=0),
        )(sc, o, t, c)
        return c.reshape(2 * NM * BLOCK, NM * BLOCK)

    spec = P(('batch', 'row'), 'col')
    return jax.shard_map(local_fn, mesh=mesh, in_specs=(spec,), out_specs=spec, check_vma=False)
```

```python
import functools
import jax
import jax.numpy as jnp
from jax import lax
from jax.experimental import pallas as pl
from jax.experimental.pallas import tpu as pltpu
from jax.sharding import PartitionSpec as P

BLOCK = 256
K_DIM = 512
PIECE = 128
PIECES = K_DIM // PIECE
NM = 16
CH = 4
NC = NM // CH
NBUF = 5
LEAD = 4
TILE = CH * BLOCK
JOBS = [(i, j) for j in range(NC) for i in range(j, NC)]
LAST = (NC - 1, NC - 1)
NOW = [job for job in JOBS if job != LAST]
NAX, NAY = 15, 14
NR = 2
O_PARTS = ((12, 4), (0, 4), (4, 4), (8, 3), (11, 1))
NX = NC + len(O_PARTS)
EXTRA = [(3, 0), (3, 1)]
LATER = [job for job in JOBS if job not in EXTRA]
PANELS = [(i, j, 0) for i, j in NOW] + [(i, j, 1) for i, j in EXTRA]


def positions():
    y = lax.axis_index('row')
    col = lax.axis_index('col')
    return y, col // 2, col % 2, col


def chunk(c):
    return pl.ds(c * CH, CH)


def panel(ref, lead, first, count):
    parts = [ref[(*lead, p, pl.ds(first, count))].reshape(count * BLOCK, PIECE) for p in range(PIECES)]
    return jnp.concatenate(parts, axis=1)


def dot_t(rows, cols):
    return lax.dot_general(rows, cols, (((1,), (1,)), ((), ())), preferred_element_type=jnp.float32)


def full_tile(out, row_ref, row_lead, i, col_ref, col_lead, j):
    prod = dot_t(panel(row_ref, row_lead, i * CH, CH), panel(col_ref, col_lead, j * CH, CH))
    out[...] = prod.astype(jnp.bfloat16).reshape(CH, BLOCK, TILE)


def diag_tile(out, row_ref, row_lead, col_ref, col_lead, j, row_blk, col_blk):
    for q in range(CH):
        prod = dot_t(panel(row_ref, row_lead, j * CH + q, CH - q), panel(col_ref, col_lead, j * CH + q, 1))
        row_id = lax.broadcasted_iota(jnp.int32, (BLOCK, BLOCK), 0) + row_blk * BLOCK
        col_id = lax.broadcasted_iota(jnp.int32, (BLOCK, BLOCK), 1) + col_blk * BLOCK
        lanes = slice(q * BLOCK, (q + 1) * BLOCK)
        out[q, :, lanes] = jnp.where(row_id >= col_id, prod[:BLOCK], 0.0).astype(jnp.bfloat16)
        if q + 1 < CH:
            out[q + 1:, :, lanes] = prod[BLOCK:].astype(jnp.bfloat16).reshape(CH - q - 1, BLOCK, BLOCK)


MESH_ID = pl.DeviceIdType.MESH


def remote(src, dst, send, recv, dev):
    return pltpu.make_async_remote_copy(src, dst, send, recv, device_id=dev, device_id_type=MESH_ID)


def signal(sem, devices):
    for dev in devices:
        pl.semaphore_signal(sem, inc=1, device_id=dev, device_id_type=MESH_ID)


def first_kernel(a_ref, sc_ref, token_ref, x_send, x_recv, y_send, y_recv):
    y, x, k, _ = positions()
    token_ref[...] = jnp.zeros_like(token_ref)

    @pl.when(k != y)
    def _():
        x_peer = (0, y, 2 * (1 - x) + k)
        y_peer = (0, 1 - y, 2 * x + y)
        barrier = pltpu.get_barrier_semaphore()
        signal(barrier, (x_peer, y_peer))
        pl.semaphore_wait(barrier, 2)
        px, py = pl.ds(0, NAX), pl.ds(0, NAY)
        xc = remote(a_ref.at[px, 1 - x], sc_ref.at[0, 2, px], x_send, x_recv, x_peer)
        yc = remote(a_ref.at[py, x], sc_ref.at[1, 1, py], y_send, y_recv, y_peer)
        xc.start()
        yc.start()
        xc.wait()
        yc.wait()


def zero_kernel(token_ref, c_ref, done_ref, zbuf, sem):
    zbuf[...] = jnp.zeros_like(zbuf)
    done_ref[...] = jnp.zeros_like(done_ref)
    copies = []
    for s in range(2):
        for i in range(NC):
            for j in range(i + 1, NC):
                copies.append(pltpu.make_async_copy(zbuf, c_ref.at[chunk(i), s, :, pl.ds(j * TILE, TILE)], sem))
            for q in range(1, CH):
                copies.append(pltpu.make_async_copy(
                    zbuf.at[pl.ds(0, q), :, pl.ds(0, BLOCK)],
                    c_ref.at[pl.ds(i * CH, q), s, :, pl.ds((i * CH + q) * BLOCK, BLOCK)], sem))
    for cp in copies:
        cp.start()
    for cp in copies:
        cp.wait()


def gather_kernel(a_ref, sc_in, token_ref, sc_ref, o_ref, t_ref, yb, yr, join, lsem, d_send, d_recv, x_send, x_recv, r_send, r_recv,
                  y_send, y_recv, b_send, b_recv, q_send, q_recv, u_send, u_recv, v_send, v_recv):
    y, x, k, col = positions()
    late = k != y
    early = k == y
    side = jnp.where(late, 1, 0)
    partner = (0, y, 2 * x + 1 - k)
    x_peer = (0, y, 2 * (1 - x) + k)
    y_early = (0, 1 - y, 2 * x + 1 - y)
    y_late = (0, 1 - y, 2 * x + y)
    tx, ty = pl.ds(NAX, NM - NAX), pl.ds(NAY, NM - NAY)

    def x_copy(n):
        if n < NC:
            return remote(a_ref.at[chunk(n), 1 - x], sc_ref.at[0, 2, chunk(n)], x_send.at[n], x_recv.at[n], x_peer)
        part = pl.ds(*O_PARTS[n - NC])
        return remote(a_ref.at[part, x], o_ref.at[2, part], x_send.at[n], x_recv.at[n], x_peer)

    def relay_copy(n):
        if n < NC:
            return s_relay(n)
        part = pl.ds(*O_PARTS[n - NC])
        return remote(o_ref.at[2, part], o_ref.at[3, part], r_send.at[n], r_recv.at[n], partner)

    def y_copy(s, c):
        return remote(sc_ref.at[0, 2, chunk(c)], sc_ref.at[1, 2 + s, chunk(c)], y_send.at[c], y_recv.at[s, c], y_late)

    def s_relay(c):
        return remote(sc_ref.at[0, 2, chunk(c)], sc_ref.at[0, 3, chunk(c)], r_send.at[c], r_recv.at[c], partner)

    def s_copy(c):
        return remote(a_ref.at[chunk(c), x], sc_ref.at[0, 1, chunk(c)], d_send.at[c], d_recv.at[c], partner)

    def yb_relay(c):
        return remote(yb.at[chunk(c)], sc_ref.at[1, 0, chunk(c)], b_send.at[1 + c], b_recv.at[1 + c], partner)

    def yr_copy(c):
        return remote(sc_ref.at[0, 2, chunk(c)], yr.at[chunk(c)], q_send.at[c], q_recv.at[c], y_early)

    def yr_relay(c):
        return remote(yr.at[chunk(c)], sc_ref.at[1, 2, chunk(c)], y_send.at[c], y_recv.at[0, c], partner)

    yb_copy = remote(a_ref.at[:, x], yb, b_send.at[0], b_recv.at[0], y_early)
    x_tail = remote(a_ref.at[tx, 1 - x], sc_ref.at[0, 2, tx], v_send, v_recv, x_peer)
    u_copy = remote(a_ref.at[ty, x], sc_ref.at[1, 1, ty], u_send, u_recv, y_late)
    o_copy = remote(a_ref.at[:, 1 - x], o_ref.at[1], d_send.at[NC], d_recv.at[NC], partner)
    l_copies = [pltpu.make_async_copy(a_ref.at[:, x], sc_ref.at[0, 0], lsem.at[0]),
                pltpu.make_async_copy(a_ref.at[:, 1 - x], o_ref.at[0], lsem.at[1])]
    for cp in l_copies:
        cp.start()
    barrier = pltpu.get_barrier_semaphore()

    @pl.when(early)
    def _():
        signal(barrier, (x_peer, y_early, partner, y_late))
        pl.semaphore_wait(barrier, 2)
        for n in range(NX):
            x_copy(n).start()
        yb_copy.start()
        for c in range(NR):
            x_copy(c).wait_recv()
            yr_copy(c).start()
        pl.semaphore_wait(join, 2)
        for c in range(NC):
            if c >= NR:
                x_copy(c).wait_recv()
            s_copy(c).start()
            relay_copy(c).start()
            if c == 0:
                yb_copy.wait_recv()
                yb_relay(c).start()
        for c in range(NC):
            if c < NR:
                yr_copy(c).wait_recv()
                yr_relay(c).start()
            if c + 1 < NC:
                yb_relay(c + 1).start()
        o_copy.start()

    @pl.when(late)
    def _():
        signal(barrier, (x_peer, y_late))
        pl.semaphore_wait(barrier, 4)
        signal(join, (partner, y_early))
        x_tail.start()
        for n in range(NC, NX):
            x_copy(n).start()
        for c in range(NC - 1):
            y_copy(1, c).start()
        u_copy.start()
        for c in range(NC):
            s_copy(c).start()
            if c < NC - 1:
                relay_copy(c).start()
        o_copy.start()
        x_tail.wait_recv()
        relay_copy(NC - 1).start()
        y_copy(1, NC - 1).start()

    def rows_ready(i):
        s_copy(i).wait_recv()
        s_relay(i).wait_recv()

    def o_step(n):
        x_copy(NC + n).wait_recv()
        relay_copy(NC + n).start()

    l_copies[0].wait()
    rows_ready(0)
    row_blk = 2 * x + y
    for c in range(NC):
        if c < NC - 1:
            o_step(c)
        else:
            o_step(len(O_PARTS) - 1)

        @pl.when(early)
        def _():
            if c < NC - NR:
                y_copy(0, NR + c).start()

        @pl.when(late)
        def _():
            yb_relay(c).wait_recv()
            if c == NC - 1:
                u_copy.wait_recv()
            for s in range(2):
                y_copy(s, c).wait_recv()

        if c < NC - 1:
            base = NOW.index((c, c))
            diag_tile(t_ref.at[base], sc_ref, (0,), sc_ref, (side,), c, row_blk, col)

            def body(i, _):
                if c == 0:
                    rows_ready(i)
                full_tile(t_ref.at[base + i - c], sc_ref, (0,), i, sc_ref, (side,), c)
                return 0
            lax.fori_loop(c + 1, NC, body, 0)
        if c == 1:
            l_copies[1].wait()
            o_copy.wait_recv()
            relay_copy(NC).wait_recv()
        if c == 2:
            o_step(c + 1)
        if c in (1, 2):
            i, j = EXTRA[c - 1]
            full_tile(t_ref.at[len(NOW) + c - 1], o_ref, (), i, sc_ref, (side,), j)

    for n in range(1, len(O_PARTS)):
        relay_copy(NC + n).wait_recv()
    for n in range(NX):
        relay_copy(n).wait_send()
    for n in range(NC, NX):
        x_copy(n).wait_send()
    for c in range(NC):
        s_copy(c).wait_send()
        y_copy(0, c).wait_send()
    o_copy.wait_send()

    @pl.when(late)
    def _():
        u_copy.wait_send()
        x_tail.wait_send()

    @pl.when(early)
    def _():
        for n in range(NC):
            x_copy(n).wait_send()
        for c in range(NR):
            yr_copy(c).wait_send()
        yb_copy.wait_send()
        for c in range(NC):
            yb_relay(c).wait_send()


def lookup(n, values):
    out = jnp.int32(values[-1])
    for m in range(len(values) - 2, -1, -1):
        out = jnp.where(n == m, jnp.int32(values[m]), out)
    return out


def write_kernel(sc_ref, o_ref, t_ref, c_in, c_ref, obuf, tsem, osem):
    y, x, k, col = positions()
    side = jnp.where(k != y, 1, 0)

    def pick(n, values):
        return [lookup(n, column) for column in zip(*values)]

    def put(src, i, j, s, sem, act):
        @pl.when(i != j)
        def _():
            act(pltpu.make_async_copy(src, c_ref.at[pl.ds(i * CH, CH), s, :, pl.ds(pl.multiple_of(j * TILE, TILE), TILE)], sem))

        @pl.when(i == j)
        def _():
            for q in range(CH):
                act(pltpu.make_async_copy(
                    src.at[pl.ds(q, CH - q), :, pl.ds(q * BLOCK, BLOCK)],
                    c_ref.at[pl.ds(i * CH + q, CH - q), s, :, pl.ds(pl.multiple_of(j * TILE + q * BLOCK, BLOCK), BLOCK)], sem))

    def put_panel(n, act):
        i, j, cls = pick(n, PANELS)
        put(t_ref.at[n], i, j, jnp.where(cls == 0, x, 1 - x), tsem, act)

    def put_job(n, act):
        i, j = pick(n, LATER)
        b = lax.rem(n, NBUF)
        put(obuf.at[b], i, j, 1 - x, osem.at[b], act)

    def start(cp):
        cp.start()

    def wait(cp):
        cp.wait()

    for n in range(LEAD):
        put_panel(jnp.int32(n), start)

    def body(n, _):
        i, j = pick(n, LATER)
        b = lax.rem(n, NBUF)

        @pl.when(n >= NBUF)
        def _():
            put_job(n - NBUF, wait)

        @pl.when(i != j)
        def _():
            full_tile(obuf.at[b], o_ref, (), i, sc_ref, (side,), j)

        @pl.when(i == j)
        def _():
            diag_tile(obuf.at[b], o_ref, (), sc_ref, (side,), j, 2 * (1 - x) + y, col)
        put_job(n, start)

        @pl.when(n + LEAD < len(PANELS))
        def _():
            put_panel(jnp.minimum(n + LEAD, len(PANELS) - 1), start)
        return 0

    lax.fori_loop(0, len(LATER), body, 0)
    last_slot = len(LATER) % NBUF
    put_job(jnp.int32(len(LATER) - NBUF), wait)
    diag_tile(obuf.at[last_slot], sc_ref, (0,), sc_ref, (side,), LAST[1], 2 * x + y, col)
    put(obuf.at[last_slot], jnp.int32(LAST[0]), jnp.int32(LAST[1]), x, osem.at[last_slot], start)

    def drain(n, _):
        put_panel(n, wait)

        @pl.when(jnp.logical_and(n > len(LATER) - NBUF, n < len(LATER)))
        def _():
            put_job(jnp.minimum(n, len(LATER) - 1), wait)
        return 0
    lax.fori_loop(0, len(PANELS), drain, 0)
    put(obuf.at[last_slot], jnp.int32(LAST[0]), jnp.int32(LAST[1]), x, osem.at[last_slot], wait)


def solution(mesh):
    def local_fn(a):
        a4 = pltpu.with_memory_space_constraint(a.reshape(NM, 2, BLOCK, PIECE), pltpu.HBM)
        any_spec = pl.BlockSpec(memory_space=pl.ANY)
        hbm = pl.BlockSpec(memory_space=pltpu.HBM)
        vmem = pl.BlockSpec(memory_space=pltpu.VMEM)
        dma = pltpu.SemaphoreType.DMA
        half_flops = 136 * 2 * BLOCK * BLOCK * K_DIM
        panels = pltpu.VMEM((2, PIECES, NM, BLOCK, PIECE), jnp.bfloat16)
        token = jax.ShapeDtypeStruct((8, 128), jnp.float32)
        sc, first = pl.pallas_call(
            first_kernel,
            out_shape=[panels, token],
            in_specs=[hbm],
            out_specs=[vmem, vmem],
            scratch_shapes=[dma(())] * 4,
            compiler_params=pltpu.CompilerParams(collective_id=0, has_side_effects=True, vmem_limit_bytes=2 * 1024 * 1024),
        )(a4)
        c, zeroed = pl.pallas_call(
            zero_kernel,
            out_shape=[jax.ShapeDtypeStruct((NM, 2, BLOCK, NM * BLOCK), jnp.bfloat16), token],
            in_specs=[any_spec],
            out_specs=[any_spec, vmem],
            scratch_shapes=[pltpu.VMEM((CH, BLOCK, TILE), jnp.bfloat16), dma(())],
            compiler_params=pltpu.CompilerParams(vmem_limit_bytes=4 * 1024 * 1024),
            cost_estimate=pl.CostEstimate(flops=half_flops, bytes_accessed=30 << 20, transcendentals=0),
        )(first)
        sc, o, t = pl.pallas_call(
            gather_kernel,
            out_shape=[panels,
                       pltpu.VMEM((PIECES, NM, BLOCK, PIECE), jnp.bfloat16),
                       pltpu.VMEM((len(PANELS), CH, BLOCK, TILE), jnp.bfloat16)],
            in_specs=[hbm, vmem, any_spec],
            out_specs=[vmem] * 3,
            input_output_aliases={1: 0},
            scratch_shapes=[pltpu.VMEM((NM, BLOCK, PIECE), jnp.bfloat16), pltpu.VMEM((NR * CH, BLOCK, PIECE), jnp.bfloat16),
                            pltpu.SemaphoreType.REGULAR,
                            dma((2,)), dma((NC + 1,)), dma((NC + 1,)), dma((NX,)), dma((NX,)), dma((NX,)), dma((NX,)),
                            dma((NC,)), dma((2, NC)), dma((NC + 1,)), dma((NC + 1,)), dma((NR,)), dma((NR,))] + [dma(())] * 4,
            compiler_params=pltpu.CompilerParams(collective_id=1, has_side_effects=True, vmem_limit_bytes=8 * 1024 * 1024),
            cost_estimate=pl.CostEstimate(flops=half_flops, bytes_accessed=2 << 20, transcendentals=0),
        )(a4, sc, zeroed)
        c = pl.pallas_call(
            write_kernel,
            out_shape=jax.ShapeDtypeStruct((NM, 2, BLOCK, NM * BLOCK), jnp.bfloat16),
            in_specs=[vmem] * 3 + [any_spec],
            out_specs=any_spec,
            input_output_aliases={3: 0},
            scratch_shapes=[pltpu.VMEM((NBUF, CH, BLOCK, TILE), jnp.bfloat16), dma(()), dma((NBUF,))],
            compiler_params=pltpu.CompilerParams(vmem_limit_bytes=15 * 1024 * 1024),
            cost_estimate=pl.CostEstimate(flops=half_flops, bytes_accessed=34 << 20, transcendentals=0),
        )(sc, o, t, c)
        return c.reshape(2 * NM * BLOCK, NM * BLOCK)

    spec = P(('batch', 'row'), 'col')
    return jax.shard_map(local_fn, mesh=mesh, in_specs=(spec,), out_specs=spec, check_vma=False)
```

```python
import functools
import jax
import jax.numpy as jnp
from jax import lax
from jax.experimental import pallas as pl
from jax.experimental.pallas import tpu as pltpu
from jax.sharding import PartitionSpec as P

BLOCK = 256
K_DIM = 512
PIECE = 128
PIECES = K_DIM // PIECE
NM = 16
CH = 4
NC = NM // CH
NBUF = 5
LEAD = 4
TILE = CH * BLOCK
JOBS = [(i, j) for j in range(NC) for i in range(j, NC)]
LAST = (NC - 1, NC - 1)
NOW = [job for job in JOBS if job != LAST]
NAX, NAY = 15, 14
NR = 2
O_PARTS = ((12, 4), (0, 4), (4, 4), (8, 3), (11, 1))
NX = NC + len(O_PARTS)
EXTRA = [(3, 0), (3, 1)]
LATER = [job for job in JOBS if job not in EXTRA]
PANELS = [(i, j, 0) for i, j in NOW] + [(i, j, 1) for i, j in EXTRA]


def positions():
    y = lax.axis_index('row')
    col = lax.axis_index('col')
    return y, col // 2, col % 2, col


def chunk(c):
    return pl.ds(c * CH, CH)


def panel(ref, lead, first, count):
    parts = [ref[(*lead, p, pl.ds(first, count))].reshape(count * BLOCK, PIECE) for p in range(PIECES)]
    return jnp.concatenate(parts, axis=1)


def dot_t(rows, cols):
    return lax.dot_general(rows, cols, (((1,), (1,)), ((), ())), preferred_element_type=jnp.float32)


def full_tile(out, row_ref, row_lead, i, col_ref, col_lead, j):
    prod = dot_t(panel(row_ref, row_lead, i * CH, CH), panel(col_ref, col_lead, j * CH, CH))
    out[...] = prod.astype(jnp.bfloat16).reshape(CH, BLOCK, TILE)


def diag_tile(out, row_ref, row_lead, col_ref, col_lead, j, row_blk, col_blk):
    for q in range(CH):
        prod = dot_t(panel(row_ref, row_lead, j * CH + q, CH - q), panel(col_ref, col_lead, j * CH + q, 1))
        row_id = lax.broadcasted_iota(jnp.int32, (BLOCK, BLOCK), 0) + row_blk * BLOCK
        col_id = lax.broadcasted_iota(jnp.int32, (BLOCK, BLOCK), 1) + col_blk * BLOCK
        lanes = slice(q * BLOCK, (q + 1) * BLOCK)
        out[q, :, lanes] = jnp.where(row_id >= col_id, prod[:BLOCK], 0.0).astype(jnp.bfloat16)
        if q + 1 < CH:
            out[q + 1:, :, lanes] = prod[BLOCK:].astype(jnp.bfloat16).reshape(CH - q - 1, BLOCK, BLOCK)


MESH_ID = pl.DeviceIdType.MESH


def remote(src, dst, send, recv, dev):
    return pltpu.make_async_remote_copy(src, dst, send, recv, device_id=dev, device_id_type=MESH_ID)


def signal(sem, devices):
    for dev in devices:
        pl.semaphore_signal(sem, inc=1, device_id=dev, device_id_type=MESH_ID)


def first_kernel(a_ref, sc_ref, token_ref, x_send, x_recv, y_send, y_recv):
    y, x, k, _ = positions()
    token_ref[...] = jnp.zeros_like(token_ref)

    @pl.when(k != y)
    def _():
        x_peer = (0, y, 2 * (1 - x) + k)
        y_peer = (0, 1 - y, 2 * x + y)
        barrier = pltpu.get_barrier_semaphore()
        signal(barrier, (x_peer, y_peer))
        pl.semaphore_wait(barrier, 2)
        px, py = pl.ds(0, NAX), pl.ds(0, NAY)
        xc = remote(a_ref.at[px, 1 - x], sc_ref.at[0, 2, px], x_send, x_recv, x_peer)
        yc = remote(a_ref.at[py, x], sc_ref.at[1, 1, py], y_send, y_recv, y_peer)
        xc.start()
        yc.start()
        xc.wait()
        yc.wait()


def zero_kernel(token_ref, c_ref, done_ref, zbuf, sem):
    zbuf[...] = jnp.zeros_like(zbuf)
    done_ref[...] = jnp.zeros_like(done_ref)
    copies = []
    for s in range(2):
        for i in range(NC):
            for j in range(i + 1, NC):
                copies.append(pltpu.make_async_copy(zbuf, c_ref.at[chunk(i), s, :, pl.ds(j * TILE, TILE)], sem))
            for q in range(1, CH):
                copies.append(pltpu.make_async_copy(
                    zbuf.at[pl.ds(0, q), :, pl.ds(0, BLOCK)],
                    c_ref.at[pl.ds(i * CH, q), s, :, pl.ds((i * CH + q) * BLOCK, BLOCK)], sem))
    for cp in copies:
        cp.start()
    for cp in copies:
        cp.wait()


def gather_kernel(a_ref, sc_in, token_ref, sc_ref, o_ref, t_ref, yb, yr, join, lsem, d_send, d_recv, x_send, x_recv, r_send, r_recv,
                  y_send, y_recv, b_send, b_recv, q_send, q_recv, u_send, u_recv, v_send, v_recv):
    y, x, k, col = positions()
    late = k != y
    early = k == y
    side = jnp.where(late, 1, 0)
    partner = (0, y, 2 * x + 1 - k)
    x_peer = (0, y, 2 * (1 - x) + k)
    y_early = (0, 1 - y, 2 * x + 1 - y)
    y_late = (0, 1 - y, 2 * x + y)
    tx, ty = pl.ds(NAX, NM - NAX), pl.ds(NAY, NM - NAY)

    def x_copy(n):
        if n < NC:
            part = pl.ds(n * NM // 2, NM // 2)
            return remote(a_ref.at[part, 1 - x], sc_ref.at[0, 2, part], x_send.at[n], x_recv.at[n], x_peer)
        part = pl.ds(*O_PARTS[n - NC])
        return remote(a_ref.at[part, x], o_ref.at[2, part], x_send.at[n], x_recv.at[n], x_peer)

    def relay_copy(n):
        if n < NC:
            return s_relay(n)
        part = pl.ds(*O_PARTS[n - NC])
        return remote(o_ref.at[2, part], o_ref.at[3, part], r_send.at[n], r_recv.at[n], partner)

    def y_copy(s, c):
        return remote(sc_ref.at[0, 2, chunk(c)], sc_ref.at[1, 2 + s, chunk(c)], y_send.at[c], y_recv.at[s, c], y_late)

    def s_relay(c):
        return remote(sc_ref.at[0, 2, chunk(c)], sc_ref.at[0, 3, chunk(c)], r_send.at[c], r_recv.at[c], partner)

    def s_copy(c):
        return remote(a_ref.at[chunk(c), x], sc_ref.at[0, 1, chunk(c)], d_send.at[c], d_recv.at[c], partner)

    def yb_relay(c):
        return remote(yb.at[chunk(c)], sc_ref.at[1, 0, chunk(c)], b_send.at[1 + c], b_recv.at[1 + c], partner)

    def yr_relay(c):
        return remote(yr.at[chunk(c)], sc_ref.at[1, 2, chunk(c)], y_send.at[c], y_recv.at[0, c], partner)

    yr_part = pl.ds(0, NR * CH)
    yr_copy = remote(sc_ref.at[0, 2, yr_part], yr, q_send, q_recv, y_early)
    yb_copy = remote(a_ref.at[:, x], yb, b_send.at[0], b_recv.at[0], y_early)
    x_tail = remote(a_ref.at[tx, 1 - x], sc_ref.at[0, 2, tx], v_send, v_recv, x_peer)
    u_copy = remote(a_ref.at[ty, x], sc_ref.at[1, 1, ty], u_send, u_recv, y_late)
    o_copy = remote(a_ref.at[:, 1 - x], o_ref.at[1], d_send.at[NC], d_recv.at[NC], partner)
    l_copies = [pltpu.make_async_copy(a_ref.at[:, x], sc_ref.at[0, 0], lsem.at[0]),
                pltpu.make_async_copy(a_ref.at[:, 1 - x], o_ref.at[0], lsem.at[1])]
    for cp in l_copies:
        cp.start()
    barrier = pltpu.get_barrier_semaphore()

    @pl.when(early)
    def _():
        signal(barrier, (x_peer, y_early, partner, y_late))
        pl.semaphore_wait(barrier, 2)
        for n in (0, 1, *range(NC, NX)):
            x_copy(n).start()
        yb_copy.start()
        x_copy(0).wait_recv()
        yr_copy.start()
        pl.semaphore_wait(join, 2)
        for c in range(NC):
            if c == NR:
                x_copy(1).wait_recv()
            s_copy(c).start()
            relay_copy(c).start()
            if c == 0:
                yb_copy.wait_recv()
                yb_relay(c).start()
        for c in range(NC):
            if c == 0:
                yr_copy.wait_recv()
            if c < NR:
                yr_relay(c).start()
            if c + 1 < NC:
                yb_relay(c + 1).start()
        o_copy.start()

    @pl.when(late)
    def _():
        signal(barrier, (x_peer, y_late))
        pl.semaphore_wait(barrier, 4)
        signal(join, (partner, y_early))
        x_tail.start()
        for n in range(NC, NX):
            x_copy(n).start()
        for c in range(NC - 1):
            y_copy(1, c).start()
        u_copy.start()
        for c in range(NC):
            s_copy(c).start()
            if c < NC - 1:
                relay_copy(c).start()
        o_copy.start()
        x_tail.wait_recv()
        relay_copy(NC - 1).start()
        y_copy(1, NC - 1).start()

    def rows_ready(i):
        s_copy(i).wait_recv()
        s_relay(i).wait_recv()

    def o_step(n):
        x_copy(NC + n).wait_recv()
        relay_copy(NC + n).start()

    l_copies[0].wait()
    rows_ready(0)
    row_blk = 2 * x + y
    for c in range(NC):
        if c < NC - 1:
            o_step(c)
        else:
            o_step(len(O_PARTS) - 1)

        @pl.when(early)
        def _():
            if c < NC - NR:
                y_copy(0, NR + c).start()

        @pl.when(late)
        def _():
            yb_relay(c).wait_recv()
            if c == NC - 1:
                u_copy.wait_recv()
            for s in range(2):
                y_copy(s, c).wait_recv()

        if c < NC - 1:
            base = NOW.index((c, c))
            diag_tile(t_ref.at[base], sc_ref, (0,), sc_ref, (side,), c, row_blk, col)

            def body(i, _):
                if c == 0:
                    rows_ready(i)
                full_tile(t_ref.at[base + i - c], sc_ref, (0,), i, sc_ref, (side,), c)
                return 0
            lax.fori_loop(c + 1, NC, body, 0)
        if c == 1:
            l_copies[1].wait()
            o_copy.wait_recv()
            relay_copy(NC).wait_recv()
        if c == 2:
            o_step(c + 1)
        if c in (1, 2):
            i, j = EXTRA[c - 1]
            full_tile(t_ref.at[len(NOW) + c - 1], o_ref, (), i, sc_ref, (side,), j)

    for n in range(1, len(O_PARTS)):
        relay_copy(NC + n).wait_recv()
    for n in range(NX):
        relay_copy(n).wait_send()
    for n in range(NC, NX):
        x_copy(n).wait_send()
    for c in range(NC):
        s_copy(c).wait_send()
        y_copy(0, c).wait_send()
    o_copy.wait_send()

    @pl.when(late)
    def _():
        u_copy.wait_send()
        x_tail.wait_send()

    @pl.when(early)
    def _():
        for n in range(2):
            x_copy(n).wait_send()
        yr_copy.wait_send()
        yb_copy.wait_send()
        for c in range(NC):
            yb_relay(c).wait_send()


def lookup(n, values):
    out = jnp.int32(values[-1])
    for m in range(len(values) - 2, -1, -1):
        out = jnp.where(n == m, jnp.int32(values[m]), out)
    return out


def write_kernel(sc_ref, o_ref, t_ref, c_in, c_ref, obuf, tsem, osem):
    y, x, k, col = positions()
    side = jnp.where(k != y, 1, 0)

    def pick(n, values):
        return [lookup(n, column) for column in zip(*values)]

    def put(src, i, j, s, sem, act):
        @pl.when(i != j)
        def _():
            act(pltpu.make_async_copy(src, c_ref.at[pl.ds(i * CH, CH), s, :, pl.ds(pl.multiple_of(j * TILE, TILE), TILE)], sem))

        @pl.when(i == j)
        def _():
            for q in range(CH):
                act(pltpu.make_async_copy(
                    src.at[pl.ds(q, CH - q), :, pl.ds(q * BLOCK, BLOCK)],
                    c_ref.at[pl.ds(i * CH + q, CH - q), s, :, pl.ds(pl.multiple_of(j * TILE + q * BLOCK, BLOCK), BLOCK)], sem))

    def put_panel(n, act):
        i, j, cls = pick(n, PANELS)
        put(t_ref.at[n], i, j, jnp.where(cls == 0, x, 1 - x), tsem, act)

    def put_job(n, act):
        i, j = pick(n, LATER)
        b = lax.rem(n, NBUF)
        put(obuf.at[b], i, j, 1 - x, osem.at[b], act)

    def start(cp):
        cp.start()

    def wait(cp):
        cp.wait()

    for n in range(LEAD):
        put_panel(jnp.int32(n), start)

    def body(n, _):
        i, j = pick(n, LATER)
        b = lax.rem(n, NBUF)

        @pl.when(n >= NBUF)
        def _():
            put_job(n - NBUF, wait)

        @pl.when(i != j)
        def _():
            full_tile(obuf.at[b], o_ref, (), i, sc_ref, (side,), j)

        @pl.when(i == j)
        def _():
            diag_tile(obuf.at[b], o_ref, (), sc_ref, (side,), j, 2 * (1 - x) + y, col)
        put_job(n, start)

        @pl.when(n + LEAD < len(PANELS))
        def _():
            put_panel(jnp.minimum(n + LEAD, len(PANELS) - 1), start)
        return 0

    lax.fori_loop(0, len(LATER), body, 0)
    last_slot = len(LATER) % NBUF
    put_job(jnp.int32(len(LATER) - NBUF), wait)
    diag_tile(obuf.at[last_slot], sc_ref, (0,), sc_ref, (side,), LAST[1], 2 * x + y, col)
    put(obuf.at[last_slot], jnp.int32(LAST[0]), jnp.int32(LAST[1]), x, osem.at[last_slot], start)

    def drain(n, _):
        put_panel(n, wait)

        @pl.when(jnp.logical_and(n > len(LATER) - NBUF, n < len(LATER)))
        def _():
            put_job(jnp.minimum(n, len(LATER) - 1), wait)
        return 0
    lax.fori_loop(0, len(PANELS), drain, 0)
    put(obuf.at[last_slot], jnp.int32(LAST[0]), jnp.int32(LAST[1]), x, osem.at[last_slot], wait)


def solution(mesh):
    def local_fn(a):
        a4 = pltpu.with_memory_space_constraint(a.reshape(NM, 2, BLOCK, PIECE), pltpu.HBM)
        any_spec = pl.BlockSpec(memory_space=pl.ANY)
        hbm = pl.BlockSpec(memory_space=pltpu.HBM)
        vmem = pl.BlockSpec(memory_space=pltpu.VMEM)
        dma = pltpu.SemaphoreType.DMA
        half_flops = 136 * 2 * BLOCK * BLOCK * K_DIM
        panels = pltpu.VMEM((2, PIECES, NM, BLOCK, PIECE), jnp.bfloat16)
        token = jax.ShapeDtypeStruct((8, 128), jnp.float32)
        sc, first = pl.pallas_call(
            first_kernel,
            out_shape=[panels, token],
            in_specs=[hbm],
            out_specs=[vmem, vmem],
            scratch_shapes=[dma(())] * 4,
            compiler_params=pltpu.CompilerParams(collective_id=0, has_side_effects=True, vmem_limit_bytes=2 * 1024 * 1024),
        )(a4)
        c, zeroed = pl.pallas_call(
            zero_kernel,
            out_shape=[jax.ShapeDtypeStruct((NM, 2, BLOCK, NM * BLOCK), jnp.bfloat16), token],
            in_specs=[any_spec],
            out_specs=[any_spec, vmem],
            scratch_shapes=[pltpu.VMEM((CH, BLOCK, TILE), jnp.bfloat16), dma(())],
            compiler_params=pltpu.CompilerParams(vmem_limit_bytes=4 * 1024 * 1024),
            cost_estimate=pl.CostEstimate(flops=half_flops, bytes_accessed=30 << 20, transcendentals=0),
        )(first)
        sc, o, t = pl.pallas_call(
            gather_kernel,
            out_shape=[panels,
                       pltpu.VMEM((PIECES, NM, BLOCK, PIECE), jnp.bfloat16),
                       pltpu.VMEM((len(PANELS), CH, BLOCK, TILE), jnp.bfloat16)],
            in_specs=[hbm, vmem, any_spec],
            out_specs=[vmem] * 3,
            input_output_aliases={1: 0},
            scratch_shapes=[pltpu.VMEM((NM, BLOCK, PIECE), jnp.bfloat16), pltpu.VMEM((NR * CH, BLOCK, PIECE), jnp.bfloat16),
                            pltpu.SemaphoreType.REGULAR,
                            dma((2,)), dma((NC + 1,)), dma((NC + 1,)), dma((NX,)), dma((NX,)), dma((NX,)), dma((NX,)),
                            dma((NC,)), dma((2, NC)), dma((NC + 1,)), dma((NC + 1,)), dma(()), dma(())] + [dma(())] * 4,
            compiler_params=pltpu.CompilerParams(collective_id=1, has_side_effects=True, vmem_limit_bytes=8 * 1024 * 1024),
            cost_estimate=pl.CostEstimate(flops=half_flops, bytes_accessed=2 << 20, transcendentals=0),
        )(a4, sc, zeroed)
        c = pl.pallas_call(
            write_kernel,
            out_shape=jax.ShapeDtypeStruct((NM, 2, BLOCK, NM * BLOCK), jnp.bfloat16),
            in_specs=[vmem] * 3 + [any_spec],
            out_specs=any_spec,
            input_output_aliases={3: 0},
            scratch_shapes=[pltpu.VMEM((NBUF, CH, BLOCK, TILE), jnp.bfloat16), dma(()), dma((NBUF,))],
            compiler_params=pltpu.CompilerParams(vmem_limit_bytes=15 * 1024 * 1024),
            cost_estimate=pl.CostEstimate(flops=half_flops, bytes_accessed=34 << 20, transcendentals=0),
        )(sc, o, t, c)
        return c.reshape(2 * NM * BLOCK, NM * BLOCK)

    spec = P(('batch', 'row'), 'col')
    return jax.shard_map(local_fn, mesh=mesh, in_specs=(spec,), out_specs=spec, check_vma=False)
```

```python
import functools
import jax
import jax.numpy as jnp
from jax import lax
from jax.experimental import pallas as pl
from jax.experimental.pallas import tpu as pltpu
from jax.sharding import PartitionSpec as P

BLOCK = 256
K_DIM = 512
PIECE = 128
PIECES = K_DIM // PIECE
NM = 16
CH = 4
NC = NM // CH
NBUF = 5
LEAD = 4
TILE = CH * BLOCK
JOBS = [(i, j) for j in range(NC) for i in range(j, NC)]
LAST = (NC - 1, NC - 1)
NOW = [job for job in JOBS if job != LAST]
NAX, NAY = 15, 15
NR = 2
O_PARTS = ((12, 4), (0, 4), (4, 4), (8, 3), (11, 1))
NX = NC + len(O_PARTS)
EXTRA = [(3, 0), (3, 1)]
LATER = [job for job in JOBS if job not in EXTRA]
PANELS = [(i, j, 0) for i, j in NOW] + [(i, j, 1) for i, j in EXTRA]


def positions():
    y = lax.axis_index('row')
    col = lax.axis_index('col')
    return y, col // 2, col % 2, col


def chunk(c):
    return pl.ds(c * CH, CH)


def panel(ref, lead, first, count):
    parts = [ref[(*lead, p, pl.ds(first, count))].reshape(count * BLOCK, PIECE) for p in range(PIECES)]
    return jnp.concatenate(parts, axis=1)


def dot_t(rows, cols):
    return lax.dot_general(rows, cols, (((1,), (1,)), ((), ())), preferred_element_type=jnp.float32)


def full_tile(out, row_ref, row_lead, i, col_ref, col_lead, j):
    prod = dot_t(panel(row_ref, row_lead, i * CH, CH), panel(col_ref, col_lead, j * CH, CH))
    out[...] = prod.astype(jnp.bfloat16).reshape(CH, BLOCK, TILE)


def diag_tile(out, row_ref, row_lead, col_ref, col_lead, j, row_blk, col_blk):
    for q in range(CH):
        prod = dot_t(panel(row_ref, row_lead, j * CH + q, CH - q), panel(col_ref, col_lead, j * CH + q, 1))
        row_id = lax.broadcasted_iota(jnp.int32, (BLOCK, BLOCK), 0) + row_blk * BLOCK
        col_id = lax.broadcasted_iota(jnp.int32, (BLOCK, BLOCK), 1) + col_blk * BLOCK
        lanes = slice(q * BLOCK, (q + 1) * BLOCK)
        out[q, :, lanes] = jnp.where(row_id >= col_id, prod[:BLOCK], 0.0).astype(jnp.bfloat16)
        if q + 1 < CH:
            out[q + 1:, :, lanes] = prod[BLOCK:].astype(jnp.bfloat16).reshape(CH - q - 1, BLOCK, BLOCK)


MESH_ID = pl.DeviceIdType.MESH


def remote(src, dst, send, recv, dev):
    return pltpu.make_async_remote_copy(src, dst, send, recv, device_id=dev, device_id_type=MESH_ID)


def signal(sem, devices):
    for dev in devices:
        pl.semaphore_signal(sem, inc=1, device_id=dev, device_id_type=MESH_ID)


def first_kernel(a_ref, sc_ref, token_ref, x_send, x_recv, y_send, y_recv):
    y, x, k, _ = positions()
    token_ref[...] = jnp.zeros_like(token_ref)

    @pl.when(k != y)
    def _():
        x_peer = (0, y, 2 * (1 - x) + k)
        y_peer = (0, 1 - y, 2 * x + y)
        barrier = pltpu.get_barrier_semaphore()
        signal(barrier, (x_peer, y_peer))
        pl.semaphore_wait(barrier, 2)
        px, py = pl.ds(0, NAX), pl.ds(0, NAY)
        xc = remote(a_ref.at[px, 1 - x], sc_ref.at[0, 2, px], x_send, x_recv, x_peer)
        yc = remote(a_ref.at[py, x], sc_ref.at[1, 1, py], y_send, y_recv, y_peer)
        xc.start()
        yc.start()
        xc.wait()
        yc.wait()


def zero_kernel(token_ref, a_ref, sc_in, c_ref, done_ref, sc_ref, o_ref, zbuf, sem, lsem):
    _, x, _, _ = positions()
    loads = [pltpu.make_async_copy(a_ref.at[:, 1 - x], o_ref.at[0], lsem),
             pltpu.make_async_copy(a_ref.at[:, x], sc_ref.at[0, 0], lsem)]
    for cp in loads:
        cp.start()
    zbuf[...] = jnp.zeros_like(zbuf)
    done_ref[...] = jnp.zeros_like(done_ref)
    copies = []
    for s in range(2):
        for i in range(NC):
            for j in range(i + 1, NC):
                copies.append(pltpu.make_async_copy(zbuf, c_ref.at[chunk(i), s, :, pl.ds(j * TILE, TILE)], sem))
            for q in range(1, CH):
                copies.append(pltpu.make_async_copy(
                    zbuf.at[pl.ds(0, q), :, pl.ds(0, BLOCK)],
                    c_ref.at[pl.ds(i * CH, q), s, :, pl.ds((i * CH + q) * BLOCK, BLOCK)], sem))
    for cp in copies:
        cp.start()
    for cp in copies + loads:
        cp.wait()


def gather_kernel(sc_in, o_in, token_ref, sc_ref, o_ref, t_ref, yb, yr, join, d_send, d_recv, x_send, x_recv, r_send, r_recv,
                  y_send, y_recv, b_send, b_recv, q_send, q_recv, u_send, u_recv, v_send, v_recv):
    y, x, k, col = positions()
    late = k != y
    early = k == y
    side = jnp.where(late, 1, 0)
    partner = (0, y, 2 * x + 1 - k)
    x_peer = (0, y, 2 * (1 - x) + k)
    y_early = (0, 1 - y, 2 * x + 1 - y)
    y_late = (0, 1 - y, 2 * x + y)
    tx, ty = pl.ds(NAX, NM - NAX), pl.ds(NAY, NM - NAY)

    def x_copy(n):
        if n < NC:
            part = pl.ds(n * NM // 2, NM // 2)
            return remote(o_ref.at[0, part], sc_ref.at[0, 2, part], x_send.at[n], x_recv.at[n], x_peer)
        part = pl.ds(*O_PARTS[n - NC])
        return remote(sc_ref.at[0, 0, part], o_ref.at[2, part], x_send.at[n], x_recv.at[n], x_peer)

    def relay_copy(n):
        if n < NC:
            return s_relay(n)
        part = pl.ds(*O_PARTS[n - NC])
        return remote(o_ref.at[2, part], o_ref.at[3, part], r_send.at[n], r_recv.at[n], partner)

    def y_copy(s, c):
        return remote(sc_ref.at[0, 2, chunk(c)], sc_ref.at[1, 2 + s, chunk(c)], y_send.at[c], y_recv.at[s, c], y_late)

    def s_relay(c):
        return remote(sc_ref.at[0, 2, chunk(c)], sc_ref.at[0, 3, chunk(c)], r_send.at[c], r_recv.at[c], partner)

    def s_copy(c):
        return remote(sc_ref.at[0, 0, chunk(c)], sc_ref.at[0, 1, chunk(c)], d_send.at[c], d_recv.at[c], partner)

    def yb_relay(c):
        return remote(yb.at[chunk(c)], sc_ref.at[1, 0, chunk(c)], b_send.at[1 + c], b_recv.at[1 + c], partner)

    def yr_relay(c):
        return remote(yr.at[chunk(c)], sc_ref.at[1, 2, chunk(c)], y_send.at[c], y_recv.at[0, c], partner)

    yr_part = pl.ds(0, NR * CH)
    yr_copy = remote(sc_ref.at[0, 2, yr_part], yr, q_send, q_recv, y_early)
    yb_copy = remote(sc_ref.at[0, 0], yb, b_send.at[0], b_recv.at[0], y_early)
    x_tail = remote(o_ref.at[0, tx], sc_ref.at[0, 2, tx], v_send, v_recv, x_peer)
    u_copy = remote(sc_ref.at[0, 0, ty], sc_ref.at[1, 1, ty], u_send, u_recv, y_late)
    o_copy = remote(o_ref.at[0], o_ref.at[1], d_send.at[NC], d_recv.at[NC], partner)
    barrier = pltpu.get_barrier_semaphore()

    @pl.when(early)
    def _():
        signal(barrier, (x_peer, y_early, partner, y_late))
        pl.semaphore_wait(barrier, 2)
        for n in (0, 1, *range(NC, NX)):
            x_copy(n).start()
        yb_copy.start()
        x_copy(0).wait_recv()
        yr_copy.start()
        pl.semaphore_wait(join, 2)
        for c in range(NC):
            if c == NR:
                x_copy(1).wait_recv()
            s_copy(c).start()
            relay_copy(c).start()
            if c == 0:
                yb_copy.wait_recv()
                yb_relay(c).start()
        for c in range(NC):
            if c == 0:
                yr_copy.wait_recv()
            if c < NR:
                yr_relay(c).start()
            if c + 1 < NC:
                yb_relay(c + 1).start()
        o_copy.start()

    @pl.when(late)
    def _():
        signal(barrier, (x_peer, y_late))
        pl.semaphore_wait(barrier, 4)
        signal(join, (partner, y_early))
        x_tail.start()
        for n in range(NC, NX):
            x_copy(n).start()
        for c in range(NC - 1):
            y_copy(1, c).start()
        u_copy.start()
        for c in range(NC):
            s_copy(c).start()
            if c < NC - 1:
                relay_copy(c).start()
        o_copy.start()
        x_tail.wait_recv()
        relay_copy(NC - 1).start()
        y_copy(1, NC - 1).start()

    def rows_ready(i):
        s_copy(i).wait_recv()
        s_relay(i).wait_recv()

    def o_step(n):
        x_copy(NC + n).wait_recv()
        relay_copy(NC + n).start()

    rows_ready(0)
    row_blk = 2 * x + y
    for c in range(NC):
        if c < NC - 1:
            o_step(c)
        else:
            o_step(len(O_PARTS) - 1)

        @pl.when(early)
        def _():
            if c < NC - NR:
                y_copy(0, NR + c).start()

        @pl.when(late)
        def _():
            yb_relay(c).wait_recv()
            if c == NC - 1:
                u_copy.wait_recv()
            for s in range(2):
                y_copy(s, c).wait_recv()

        if c < NC - 1:
            base = NOW.index((c, c))
            diag_tile(t_ref.at[base], sc_ref, (0,), sc_ref, (side,), c, row_blk, col)

            def body(i, _):
                if c == 0:
                    rows_ready(i)
                full_tile(t_ref.at[base + i - c], sc_ref, (0,), i, sc_ref, (side,), c)
                return 0
            lax.fori_loop(c + 1, NC, body, 0)
        if c == 1:
            o_copy.wait_recv()
            relay_copy(NC).wait_recv()
        if c == 2:
            o_step(c + 1)
        if c in (1, 2):
            i, j = EXTRA[c - 1]
            full_tile(t_ref.at[len(NOW) + c - 1], o_ref, (), i, sc_ref, (side,), j)

    for n in range(1, len(O_PARTS)):
        relay_copy(NC + n).wait_recv()
    for n in range(NX):
        relay_copy(n).wait_send()
    for n in range(NC, NX):
        x_copy(n).wait_send()
    for c in range(NC):
        s_copy(c).wait_send()
        y_copy(0, c).wait_send()
    o_copy.wait_send()

    @pl.when(late)
    def _():
        u_copy.wait_send()
        x_tail.wait_send()

    @pl.when(early)
    def _():
        for n in range(2):
            x_copy(n).wait_send()
        yr_copy.wait_send()
        yb_copy.wait_send()
        for c in range(NC):
            yb_relay(c).wait_send()


def lookup(n, values):
    out = jnp.int32(values[-1])
    for m in range(len(values) - 2, -1, -1):
        out = jnp.where(n == m, jnp.int32(values[m]), out)
    return out


def write_kernel(sc_ref, o_ref, t_ref, c_in, c_ref, obuf, tsem, osem):
    y, x, k, col = positions()
    side = jnp.where(k != y, 1, 0)

    def pick(n, values):
        return [lookup(n, column) for column in zip(*values)]

    def put(src, i, j, s, sem, act):
        @pl.when(i != j)
        def _():
            act(pltpu.make_async_copy(src, c_ref.at[pl.ds(i * CH, CH), s, :, pl.ds(pl.multiple_of(j * TILE, TILE), TILE)], sem))

        @pl.when(i == j)
        def _():
            for q in range(CH):
                act(pltpu.make_async_copy(
                    src.at[pl.ds(q, CH - q), :, pl.ds(q * BLOCK, BLOCK)],
                    c_ref.at[pl.ds(i * CH + q, CH - q), s, :, pl.ds(pl.multiple_of(j * TILE + q * BLOCK, BLOCK), BLOCK)], sem))

    def put_panel(n, act):
        i, j, cls = pick(n, PANELS)
        put(t_ref.at[n], i, j, jnp.where(cls == 0, x, 1 - x), tsem, act)

    def put_job(n, act):
        i, j = pick(n, LATER)
        b = lax.rem(n, NBUF)
        put(obuf.at[b], i, j, 1 - x, osem.at[b], act)

    def start(cp):
        cp.start()

    def wait(cp):
        cp.wait()

    for n in range(LEAD):
        put_panel(jnp.int32(n), start)

    def body(n, _):
        i, j = pick(n, LATER)
        b = lax.rem(n, NBUF)

        @pl.when(n >= NBUF)
        def _():
            put_job(n - NBUF, wait)

        @pl.when(i != j)
        def _():
            full_tile(obuf.at[b], o_ref, (), i, sc_ref, (side,), j)

        @pl.when(i == j)
        def _():
            diag_tile(obuf.at[b], o_ref, (), sc_ref, (side,), j, 2 * (1 - x) + y, col)
        put_job(n, start)

        @pl.when(n + LEAD < len(PANELS))
        def _():
            put_panel(jnp.minimum(n + LEAD, len(PANELS) - 1), start)
        return 0

    lax.fori_loop(0, len(LATER), body, 0)
    last_slot = len(LATER) % NBUF
    put_job(jnp.int32(len(LATER) - NBUF), wait)
    diag_tile(obuf.at[last_slot], sc_ref, (0,), sc_ref, (side,), LAST[1], 2 * x + y, col)
    put(obuf.at[last_slot], jnp.int32(LAST[0]), jnp.int32(LAST[1]), x, osem.at[last_slot], start)

    def drain(n, _):
        put_panel(n, wait)

        @pl.when(jnp.logical_and(n > len(LATER) - NBUF, n < len(LATER)))
        def _():
            put_job(jnp.minimum(n, len(LATER) - 1), wait)
        return 0
    lax.fori_loop(0, len(PANELS), drain, 0)
    put(obuf.at[last_slot], jnp.int32(LAST[0]), jnp.int32(LAST[1]), x, osem.at[last_slot], wait)


def solution(mesh):
    def local_fn(a):
        a4 = pltpu.with_memory_space_constraint(a.reshape(NM, 2, BLOCK, PIECE), pltpu.HBM)
        any_spec = pl.BlockSpec(memory_space=pl.ANY)
        hbm = pl.BlockSpec(memory_space=pltpu.HBM)
        vmem = pl.BlockSpec(memory_space=pltpu.VMEM)
        dma = pltpu.SemaphoreType.DMA
        half_flops = 136 * 2 * BLOCK * BLOCK * K_DIM
        panels = pltpu.VMEM((2, PIECES, NM, BLOCK, PIECE), jnp.bfloat16)
        token = jax.ShapeDtypeStruct((8, 128), jnp.float32)
        sc, first = pl.pallas_call(
            first_kernel,
            out_shape=[panels, token],
            in_specs=[hbm],
            out_specs=[vmem, vmem],
            scratch_shapes=[dma(())] * 4,
            compiler_params=pltpu.CompilerParams(collective_id=0, has_side_effects=True, vmem_limit_bytes=2 * 1024 * 1024),
        )(a4)
        rest = pltpu.VMEM((PIECES, NM, BLOCK, PIECE), jnp.bfloat16)
        c, zeroed, sc, o = pl.pallas_call(
            zero_kernel,
            out_shape=[jax.ShapeDtypeStruct((NM, 2, BLOCK, NM * BLOCK), jnp.bfloat16), token, panels, rest],
            in_specs=[any_spec, hbm, vmem],
            out_specs=[any_spec, vmem, vmem, vmem],
            input_output_aliases={2: 2},
            scratch_shapes=[pltpu.VMEM((CH, BLOCK, TILE), jnp.bfloat16), dma(()), dma(())],
            compiler_params=pltpu.CompilerParams(vmem_limit_bytes=4 * 1024 * 1024),
            cost_estimate=pl.CostEstimate(flops=half_flops, bytes_accessed=30 << 20, transcendentals=0),
        )(first, a4, sc)
        sc, o, t = pl.pallas_call(
            gather_kernel,
            out_shape=[panels, rest,
                       pltpu.VMEM((len(PANELS), CH, BLOCK, TILE), jnp.bfloat16)],
            in_specs=[vmem, vmem, any_spec],
            out_specs=[vmem] * 3,
            input_output_aliases={0: 0, 1: 1},
            scratch_shapes=[pltpu.VMEM((NM, BLOCK, PIECE), jnp.bfloat16), pltpu.VMEM((NR * CH, BLOCK, PIECE), jnp.bfloat16),
                            pltpu.SemaphoreType.REGULAR,
                            dma((NC + 1,)), dma((NC + 1,)), dma((NX,)), dma((NX,)), dma((NX,)), dma((NX,)),
                            dma((NC,)), dma((2, NC)), dma((NC + 1,)), dma((NC + 1,)), dma(()), dma(())] + [dma(())] * 4,
            compiler_params=pltpu.CompilerParams(collective_id=1, has_side_effects=True, vmem_limit_bytes=8 * 1024 * 1024),
            cost_estimate=pl.CostEstimate(flops=half_flops, bytes_accessed=2 << 20, transcendentals=0),
        )(sc, o, zeroed)
        c = pl.pallas_call(
            write_kernel,
            out_shape=jax.ShapeDtypeStruct((NM, 2, BLOCK, NM * BLOCK), jnp.bfloat16),
            in_specs=[vmem] * 3 + [any_spec],
            out_specs=any_spec,
            input_output_aliases={3: 0},
            scratch_shapes=[pltpu.VMEM((NBUF, CH, BLOCK, TILE), jnp.bfloat16), dma(()), dma((NBUF,))],
            compiler_params=pltpu.CompilerParams(vmem_limit_bytes=15 * 1024 * 1024),
            cost_estimate=pl.CostEstimate(flops=half_flops, bytes_accessed=34 << 20, transcendentals=0),
        )(sc, o, t, c)
        return c.reshape(2 * NM * BLOCK, NM * BLOCK)

    spec = P(('batch', 'row'), 'col')
    return jax.shard_map(local_fn, mesh=mesh, in_specs=(spec,), out_specs=spec, check_vma=False)
```

```python
import functools
import jax
import jax.numpy as jnp
from jax import lax
from jax.experimental import pallas as pl
from jax.experimental.pallas import tpu as pltpu
from jax.sharding import PartitionSpec as P

BLOCK = 256
K_DIM = 512
PIECE = 128
PIECES = K_DIM // PIECE
NM = 16
CH = 4
NC = NM // CH
NBUF = 5
LEAD = 4
TILE = CH * BLOCK
JOBS = [(i, j) for j in range(NC) for i in range(j, NC)]
LAST = (NC - 1, NC - 1)
NOW = [job for job in JOBS if job != LAST]
NAX, NAY = 15, 15
NR = 2
O_PARTS = ((12, 4), (0, 4), (4, 4), (8, 3), (11, 1))
NX = NC + len(O_PARTS)
EXTRA = [(3, 0), (3, 1)]
LATER = [job for job in JOBS if job not in EXTRA]
PANELS = [(i, j, 0) for i, j in NOW] + [(i, j, 1) for i, j in EXTRA]


def positions():
    y = lax.axis_index('row')
    col = lax.axis_index('col')
    return y, col // 2, col % 2, col


def chunk(c):
    return pl.ds(c * CH, CH)


def panel(ref, lead, first, count):
    parts = [ref[(*lead, p, pl.ds(first, count))].reshape(count * BLOCK, PIECE) for p in range(PIECES)]
    return jnp.concatenate(parts, axis=1)


def dot_t(rows, cols):
    return lax.dot_general(rows, cols, (((1,), (1,)), ((), ())), preferred_element_type=jnp.float32)


def full_tile(out, row_ref, row_lead, i, col_ref, col_lead, j):
    prod = dot_t(panel(row_ref, row_lead, i * CH, CH), panel(col_ref, col_lead, j * CH, CH))
    out[...] = prod.astype(jnp.bfloat16).reshape(CH, BLOCK, TILE)


def diag_tile(out, row_ref, row_lead, col_ref, col_lead, j, row_blk, col_blk):
    for q in range(CH):
        prod = dot_t(panel(row_ref, row_lead, j * CH + q, CH - q), panel(col_ref, col_lead, j * CH + q, 1))
        row_id = lax.broadcasted_iota(jnp.int32, (BLOCK, BLOCK), 0) + row_blk * BLOCK
        col_id = lax.broadcasted_iota(jnp.int32, (BLOCK, BLOCK), 1) + col_blk * BLOCK
        lanes = slice(q * BLOCK, (q + 1) * BLOCK)
        out[q, :, lanes] = jnp.where(row_id >= col_id, prod[:BLOCK], 0.0).astype(jnp.bfloat16)
        if q + 1 < CH:
            out[q + 1:, :, lanes] = prod[BLOCK:].astype(jnp.bfloat16).reshape(CH - q - 1, BLOCK, BLOCK)


MESH_ID = pl.DeviceIdType.MESH


def remote(src, dst, send, recv, dev):
    return pltpu.make_async_remote_copy(src, dst, send, recv, device_id=dev, device_id_type=MESH_ID)


def signal(sem, devices):
    for dev in devices:
        pl.semaphore_signal(sem, inc=1, device_id=dev, device_id_type=MESH_ID)


def first_kernel(a_ref, sc_ref, token_ref, x_send, x_recv, y_send, y_recv):
    y, x, k, _ = positions()
    token_ref[...] = jnp.zeros_like(token_ref)

    @pl.when(k != y)
    def _():
        x_peer = (0, y, 2 * (1 - x) + k)
        y_peer = (0, 1 - y, 2 * x + y)
        barrier = pltpu.get_barrier_semaphore()
        signal(barrier, (x_peer, y_peer))
        pl.semaphore_wait(barrier, 2)
        px, py = pl.ds(0, NAX), pl.ds(0, NAY)
        xc = remote(a_ref.at[px, 1 - x], sc_ref.at[0, 2, px], x_send, x_recv, x_peer)
        yc = remote(a_ref.at[py, x], sc_ref.at[1, 1, py], y_send, y_recv, y_peer)
        xc.start()
        yc.start()
        xc.wait()
        yc.wait()


def zero_kernel(token_ref, a_ref, sc_in, c_ref, done_ref, sc_ref, o_ref, zbuf, sem, lsem):
    _, x, _, _ = positions()
    loads = [pltpu.make_async_copy(a_ref.at[:, 1 - x], o_ref.at[0], lsem),
             pltpu.make_async_copy(a_ref.at[:, x], sc_ref.at[0, 0], lsem)]
    for cp in loads:
        cp.start()
    zbuf[...] = jnp.zeros_like(zbuf)
    done_ref[...] = jnp.zeros_like(done_ref)
    copies = []
    for s in range(2):
        for i in range(NC):
            for j in range(i + 1, NC):
                copies.append(pltpu.make_async_copy(zbuf, c_ref.at[chunk(i), s, :, pl.ds(j * TILE, TILE)], sem))
            for q in range(1, CH):
                copies.append(pltpu.make_async_copy(
                    zbuf.at[pl.ds(0, q), :, pl.ds(0, BLOCK)],
                    c_ref.at[pl.ds(i * CH, q), s, :, pl.ds((i * CH + q) * BLOCK, BLOCK)], sem))
    for cp in copies:
        cp.start()
    for cp in copies + loads:
        cp.wait()


def gather_kernel(sc_in, o_in, token_ref, sc_ref, o_ref, t_ref, yb, yr, join, d_send, d_recv, x_send, x_recv, r_send, r_recv,
                  y_send, y_recv, b_send, b_recv, q_send, q_recv, u_send, u_recv, v_send, v_recv):
    y, x, k, col = positions()
    late = k != y
    early = k == y
    side = jnp.where(late, 1, 0)
    partner = (0, y, 2 * x + 1 - k)
    x_peer = (0, y, 2 * (1 - x) + k)
    y_early = (0, 1 - y, 2 * x + 1 - y)
    y_late = (0, 1 - y, 2 * x + y)
    tx, ty = pl.ds(NAX, NM - NAX), pl.ds(NAY, NM - NAY)

    def x_copy(n):
        if n < NC:
            part = pl.ds(n * NM // 2, NM // 2)
            return remote(o_ref.at[0, part], sc_ref.at[0, 2, part], x_send.at[n], x_recv.at[n], x_peer)
        part = pl.ds(*O_PARTS[n - NC])
        return remote(sc_ref.at[0, 0, part], o_ref.at[2, part], x_send.at[n], x_recv.at[n], x_peer)

    def relay_copy(n):
        if n < NC:
            return s_relay(n)
        part = pl.ds(*O_PARTS[n - NC])
        return remote(o_ref.at[2, part], o_ref.at[3, part], r_send.at[n], r_recv.at[n], partner)

    def y_copy(s, c):
        return remote(sc_ref.at[0, 2, chunk(c)], sc_ref.at[1, 2 + s, chunk(c)], y_send.at[c], y_recv.at[s, c], y_late)

    def s_relay(c):
        return remote(sc_ref.at[0, 2, chunk(c)], sc_ref.at[0, 3, chunk(c)], r_send.at[c], r_recv.at[c], partner)

    def s_copy(c):
        return remote(sc_ref.at[0, 0, chunk(c)], sc_ref.at[0, 1, chunk(c)], d_send.at[c], d_recv.at[c], partner)

    def yb_relay(c):
        return remote(yb.at[chunk(c)], sc_ref.at[1, 0, chunk(c)], b_send.at[1 + c], b_recv.at[1 + c], partner)

    def yr_relay(c):
        return remote(yr.at[chunk(c)], sc_ref.at[1, 2, chunk(c)], y_send.at[c], y_recv.at[0, c], partner)

    yr_part = pl.ds(0, NR * CH)
    yr_copy = remote(sc_ref.at[0, 2, yr_part], yr, q_send, q_recv, y_early)
    yb_copy = remote(sc_ref.at[0, 0], yb, b_send.at[0], b_recv.at[0], y_early)
    x_tail = remote(o_ref.at[0, tx], sc_ref.at[0, 2, tx], v_send, v_recv, x_peer)
    u_copy = remote(sc_ref.at[0, 0, ty], sc_ref.at[1, 1, ty], u_send, u_recv, y_late)
    o_copy = remote(o_ref.at[0], o_ref.at[1], d_send.at[NC], d_recv.at[NC], partner)
    barrier = pltpu.get_barrier_semaphore()

    @pl.when(early)
    def _():
        signal(barrier, (x_peer, y_early, partner, y_late))
        pl.semaphore_wait(barrier, 2)
        for n in (0, 1, *range(NC, NX)):
            x_copy(n).start()
        yb_copy.start()
        x_copy(0).wait_recv()
        yr_copy.start()
        pl.semaphore_wait(join, 2)
        for c in range(NC):
            if c == NR:
                x_copy(1).wait_recv()
            s_copy(c).start()
            relay_copy(c).start()
            if c == 0:
                yb_copy.wait_recv()
                yb_relay(c).start()
        for c in range(NC):
            if c == 0:
                yr_copy.wait_recv()
            if c < NR:
                yr_relay(c).start()
            if c + 1 < NC:
                yb_relay(c + 1).start()
        o_copy.start()

    @pl.when(late)
    def _():
        signal(barrier, (x_peer, y_late))
        pl.semaphore_wait(barrier, 4)
        signal(join, (partner, y_early))
        x_tail.start()
        for n in range(NC, NX):
            x_copy(n).start()
        for c in range(NC - 1):
            y_copy(1, c).start()
        u_copy.start()
        for c in range(NC):
            s_copy(c).start()
            if c < NC - 1:
                relay_copy(c).start()
        o_copy.start()
        x_tail.wait_recv()
        relay_copy(NC - 1).start()
        y_copy(1, NC - 1).start()

    def rows_ready(i):
        s_copy(i).wait_recv()
        s_relay(i).wait_recv()

    def o_step(n):
        x_copy(NC + n).wait_recv()
        relay_copy(NC + n).start()

    rows_ready(0)
    row_blk = 2 * x + y
    for c in range(NC):
        if c < NC - 1:
            o_step(c)
        else:
            o_step(len(O_PARTS) - 1)

        @pl.when(early)
        def _():
            if c in (0, 2):
                y_copy(0, NR + c // 2).start()

        @pl.when(late)
        def _():
            yb_relay(c).wait_recv()
            if c == NC - 1:
                u_copy.wait_recv()
            for s in range(2):
                y_copy(s, c).wait_recv()

        if c < NC - 1:
            base = NOW.index((c, c))
            diag_tile(t_ref.at[base], sc_ref, (0,), sc_ref, (side,), c, row_blk, col)

            def body(i, _):
                if c == 0:
                    rows_ready(i)
                full_tile(t_ref.at[base + i - c], sc_ref, (0,), i, sc_ref, (side,), c)
                return 0
            lax.fori_loop(c + 1, NC, body, 0)
        if c == 1:
            o_copy.wait_recv()
            relay_copy(NC).wait_recv()
            for m, (i, j) in enumerate(EXTRA):
                full_tile(t_ref.at[len(NOW) + m], o_ref, (), i, sc_ref, (side,), j)
        if c == 2:
            o_step(c + 1)

    for n in range(1, len(O_PARTS)):
        relay_copy(NC + n).wait_recv()
    for n in range(NX):
        relay_copy(n).wait_send()
    for n in range(NC, NX):
        x_copy(n).wait_send()
    for c in range(NC):
        s_copy(c).wait_send()
        y_copy(0, c).wait_send()
    o_copy.wait_send()

    @pl.when(late)
    def _():
        u_copy.wait_send()
        x_tail.wait_send()

    @pl.when(early)
    def _():
        for n in range(2):
            x_copy(n).wait_send()
        yr_copy.wait_send()
        yb_copy.wait_send()
        for c in range(NC):
            yb_relay(c).wait_send()


def lookup(n, values):
    out = jnp.int32(values[-1])
    for m in range(len(values) - 2, -1, -1):
        out = jnp.where(n == m, jnp.int32(values[m]), out)
    return out


def write_kernel(sc_ref, o_ref, t_ref, c_in, c_ref, obuf, tsem, osem):
    y, x, k, col = positions()
    side = jnp.where(k != y, 1, 0)

    def pick(n, values):
        return [lookup(n, column) for column in zip(*values)]

    def put(src, i, j, s, sem, act):
        @pl.when(i != j)
        def _():
            act(pltpu.make_async_copy(src, c_ref.at[pl.ds(i * CH, CH), s, :, pl.ds(pl.multiple_of(j * TILE, TILE), TILE)], sem))

        @pl.when(i == j)
        def _():
            for q in range(CH):
                act(pltpu.make_async_copy(
                    src.at[pl.ds(q, CH - q), :, pl.ds(q * BLOCK, BLOCK)],
                    c_ref.at[pl.ds(i * CH + q, CH - q), s, :, pl.ds(pl.multiple_of(j * TILE + q * BLOCK, BLOCK), BLOCK)], sem))

    def put_panel(n, act):
        i, j, cls = pick(n, PANELS)
        put(t_ref.at[n], i, j, jnp.where(cls == 0, x, 1 - x), tsem, act)

    def put_job(n, act):
        i, j = pick(n, LATER)
        b = lax.rem(n, NBUF)
        put(obuf.at[b], i, j, 1 - x, osem.at[b], act)

    def start(cp):
        cp.start()

    def wait(cp):
        cp.wait()

    for n in range(LEAD):
        put_panel(jnp.int32(n), start)

    def body(n, _):
        i, j = pick(n, LATER)
        b = lax.rem(n, NBUF)

        @pl.when(n >= NBUF)
        def _():
            put_job(n - NBUF, wait)

        @pl.when(i != j)
        def _():
            full_tile(obuf.at[b], o_ref, (), i, sc_ref, (side,), j)

        @pl.when(i == j)
        def _():
            diag_tile(obuf.at[b], o_ref, (), sc_ref, (side,), j, 2 * (1 - x) + y, col)
        put_job(n, start)

        @pl.when(n + LEAD < len(PANELS))
        def _():
            put_panel(jnp.minimum(n + LEAD, len(PANELS) - 1), start)
        return 0

    lax.fori_loop(0, len(LATER), body, 0)
    last_slot = len(LATER) % NBUF
    put_job(jnp.int32(len(LATER) - NBUF), wait)
    diag_tile(obuf.at[last_slot], sc_ref, (0,), sc_ref, (side,), LAST[1], 2 * x + y, col)
    put(obuf.at[last_slot], jnp.int32(LAST[0]), jnp.int32(LAST[1]), x, osem.at[last_slot], start)

    def drain(n, _):
        put_panel(n, wait)

        @pl.when(jnp.logical_and(n > len(LATER) - NBUF, n < len(LATER)))
        def _():
            put_job(jnp.minimum(n, len(LATER) - 1), wait)
        return 0
    lax.fori_loop(0, len(PANELS), drain, 0)
    put(obuf.at[last_slot], jnp.int32(LAST[0]), jnp.int32(LAST[1]), x, osem.at[last_slot], wait)


def solution(mesh):
    def local_fn(a):
        a4 = pltpu.with_memory_space_constraint(a.reshape(NM, 2, BLOCK, PIECE), pltpu.HBM)
        any_spec = pl.BlockSpec(memory_space=pl.ANY)
        hbm = pl.BlockSpec(memory_space=pltpu.HBM)
        vmem = pl.BlockSpec(memory_space=pltpu.VMEM)
        dma = pltpu.SemaphoreType.DMA
        half_flops = 136 * 2 * BLOCK * BLOCK * K_DIM
        panels = pltpu.VMEM((2, PIECES, NM, BLOCK, PIECE), jnp.bfloat16)
        token = jax.ShapeDtypeStruct((8, 128), jnp.float32)
        sc, first = pl.pallas_call(
            first_kernel,
            out_shape=[panels, token],
            in_specs=[hbm],
            out_specs=[vmem, vmem],
            scratch_shapes=[dma(())] * 4,
            compiler_params=pltpu.CompilerParams(collective_id=0, has_side_effects=True, vmem_limit_bytes=2 * 1024 * 1024),
        )(a4)
        rest = pltpu.VMEM((PIECES, NM, BLOCK, PIECE), jnp.bfloat16)
        c, zeroed, sc, o = pl.pallas_call(
            zero_kernel,
            out_shape=[jax.ShapeDtypeStruct((NM, 2, BLOCK, NM * BLOCK), jnp.bfloat16), token, panels, rest],
            in_specs=[any_spec, hbm, vmem],
            out_specs=[any_spec, vmem, vmem, vmem],
            input_output_aliases={2: 2},
            scratch_shapes=[pltpu.VMEM((CH, BLOCK, TILE), jnp.bfloat16), dma(()), dma(())],
            compiler_params=pltpu.CompilerParams(vmem_limit_bytes=4 * 1024 * 1024),
            cost_estimate=pl.CostEstimate(flops=half_flops, bytes_accessed=30 << 20, transcendentals=0),
        )(first, a4, sc)
        sc, o, t = pl.pallas_call(
            gather_kernel,
            out_shape=[panels, rest,
                       pltpu.VMEM((len(PANELS), CH, BLOCK, TILE), jnp.bfloat16)],
            in_specs=[vmem, vmem, any_spec],
            out_specs=[vmem] * 3,
            input_output_aliases={0: 0, 1: 1},
            scratch_shapes=[pltpu.VMEM((NM, BLOCK, PIECE), jnp.bfloat16), pltpu.VMEM((NR * CH, BLOCK, PIECE), jnp.bfloat16),
                            pltpu.SemaphoreType.REGULAR,
                            dma((NC + 1,)), dma((NC + 1,)), dma((NX,)), dma((NX,)), dma((NX,)), dma((NX,)),
                            dma((NC,)), dma((2, NC)), dma((NC + 1,)), dma((NC + 1,)), dma(()), dma(())] + [dma(())] * 4,
            compiler_params=pltpu.CompilerParams(collective_id=1, has_side_effects=True, vmem_limit_bytes=8 * 1024 * 1024),
            cost_estimate=pl.CostEstimate(flops=half_flops, bytes_accessed=2 << 20, transcendentals=0),
        )(sc, o, zeroed)
        c = pl.pallas_call(
            write_kernel,
            out_shape=jax.ShapeDtypeStruct((NM, 2, BLOCK, NM * BLOCK), jnp.bfloat16),
            in_specs=[vmem] * 3 + [any_spec],
            out_specs=any_spec,
            input_output_aliases={3: 0},
            scratch_shapes=[pltpu.VMEM((NBUF, CH, BLOCK, TILE), jnp.bfloat16), dma(()), dma((NBUF,))],
            compiler_params=pltpu.CompilerParams(vmem_limit_bytes=15 * 1024 * 1024),
            cost_estimate=pl.CostEstimate(flops=half_flops, bytes_accessed=34 << 20, transcendentals=0),
        )(sc, o, t, c)
        return c.reshape(2 * NM * BLOCK, NM * BLOCK)

    spec = P(('batch', 'row'), 'col')
    return jax.shard_map(local_fn, mesh=mesh, in_specs=(spec,), out_specs=spec, check_vma=False)
```

```python
import functools
import jax
import jax.numpy as jnp
from jax import lax
from jax.experimental import pallas as pl
from jax.experimental.pallas import tpu as pltpu
from jax.sharding import PartitionSpec as P

BLOCK = 256
K_DIM = 512
PIECE = 128
PIECES = K_DIM // PIECE
NM = 16
CH = 4
NC = NM // CH
NBUF = 5
LEAD = 4
TILE = CH * BLOCK
JOBS = [(i, j) for j in range(NC) for i in range(j, NC)]
LAST = (NC - 1, NC - 1)
NOW = [job for job in JOBS if job != LAST]
NAX, NAY = 15, 15
NR = 2
O_PARTS = ((12, 4), (0, 4), (4, 4), (8, 3), (11, 1))
NX = NC + len(O_PARTS)
EXTRA = [(3, 0), (3, 1)]
LATER = [job for job in JOBS if job not in EXTRA]
PANELS = [(i, j, 0) for i, j in NOW] + [(i, j, 1) for i, j in EXTRA]


def positions():
    y = lax.axis_index('row')
    col = lax.axis_index('col')
    return y, col // 2, col % 2, col


def chunk(c):
    return pl.ds(c * CH, CH)


def panel(ref, lead, first, count):
    parts = [ref[(*lead, p, pl.ds(first, count))].reshape(count * BLOCK, PIECE) for p in range(PIECES)]
    return jnp.concatenate(parts, axis=1)


def dot_t(rows, cols):
    return lax.dot_general(rows, cols, (((1,), (1,)), ((), ())), preferred_element_type=jnp.float32)


def full_tile(out, row_ref, row_lead, i, col_ref, col_lead, j):
    prod = dot_t(panel(row_ref, row_lead, i * CH, CH), panel(col_ref, col_lead, j * CH, CH))
    out[...] = prod.astype(jnp.bfloat16).reshape(CH, BLOCK, TILE)


def diag_tile(out, row_ref, row_lead, col_ref, col_lead, j, row_blk, col_blk):
    for q in range(CH):
        prod = dot_t(panel(row_ref, row_lead, j * CH + q, CH - q), panel(col_ref, col_lead, j * CH + q, 1))
        row_id = lax.broadcasted_iota(jnp.int32, (BLOCK, BLOCK), 0) + row_blk * BLOCK
        col_id = lax.broadcasted_iota(jnp.int32, (BLOCK, BLOCK), 1) + col_blk * BLOCK
        lanes = slice(q * BLOCK, (q + 1) * BLOCK)
        out[q, :, lanes] = jnp.where(row_id >= col_id, prod[:BLOCK], 0.0).astype(jnp.bfloat16)
        if q + 1 < CH:
            out[q + 1:, :, lanes] = prod[BLOCK:].astype(jnp.bfloat16).reshape(CH - q - 1, BLOCK, BLOCK)


MESH_ID = pl.DeviceIdType.MESH


def remote(src, dst, send, recv, dev):
    return pltpu.make_async_remote_copy(src, dst, send, recv, device_id=dev, device_id_type=MESH_ID)


def signal(sem, devices):
    for dev in devices:
        pl.semaphore_signal(sem, inc=1, device_id=dev, device_id_type=MESH_ID)


def first_kernel(a_ref, sc_ref, token_ref, x_send, x_recv, y_send, y_recv):
    y, x, k, _ = positions()
    token_ref[...] = jnp.zeros_like(token_ref)

    @pl.when(k != y)
    def _():
        x_peer = (0, y, 2 * (1 - x) + k)
        y_peer = (0, 1 - y, 2 * x + y)
        barrier = pltpu.get_barrier_semaphore()
        signal(barrier, (x_peer, y_peer))
        pl.semaphore_wait(barrier, 2)
        px, py = pl.ds(0, NAX), pl.ds(0, NAY)
        xc = remote(a_ref.at[px, 1 - x], sc_ref.at[0, 2, px], x_send, x_recv, x_peer)
        yc = remote(a_ref.at[py, x], sc_ref.at[1, 1, py], y_send, y_recv, y_peer)
        xc.start()
        yc.start()
        xc.wait()
        yc.wait()


def zero_kernel(token_ref, a_ref, sc_in, c_ref, done_ref, sc_ref, o_ref, zbuf, sem, lsem):
    _, x, _, _ = positions()
    loads = [pltpu.make_async_copy(a_ref.at[:, 1 - x], o_ref.at[0], lsem),
             pltpu.make_async_copy(a_ref.at[:, x], sc_ref.at[0, 0], lsem)]
    for cp in loads:
        cp.start()
    zbuf[...] = jnp.zeros_like(zbuf)
    done_ref[...] = jnp.zeros_like(done_ref)
    copies = []
    for s in range(2):
        for i in range(NC):
            for j in range(i + 1, NC):
                copies.append(pltpu.make_async_copy(zbuf, c_ref.at[chunk(i), s, :, pl.ds(j * TILE, TILE)], sem))
            for q in range(1, CH):
                copies.append(pltpu.make_async_copy(
                    zbuf.at[pl.ds(0, q), :, pl.ds(0, BLOCK)],
                    c_ref.at[pl.ds(i * CH, q), s, :, pl.ds((i * CH + q) * BLOCK, BLOCK)], sem))
    for cp in copies:
        cp.start()
    for cp in copies + loads:
        cp.wait()


def gather_kernel(sc_in, o_in, token_ref, sc_ref, o_ref, t_ref, yb, yr, join, d_send, d_recv, x_send, x_recv, r_send, r_recv,
                  y_send, y_recv, b_send, b_recv, q_send, q_recv, u_send, u_recv, v_send, v_recv):
    y, x, k, col = positions()
    late = k != y
    early = k == y
    side = jnp.where(late, 1, 0)
    partner = (0, y, 2 * x + 1 - k)
    x_peer = (0, y, 2 * (1 - x) + k)
    y_early = (0, 1 - y, 2 * x + 1 - y)
    y_late = (0, 1 - y, 2 * x + y)
    tx, ty = pl.ds(NAX, NM - NAX), pl.ds(NAY, NM - NAY)

    def x_copy(n):
        if n < NC:
            part = pl.ds(n * NM // 2, NM // 2)
            return remote(o_ref.at[0, part], sc_ref.at[0, 2, part], x_send.at[n], x_recv.at[n], x_peer)
        part = pl.ds(*O_PARTS[n - NC])
        return remote(sc_ref.at[0, 0, part], o_ref.at[2, part], x_send.at[n], x_recv.at[n], x_peer)

    def relay_copy(n):
        if n < NC:
            return s_relay(n)
        part = pl.ds(*O_PARTS[n - NC])
        return remote(o_ref.at[2, part], o_ref.at[3, part], r_send.at[n], r_recv.at[n], partner)

    def y_copy(s, c):
        return remote(sc_ref.at[0, 2, chunk(c)], sc_ref.at[1, 2 + s, chunk(c)], y_send.at[c], y_recv.at[s, c], y_late)

    def s_relay(c):
        return remote(sc_ref.at[0, 2, chunk(c)], sc_ref.at[0, 3, chunk(c)], r_send.at[c], r_recv.at[c], partner)

    def s_copy(c):
        return remote(sc_ref.at[0, 0, chunk(c)], sc_ref.at[0, 1, chunk(c)], d_send.at[c], d_recv.at[c], partner)

    def yb_relay(c):
        return remote(yb.at[chunk(c)], sc_ref.at[1, 0, chunk(c)], b_send.at[1 + c], b_recv.at[1 + c], partner)

    def yr_relay(c):
        return remote(yr.at[chunk(c)], sc_ref.at[1, 2, chunk(c)], y_send.at[c], y_recv.at[0, c], partner)

    yr_part = pl.ds(0, NR * CH)
    yr_copy = remote(sc_ref.at[0, 2, yr_part], yr, q_send, q_recv, y_early)
    yb_copy = remote(sc_ref.at[0, 0], yb, b_send.at[0], b_recv.at[0], y_early)
    x_tail = remote(o_ref.at[0, tx], sc_ref.at[0, 2, tx], v_send, v_recv, x_peer)
    u_copy = remote(sc_ref.at[0, 0, ty], sc_ref.at[1, 1, ty], u_send, u_recv, y_late)
    o_copy = remote(o_ref.at[0], o_ref.at[1], d_send.at[NC], d_recv.at[NC], partner)
    barrier = pltpu.get_barrier_semaphore()

    @pl.when(early)
    def _():
        signal(barrier, (x_peer, y_early, partner, y_late))
        pl.semaphore_wait(barrier, 2)
        for n in (0, 1, *range(NC, NX)):
            x_copy(n).start()
        yb_copy.start()
        x_copy(0).wait_recv()
        yr_copy.start()
        pl.semaphore_wait(join, 2)
        for c in range(NC):
            if c == NR:
                x_copy(1).wait_recv()
            s_copy(c).start()
            relay_copy(c).start()
            if c == 0:
                yb_copy.wait_recv()
                yb_relay(c).start()
        for c in range(NC):
            if c == 0:
                yr_copy.wait_recv()
            if c < NR:
                yr_relay(c).start()
            if c + 1 < NC:
                yb_relay(c + 1).start()
        o_copy.start()

    @pl.when(late)
    def _():
        signal(barrier, (x_peer, y_late))
        pl.semaphore_wait(barrier, 4)
        signal(join, (partner, y_early))
        x_tail.start()
        for n in range(NC, NX):
            x_copy(n).start()
        for c in range(NC - 1):
            y_copy(1, c).start()
        u_copy.start()
        for c in range(NC):
            s_copy(c).start()
            if c < NC - 1:
                relay_copy(c).start()
        o_copy.start()
        x_tail.wait_recv()
        relay_copy(NC - 1).start()
        y_copy(1, NC - 1).start()

    def rows_ready(i):
        s_copy(i).wait_recv()
        s_relay(i).wait_recv()

    def o_step(n):
        x_copy(NC + n).wait_recv()
        relay_copy(NC + n).start()

    rows_ready(0)
    row_blk = 2 * x + y
    for c in range(NC):
        if c == NC - 1:
            o_step(len(O_PARTS) - 1)

        @pl.when(early)
        def _():
            if c in (0, 2):
                y_copy(0, NR + c // 2).start()

        @pl.when(late)
        def _():
            yb_relay(c).wait_recv()
            if c == NC - 1:
                u_copy.wait_recv()
            for s in range(2):
                y_copy(s, c).wait_recv()

        if c < NC - 1:
            base = NOW.index((c, c))
            diag_tile(t_ref.at[base], sc_ref, (0,), sc_ref, (side,), c, row_blk, col)

            def body(i, _):
                if c == 0:
                    rows_ready(i)
                full_tile(t_ref.at[base + i - c], sc_ref, (0,), i, sc_ref, (side,), c)
                return 0
            lax.fori_loop(c + 1, NC, body, 0)
            o_step(c)
        if c == 1:
            o_copy.wait_recv()
            relay_copy(NC).wait_recv()
            for m, (i, j) in enumerate(EXTRA):
                full_tile(t_ref.at[len(NOW) + m], o_ref, (), i, sc_ref, (side,), j)
        if c == 2:
            o_step(c + 1)

    for n in range(1, len(O_PARTS)):
        relay_copy(NC + n).wait_recv()
    for n in range(NX):
        relay_copy(n).wait_send()
    for n in range(NC, NX):
        x_copy(n).wait_send()
    for c in range(NC):
        s_copy(c).wait_send()
        y_copy(0, c).wait_send()
    o_copy.wait_send()

    @pl.when(late)
    def _():
        u_copy.wait_send()
        x_tail.wait_send()

    @pl.when(early)
    def _():
        for n in range(2):
            x_copy(n).wait_send()
        yr_copy.wait_send()
        yb_copy.wait_send()
        for c in range(NC):
            yb_relay(c).wait_send()


def lookup(n, values):
    out = jnp.int32(values[-1])
    for m in range(len(values) - 2, -1, -1):
        out = jnp.where(n == m, jnp.int32(values[m]), out)
    return out


def write_kernel(sc_ref, o_ref, t_ref, c_in, c_ref, obuf, tsem, osem):
    y, x, k, col = positions()
    side = jnp.where(k != y, 1, 0)

    def pick(n, values):
        return [lookup(n, column) for column in zip(*values)]

    def put(src, i, j, s, sem, act):
        @pl.when(i != j)
        def _():
            act(pltpu.make_async_copy(src, c_ref.at[pl.ds(i * CH, CH), s, :, pl.ds(pl.multiple_of(j * TILE, TILE), TILE)], sem))

        @pl.when(i == j)
        def _():
            for q in range(CH):
                act(pltpu.make_async_copy(
                    src.at[pl.ds(q, CH - q), :, pl.ds(q * BLOCK, BLOCK)],
                    c_ref.at[pl.ds(i * CH + q, CH - q), s, :, pl.ds(pl.multiple_of(j * TILE + q * BLOCK, BLOCK), BLOCK)], sem))

    def put_panel(n, act):
        i, j, cls = pick(n, PANELS)
        put(t_ref.at[n], i, j, jnp.where(cls == 0, x, 1 - x), tsem, act)

    def put_job(n, act):
        i, j = pick(n, LATER)
        b = lax.rem(n, NBUF)
        put(obuf.at[b], i, j, 1 - x, osem.at[b], act)

    def start(cp):
        cp.start()

    def wait(cp):
        cp.wait()

    for n in range(LEAD):
        put_panel(jnp.int32(n), start)

    def body(n, _):
        i, j = pick(n, LATER)
        b = lax.rem(n, NBUF)

        @pl.when(n >= NBUF)
        def _():
            put_job(n - NBUF, wait)

        @pl.when(i != j)
        def _():
            full_tile(obuf.at[b], o_ref, (), i, sc_ref, (side,), j)

        @pl.when(i == j)
        def _():
            diag_tile(obuf.at[b], o_ref, (), sc_ref, (side,), j, 2 * (1 - x) + y, col)
        put_job(n, start)

        @pl.when(n + LEAD < len(PANELS))
        def _():
            put_panel(jnp.minimum(n + LEAD, len(PANELS) - 1), start)
        return 0

    lax.fori_loop(0, len(LATER), body, 0)
    last_slot = len(LATER) % NBUF
    put_job(jnp.int32(len(LATER) - NBUF), wait)
    diag_tile(obuf.at[last_slot], sc_ref, (0,), sc_ref, (side,), LAST[1], 2 * x + y, col)
    put(obuf.at[last_slot], jnp.int32(LAST[0]), jnp.int32(LAST[1]), x, osem.at[last_slot], start)

    def drain(n, _):
        put_panel(n, wait)

        @pl.when(jnp.logical_and(n > len(LATER) - NBUF, n < len(LATER)))
        def _():
            put_job(jnp.minimum(n, len(LATER) - 1), wait)
        return 0
    lax.fori_loop(0, len(PANELS), drain, 0)
    put(obuf.at[last_slot], jnp.int32(LAST[0]), jnp.int32(LAST[1]), x, osem.at[last_slot], wait)


def solution(mesh):
    def local_fn(a):
        a4 = pltpu.with_memory_space_constraint(a.reshape(NM, 2, BLOCK, PIECE), pltpu.HBM)
        any_spec = pl.BlockSpec(memory_space=pl.ANY)
        hbm = pl.BlockSpec(memory_space=pltpu.HBM)
        vmem = pl.BlockSpec(memory_space=pltpu.VMEM)
        dma = pltpu.SemaphoreType.DMA
        half_flops = 136 * 2 * BLOCK * BLOCK * K_DIM
        panels = pltpu.VMEM((2, PIECES, NM, BLOCK, PIECE), jnp.bfloat16)
        token = jax.ShapeDtypeStruct((8, 128), jnp.float32)
        sc, first = pl.pallas_call(
            first_kernel,
            out_shape=[panels, token],
            in_specs=[hbm],
            out_specs=[vmem, vmem],
            scratch_shapes=[dma(())] * 4,
            compiler_params=pltpu.CompilerParams(collective_id=0, has_side_effects=True, vmem_limit_bytes=2 * 1024 * 1024),
        )(a4)
        rest = pltpu.VMEM((PIECES, NM, BLOCK, PIECE), jnp.bfloat16)
        c, zeroed, sc, o = pl.pallas_call(
            zero_kernel,
            out_shape=[jax.ShapeDtypeStruct((NM, 2, BLOCK, NM * BLOCK), jnp.bfloat16), token, panels, rest],
            in_specs=[any_spec, hbm, vmem],
            out_specs=[any_spec, vmem, vmem, vmem],
            input_output_aliases={2: 2},
            scratch_shapes=[pltpu.VMEM((CH, BLOCK, TILE), jnp.bfloat16), dma(()), dma(())],
            compiler_params=pltpu.CompilerParams(vmem_limit_bytes=4 * 1024 * 1024),
            cost_estimate=pl.CostEstimate(flops=half_flops, bytes_accessed=30 << 20, transcendentals=0),
        )(first, a4, sc)
        sc, o, t = pl.pallas_call(
            gather_kernel,
            out_shape=[panels, rest,
                       pltpu.VMEM((len(PANELS), CH, BLOCK, TILE), jnp.bfloat16)],
            in_specs=[vmem, vmem, any_spec],
            out_specs=[vmem] * 3,
            input_output_aliases={0: 0, 1: 1},
            scratch_shapes=[pltpu.VMEM((NM, BLOCK, PIECE), jnp.bfloat16), pltpu.VMEM((NR * CH, BLOCK, PIECE), jnp.bfloat16),
                            pltpu.SemaphoreType.REGULAR,
                            dma((NC + 1,)), dma((NC + 1,)), dma((NX,)), dma((NX,)), dma((NX,)), dma((NX,)),
                            dma((NC,)), dma((2, NC)), dma((NC + 1,)), dma((NC + 1,)), dma(()), dma(())] + [dma(())] * 4,
            compiler_params=pltpu.CompilerParams(collective_id=1, has_side_effects=True, vmem_limit_bytes=8 * 1024 * 1024),
            cost_estimate=pl.CostEstimate(flops=half_flops, bytes_accessed=2 << 20, transcendentals=0),
        )(sc, o, zeroed)
        c = pl.pallas_call(
            write_kernel,
            out_shape=jax.ShapeDtypeStruct((NM, 2, BLOCK, NM * BLOCK), jnp.bfloat16),
            in_specs=[vmem] * 3 + [any_spec],
            out_specs=any_spec,
            input_output_aliases={3: 0},
            scratch_shapes=[pltpu.VMEM((NBUF, CH, BLOCK, TILE), jnp.bfloat16), dma(()), dma((NBUF,))],
            compiler_params=pltpu.CompilerParams(vmem_limit_bytes=15 * 1024 * 1024),
            cost_estimate=pl.CostEstimate(flops=half_flops, bytes_accessed=34 << 20, transcendentals=0),
        )(sc, o, t, c)
        return c.reshape(2 * NM * BLOCK, NM * BLOCK)

    spec = P(('batch', 'row'), 'col')
    return jax.shard_map(local_fn, mesh=mesh, in_specs=(spec,), out_specs=spec, check_vma=False)
```

```python
import functools
import jax
import jax.numpy as jnp
from jax import lax
from jax.experimental import pallas as pl
from jax.experimental.pallas import tpu as pltpu
from jax.sharding import PartitionSpec as P

BLOCK = 256
K_DIM = 512
PIECE = 128
PIECES = K_DIM // PIECE
NM = 16
CH = 4
NC = NM // CH
NBUF = 5
LEAD = 4
TILE = CH * BLOCK
JOBS = [(i, j) for j in range(NC) for i in range(j, NC)]
LAST = (NC - 1, NC - 1)
NOW = [job for job in JOBS if job != LAST]
HEAD = 2
NAX, NAY = 15, 15
NR = 2
O_PARTS = ((12, 4), (0, 4), (4, 4), (8, 3), (11, 1))
NX = NC + len(O_PARTS)
EXTRA = [(3, 0), (3, 1)]
LATER = [job for job in JOBS if job not in EXTRA]
PANELS = [(i, j, 0) for i, j in NOW] + [(i, j, 1) for i, j in EXTRA]


def positions():
    y = lax.axis_index('row')
    col = lax.axis_index('col')
    return y, col // 2, col % 2, col


def chunk(c):
    return pl.ds(c * CH, CH)


def panel(ref, lead, first, count):
    parts = [ref[(*lead, p, pl.ds(first, count))].reshape(count * BLOCK, PIECE) for p in range(PIECES)]
    return jnp.concatenate(parts, axis=1)


def dot_t(rows, cols):
    return lax.dot_general(rows, cols, (((1,), (1,)), ((), ())), preferred_element_type=jnp.float32)


def full_tile(out, row_ref, row_lead, i, col_ref, col_lead, j):
    prod = dot_t(panel(row_ref, row_lead, i * CH, CH), panel(col_ref, col_lead, j * CH, CH))
    out[...] = prod.astype(jnp.bfloat16).reshape(CH, BLOCK, TILE)


def diag_tile(out, row_ref, row_lead, col_ref, col_lead, j, row_blk, col_blk):
    for q in range(CH):
        prod = dot_t(panel(row_ref, row_lead, j * CH + q, CH - q), panel(col_ref, col_lead, j * CH + q, 1))
        row_id = lax.broadcasted_iota(jnp.int32, (BLOCK, BLOCK), 0) + row_blk * BLOCK
        col_id = lax.broadcasted_iota(jnp.int32, (BLOCK, BLOCK), 1) + col_blk * BLOCK
        lanes = slice(q * BLOCK, (q + 1) * BLOCK)
        out[q, :, lanes] = jnp.where(row_id >= col_id, prod[:BLOCK], 0.0).astype(jnp.bfloat16)
        if q + 1 < CH:
            out[q + 1:, :, lanes] = prod[BLOCK:].astype(jnp.bfloat16).reshape(CH - q - 1, BLOCK, BLOCK)


MESH_ID = pl.DeviceIdType.MESH


def remote(src, dst, send, recv, dev):
    return pltpu.make_async_remote_copy(src, dst, send, recv, device_id=dev, device_id_type=MESH_ID)


def signal(sem, devices):
    for dev in devices:
        pl.semaphore_signal(sem, inc=1, device_id=dev, device_id_type=MESH_ID)


def first_kernel(a_ref, sc_ref, token_ref, head, lsem, x_send, x_recv, y_send, y_recv):
    y, x, k, _ = positions()
    token_ref[...] = jnp.zeros_like(token_ref)

    @pl.when(k != y)
    def _():
        x_peer = (0, y, 2 * (1 - x) + k)
        y_peer = (0, 1 - y, 2 * x + y)
        first = pl.ds(0, HEAD)
        loads = [pltpu.make_async_copy(a_ref.at[first, 1 - x], head.at[0], lsem.at[0]),
                 pltpu.make_async_copy(a_ref.at[first, x], head.at[1], lsem.at[1])]
        for cp in loads:
            cp.start()
        barrier = pltpu.get_barrier_semaphore()
        signal(barrier, (x_peer, y_peer))
        pl.semaphore_wait(barrier, 2)
        px, py = pl.ds(HEAD, NAX - HEAD), pl.ds(HEAD, NAY - HEAD)
        sends = [remote(head.at[0], sc_ref.at[0, 2, first], x_send.at[0], x_recv.at[0], x_peer),
                 remote(head.at[1], sc_ref.at[1, 1, first], y_send.at[0], y_recv.at[0], y_peer),
                 remote(a_ref.at[px, 1 - x], sc_ref.at[0, 2, px], x_send.at[1], x_recv.at[1], x_peer),
                 remote(a_ref.at[py, x], sc_ref.at[1, 1, py], y_send.at[1], y_recv.at[1], y_peer)]
        for cp in loads:
            cp.wait()
        for cp in sends:
            cp.start()
        for cp in sends:
            cp.wait()


def zero_kernel(token_ref, a_ref, sc_in, c_ref, done_ref, sc_ref, o_ref, zbuf, sem, lsem):
    _, x, _, _ = positions()
    loads = [pltpu.make_async_copy(a_ref.at[:, 1 - x], o_ref.at[0], lsem),
             pltpu.make_async_copy(a_ref.at[:, x], sc_ref.at[0, 0], lsem)]
    for cp in loads:
        cp.start()
    zbuf[...] = jnp.zeros_like(zbuf)
    done_ref[...] = jnp.zeros_like(done_ref)
    copies = []
    for s in range(2):
        for i in range(NC):
            for j in range(i + 1, NC):
                copies.append(pltpu.make_async_copy(zbuf, c_ref.at[chunk(i), s, :, pl.ds(j * TILE, TILE)], sem))
            for q in range(1, CH):
                copies.append(pltpu.make_async_copy(
                    zbuf.at[pl.ds(0, q), :, pl.ds(0, BLOCK)],
                    c_ref.at[pl.ds(i * CH, q), s, :, pl.ds((i * CH + q) * BLOCK, BLOCK)], sem))
    for cp in copies:
        cp.start()
    for cp in copies + loads:
        cp.wait()


def gather_kernel(sc_in, o_in, token_ref, sc_ref, o_ref, t_ref, yb, yr, join, d_send, d_recv, x_send, x_recv, r_send, r_recv,
                  y_send, y_recv, b_send, b_recv, q_send, q_recv, u_send, u_recv, v_send, v_recv):
    y, x, k, col = positions()
    late = k != y
    early = k == y
    side = jnp.where(late, 1, 0)
    partner = (0, y, 2 * x + 1 - k)
    x_peer = (0, y, 2 * (1 - x) + k)
    y_early = (0, 1 - y, 2 * x + 1 - y)
    y_late = (0, 1 - y, 2 * x + y)
    tx, ty = pl.ds(NAX, NM - NAX), pl.ds(NAY, NM - NAY)

    def x_copy(n):
        if n < NC:
            part = pl.ds(n * NM // 2, NM // 2)
            return remote(o_ref.at[0, part], sc_ref.at[0, 2, part], x_send.at[n], x_recv.at[n], x_peer)
        part = pl.ds(*O_PARTS[n - NC])
        return remote(sc_ref.at[0, 0, part], o_ref.at[2, part], x_send.at[n], x_recv.at[n], x_peer)

    def relay_copy(n):
        if n < NC:
            return s_relay(n)
        part = pl.ds(*O_PARTS[n - NC])
        return remote(o_ref.at[2, part], o_ref.at[3, part], r_send.at[n], r_recv.at[n], partner)

    def y_copy(s, c):
        return remote(sc_ref.at[0, 2, chunk(c)], sc_ref.at[1, 2 + s, chunk(c)], y_send.at[c], y_recv.at[s, c], y_late)

    def s_relay(c):
        return remote(sc_ref.at[0, 2, chunk(c)], sc_ref.at[0, 3, chunk(c)], r_send.at[c], r_recv.at[c], partner)

    def s_copy(c):
        return remote(sc_ref.at[0, 0, chunk(c)], sc_ref.at[0, 1, chunk(c)], d_send.at[c], d_recv.at[c], partner)

    def yb_relay(c):
        return remote(yb.at[chunk(c)], sc_ref.at[1, 0, chunk(c)], b_send.at[1 + c], b_recv.at[1 + c], partner)

    def yr_relay(c):
        return remote(yr.at[chunk(c)], sc_ref.at[1, 2, chunk(c)], y_send.at[c], y_recv.at[0, c], partner)

    yr_part = pl.ds(0, NR * CH)
    yr_copy = remote(sc_ref.at[0, 2, yr_part], yr, q_send, q_recv, y_early)
    yb_copy = remote(sc_ref.at[0, 0], yb, b_send.at[0], b_recv.at[0], y_early)
    x_tail = remote(o_ref.at[0, tx], sc_ref.at[0, 2, tx], v_send, v_recv, x_peer)
    u_copy = remote(sc_ref.at[0, 0, ty], sc_ref.at[1, 1, ty], u_send, u_recv, y_late)
    o_copy = remote(o_ref.at[0], o_ref.at[1], d_send.at[NC], d_recv.at[NC], partner)
    barrier = pltpu.get_barrier_semaphore()

    @pl.when(early)
    def _():
        signal(barrier, (x_peer, y_early, partner, y_late))
        pl.semaphore_wait(barrier, 2)
        for n in (0, 1, *range(NC, NX)):
            x_copy(n).start()
        yb_copy.start()
        x_copy(0).wait_recv()
        yr_copy.start()
        pl.semaphore_wait(join, 2)
        for c in range(NC):
            if c == NR:
                x_copy(1).wait_recv()
            s_copy(c).start()
            relay_copy(c).start()
            if c == 0:
                yb_copy.wait_recv()
                yb_relay(c).start()
        for c in range(NC):
            if c == 0:
                yr_copy.wait_recv()
            if c < NR:
                yr_relay(c).start()
            if c + 1 < NC:
                yb_relay(c + 1).start()
        o_copy.start()

    @pl.when(late)
    def _():
        signal(barrier, (x_peer, y_late))
        pl.semaphore_wait(barrier, 4)
        signal(join, (partner, y_early))
        x_tail.start()
        for n in range(NC, NX):
            x_copy(n).start()
        for c in range(NC - 1):
            y_copy(1, c).start()
        u_copy.start()
        for c in range(NC):
            s_copy(c).start()
            if c < NC - 1:
                relay_copy(c).start()
        o_copy.start()
        x_tail.wait_recv()
        relay_copy(NC - 1).start()
        y_copy(1, NC - 1).start()

    def rows_ready(i):
        s_copy(i).wait_recv()
        s_relay(i).wait_recv()

    def o_step(n):
        x_copy(NC + n).wait_recv()
        relay_copy(NC + n).start()

    rows_ready(0)
    row_blk = 2 * x + y
    for c in range(NC):
        if c == NC - 1:
            o_step(len(O_PARTS) - 1)

        @pl.when(early)
        def _():
            if c in (0, 2):
                y_copy(0, NR + c // 2).start()

        @pl.when(late)
        def _():
            yb_relay(c).wait_recv()
            if c == NC - 1:
                u_copy.wait_recv()
            for s in range(2):
                y_copy(s, c).wait_recv()

        if c < NC - 1:
            base = NOW.index((c, c))
            diag_tile(t_ref.at[base], sc_ref, (0,), sc_ref, (side,), c, row_blk, col)

            def body(i, _):
                if c == 0:
                    rows_ready(i)
                full_tile(t_ref.at[base + i - c], sc_ref, (0,), i, sc_ref, (side,), c)
                return 0
            lax.fori_loop(c + 1, NC, body, 0)
            o_step(c)
        if c == 1:
            o_copy.wait_recv()
            relay_copy(NC).wait_recv()
            for m, (i, j) in enumerate(EXTRA):
                full_tile(t_ref.at[len(NOW) + m], o_ref, (), i, sc_ref, (side,), j)
        if c == 2:
            o_step(c + 1)

    for n in range(1, len(O_PARTS)):
        relay_copy(NC + n).wait_recv()
    for n in range(NX):
        relay_copy(n).wait_send()
    for n in range(NC, NX):
        x_copy(n).wait_send()
    for c in range(NC):
        s_copy(c).wait_send()
        y_copy(0, c).wait_send()
    o_copy.wait_send()

    @pl.when(late)
    def _():
        u_copy.wait_send()
        x_tail.wait_send()

    @pl.when(early)
    def _():
        for n in range(2):
            x_copy(n).wait_send()
        yr_copy.wait_send()
        yb_copy.wait_send()
        for c in range(NC):
            yb_relay(c).wait_send()


def lookup(n, values):
    out = jnp.int32(values[-1])
    for m in range(len(values) - 2, -1, -1):
        out = jnp.where(n == m, jnp.int32(values[m]), out)
    return out


def write_kernel(sc_ref, o_ref, t_ref, c_in, c_ref, obuf, tsem, osem):
    y, x, k, col = positions()
    side = jnp.where(k != y, 1, 0)

    def pick(n, values):
        return [lookup(n, column) for column in zip(*values)]

    def put(src, i, j, s, sem, act):
        @pl.when(i != j)
        def _():
            act(pltpu.make_async_copy(src, c_ref.at[pl.ds(i * CH, CH), s, :, pl.ds(pl.multiple_of(j * TILE, TILE), TILE)], sem))

        @pl.when(i == j)
        def _():
            for q in range(CH):
                act(pltpu.make_async_copy(
                    src.at[pl.ds(q, CH - q), :, pl.ds(q * BLOCK, BLOCK)],
                    c_ref.at[pl.ds(i * CH + q, CH - q), s, :, pl.ds(pl.multiple_of(j * TILE + q * BLOCK, BLOCK), BLOCK)], sem))

    def put_panel(n, act):
        i, j, cls = pick(n, PANELS)
        put(t_ref.at[n], i, j, jnp.where(cls == 0, x, 1 - x), tsem, act)

    def put_job(n, act):
        i, j = pick(n, LATER)
        b = lax.rem(n, NBUF)
        put(obuf.at[b], i, j, 1 - x, osem.at[b], act)

    def start(cp):
        cp.start()

    def wait(cp):
        cp.wait()

    for n in range(LEAD):
        put_panel(jnp.int32(n), start)

    def body(n, _):
        i, j = pick(n, LATER)
        b = lax.rem(n, NBUF)

        @pl.when(n >= NBUF)
        def _():
            put_job(n - NBUF, wait)

        @pl.when(i != j)
        def _():
            full_tile(obuf.at[b], o_ref, (), i, sc_ref, (side,), j)

        @pl.when(i == j)
        def _():
            diag_tile(obuf.at[b], o_ref, (), sc_ref, (side,), j, 2 * (1 - x) + y, col)
        put_job(n, start)

        @pl.when(n + LEAD < len(PANELS))
        def _():
            put_panel(jnp.minimum(n + LEAD, len(PANELS) - 1), start)
        return 0

    lax.fori_loop(0, len(LATER), body, 0)
    last_slot = len(LATER) % NBUF
    put_job(jnp.int32(len(LATER) - NBUF), wait)
    diag_tile(obuf.at[last_slot], sc_ref, (0,), sc_ref, (side,), LAST[1], 2 * x + y, col)
    put(obuf.at[last_slot], jnp.int32(LAST[0]), jnp.int32(LAST[1]), x, osem.at[last_slot], start)

    def drain(n, _):
        put_panel(n, wait)

        @pl.when(jnp.logical_and(n > len(LATER) - NBUF, n < len(LATER)))
        def _():
            put_job(jnp.minimum(n, len(LATER) - 1), wait)
        return 0
    lax.fori_loop(0, len(PANELS), drain, 0)
    put(obuf.at[last_slot], jnp.int32(LAST[0]), jnp.int32(LAST[1]), x, osem.at[last_slot], wait)


def solution(mesh):
    def local_fn(a):
        a4 = pltpu.with_memory_space_constraint(a.reshape(NM, 2, BLOCK, PIECE), pltpu.HBM)
        any_spec = pl.BlockSpec(memory_space=pl.ANY)
        hbm = pl.BlockSpec(memory_space=pltpu.HBM)
        vmem = pl.BlockSpec(memory_space=pltpu.VMEM)
        dma = pltpu.SemaphoreType.DMA
        half_flops = 136 * 2 * BLOCK * BLOCK * K_DIM
        panels = pltpu.VMEM((2, PIECES, NM, BLOCK, PIECE), jnp.bfloat16)
        token = jax.ShapeDtypeStruct((8, 128), jnp.float32)
        sc, first = pl.pallas_call(
            first_kernel,
            out_shape=[panels, token],
            in_specs=[hbm],
            out_specs=[vmem, vmem],
            scratch_shapes=[pltpu.VMEM((2, HEAD, BLOCK, PIECE), jnp.bfloat16)] + [dma((2,))] * 5,
            compiler_params=pltpu.CompilerParams(collective_id=0, has_side_effects=True, vmem_limit_bytes=2 * 1024 * 1024),
        )(a4)
        rest = pltpu.VMEM((PIECES, NM, BLOCK, PIECE), jnp.bfloat16)
        c, zeroed, sc, o = pl.pallas_call(
            zero_kernel,
            out_shape=[jax.ShapeDtypeStruct((NM, 2, BLOCK, NM * BLOCK), jnp.bfloat16), token, panels, rest],
            in_specs=[any_spec, hbm, vmem],
            out_specs=[any_spec, vmem, vmem, vmem],
            input_output_aliases={2: 2},
            scratch_shapes=[pltpu.VMEM((CH, BLOCK, TILE), jnp.bfloat16), dma(()), dma(())],
            compiler_params=pltpu.CompilerParams(vmem_limit_bytes=4 * 1024 * 1024),
            cost_estimate=pl.CostEstimate(flops=half_flops, bytes_accessed=30 << 20, transcendentals=0),
        )(first, a4, sc)
        sc, o, t = pl.pallas_call(
            gather_kernel,
            out_shape=[panels, rest,
                       pltpu.VMEM((len(PANELS), CH, BLOCK, TILE), jnp.bfloat16)],
            in_specs=[vmem, vmem, any_spec],
            out_specs=[vmem] * 3,
            input_output_aliases={0: 0, 1: 1},
            scratch_shapes=[pltpu.VMEM((NM, BLOCK, PIECE), jnp.bfloat16), pltpu.VMEM((NR * CH, BLOCK, PIECE), jnp.bfloat16),
                            pltpu.SemaphoreType.REGULAR,
                            dma((NC + 1,)), dma((NC + 1,)), dma((NX,)), dma((NX,)), dma((NX,)), dma((NX,)),
                            dma((NC,)), dma((2, NC)), dma((NC + 1,)), dma((NC + 1,)), dma(()), dma(())] + [dma(())] * 4,
            compiler_params=pltpu.CompilerParams(collective_id=1, has_side_effects=True, vmem_limit_bytes=8 * 1024 * 1024),
            cost_estimate=pl.CostEstimate(flops=half_flops, bytes_accessed=2 << 20, transcendentals=0),
        )(sc, o, zeroed)
        c = pl.pallas_call(
            write_kernel,
            out_shape=jax.ShapeDtypeStruct((NM, 2, BLOCK, NM * BLOCK), jnp.bfloat16),
            in_specs=[vmem] * 3 + [any_spec],
            out_specs=any_spec,
            input_output_aliases={3: 0},
            scratch_shapes=[pltpu.VMEM((NBUF, CH, BLOCK, TILE), jnp.bfloat16), dma(()), dma((NBUF,))],
            compiler_params=pltpu.CompilerParams(vmem_limit_bytes=15 * 1024 * 1024),
            cost_estimate=pl.CostEstimate(flops=half_flops, bytes_accessed=34 << 20, transcendentals=0),
        )(sc, o, t, c)
        return c.reshape(2 * NM * BLOCK, NM * BLOCK)

    spec = P(('batch', 'row'), 'col')
    return jax.shard_map(local_fn, mesh=mesh, in_specs=(spec,), out_specs=spec, check_vma=False)
```

```python
import functools
import jax
import jax.numpy as jnp
from jax import lax
from jax.experimental import pallas as pl
from jax.experimental.pallas import tpu as pltpu
from jax.sharding import PartitionSpec as P

BLOCK = 256
K_DIM = 512
PIECE = 128
PIECES = K_DIM // PIECE
NM = 16
CH = 4
NC = NM // CH
NBUF = 5
LEAD = 5
TILE = CH * BLOCK
JOBS = [(i, j) for j in range(NC) for i in range(j, NC)]
LAST = (NC - 1, NC - 1)
NOW = [job for job in JOBS if job != LAST]
NAX, NAY = 15, 15
NR = 2
O_PARTS = ((12, 4), (0, 4), (4, 4), (8, 3), (11, 1))
NX = NC + len(O_PARTS)
EXTRA = [(3, 0), (3, 1), (3, 2)]
LATER = [job for job in JOBS if job not in EXTRA]
PANELS = [(i, j, 0) for i, j in NOW] + [(i, j, 1) for i, j in EXTRA]


def positions():
    y = lax.axis_index('row')
    col = lax.axis_index('col')
    return y, col // 2, col % 2, col


def chunk(c):
    return pl.ds(c * CH, CH)


def panel(ref, lead, first, count):
    parts = [ref[(*lead, p, pl.ds(first, count))].reshape(count * BLOCK, PIECE) for p in range(PIECES)]
    return jnp.concatenate(parts, axis=1)


def dot_t(rows, cols):
    return lax.dot_general(rows, cols, (((1,), (1,)), ((), ())), preferred_element_type=jnp.float32)


def full_tile(out, row_ref, row_lead, i, col_ref, col_lead, j):
    prod = dot_t(panel(row_ref, row_lead, i * CH, CH), panel(col_ref, col_lead, j * CH, CH))
    out[...] = prod.astype(jnp.bfloat16).reshape(CH, BLOCK, TILE)


def diag_tile(out, row_ref, row_lead, col_ref, col_lead, j, row_blk, col_blk):
    for q in range(CH):
        prod = dot_t(panel(row_ref, row_lead, j * CH + q, CH - q), panel(col_ref, col_lead, j * CH + q, 1))
        row_id = lax.broadcasted_iota(jnp.int32, (BLOCK, BLOCK), 0) + row_blk * BLOCK
        col_id = lax.broadcasted_iota(jnp.int32, (BLOCK, BLOCK), 1) + col_blk * BLOCK
        lanes = slice(q * BLOCK, (q + 1) * BLOCK)
        out[q, :, lanes] = jnp.where(row_id >= col_id, prod[:BLOCK], 0.0).astype(jnp.bfloat16)
        if q + 1 < CH:
            out[q + 1:, :, lanes] = prod[BLOCK:].astype(jnp.bfloat16).reshape(CH - q - 1, BLOCK, BLOCK)


MESH_ID = pl.DeviceIdType.MESH


def remote(src, dst, send, recv, dev):
    return pltpu.make_async_remote_copy(src, dst, send, recv, device_id=dev, device_id_type=MESH_ID)


def signal(sem, devices):
    for dev in devices:
        pl.semaphore_signal(sem, inc=1, device_id=dev, device_id_type=MESH_ID)


def first_kernel(a_ref, sc_ref, token_ref, x_send, x_recv, y_send, y_recv):
    y, x, k, _ = positions()
    token_ref[...] = jnp.zeros_like(token_ref)

    @pl.when(k != y)
    def _():
        x_peer = (0, y, 2 * (1 - x) + k)
        y_peer = (0, 1 - y, 2 * x + y)
        barrier = pltpu.get_barrier_semaphore()
        signal(barrier, (x_peer, y_peer))
        pl.semaphore_wait(barrier, 2)
        px, py = pl.ds(0, NAX), pl.ds(0, NAY)
        xc = remote(a_ref.at[px, 1 - x], sc_ref.at[0, 2, px], x_send, x_recv, x_peer)
        yc = remote(a_ref.at[py, x], sc_ref.at[1, 1, py], y_send, y_recv, y_peer)
        xc.start()
        yc.start()
        xc.wait()
        yc.wait()


def zero_kernel(token_ref, a_ref, sc_in, c_ref, done_ref, sc_ref, o_ref, zbuf, sem, lsem):
    _, x, _, _ = positions()
    loads = [pltpu.make_async_copy(a_ref.at[:, 1 - x], o_ref.at[0], lsem),
             pltpu.make_async_copy(a_ref.at[:, x], sc_ref.at[0, 0], lsem)]
    for cp in loads:
        cp.start()
    zbuf[...] = jnp.zeros_like(zbuf)
    done_ref[...] = jnp.zeros_like(done_ref)
    copies = []
    for s in range(2):
        for i in range(NC):
            for j in range(i + 1, NC):
                copies.append(pltpu.make_async_copy(zbuf, c_ref.at[chunk(i), s, :, pl.ds(j * TILE, TILE)], sem))
            for q in range(1, CH):
                copies.append(pltpu.make_async_copy(
                    zbuf.at[pl.ds(0, q), :, pl.ds(0, BLOCK)],
                    c_ref.at[pl.ds(i * CH, q), s, :, pl.ds((i * CH + q) * BLOCK, BLOCK)], sem))
    for cp in copies:
        cp.start()
    for cp in copies + loads:
        cp.wait()


def gather_kernel(sc_in, o_in, token_ref, sc_ref, o_ref, t_ref, yb, yr, join, d_send, d_recv, x_send, x_recv, r_send, r_recv,
                  y_send, y_recv, b_send, b_recv, q_send, q_recv, u_send, u_recv, v_send, v_recv):
    y, x, k, col = positions()
    late = k != y
    early = k == y
    side = jnp.where(late, 1, 0)
    partner = (0, y, 2 * x + 1 - k)
    x_peer = (0, y, 2 * (1 - x) + k)
    y_early = (0, 1 - y, 2 * x + 1 - y)
    y_late = (0, 1 - y, 2 * x + y)
    tx, ty = pl.ds(NAX, NM - NAX), pl.ds(NAY, NM - NAY)

    def x_copy(n):
        if n < NC:
            part = pl.ds(n * NM // 2, NM // 2)
            return remote(o_ref.at[0, part], sc_ref.at[0, 2, part], x_send.at[n], x_recv.at[n], x_peer)
        part = pl.ds(*O_PARTS[n - NC])
        return remote(sc_ref.at[0, 0, part], o_ref.at[2, part], x_send.at[n], x_recv.at[n], x_peer)

    def relay_copy(n):
        if n < NC:
            return s_relay(n)
        part = pl.ds(*O_PARTS[n - NC])
        return remote(o_ref.at[2, part], o_ref.at[3, part], r_send.at[n], r_recv.at[n], partner)

    def y_copy(s, c):
        return remote(sc_ref.at[0, 2, chunk(c)], sc_ref.at[1, 2 + s, chunk(c)], y_send.at[c], y_recv.at[s, c], y_late)

    def s_relay(c):
        return remote(sc_ref.at[0, 2, chunk(c)], sc_ref.at[0, 3, chunk(c)], r_send.at[c], r_recv.at[c], partner)

    def s_copy(c):
        return remote(sc_ref.at[0, 0, chunk(c)], sc_ref.at[0, 1, chunk(c)], d_send.at[c], d_recv.at[c], partner)

    def yb_relay(c):
        return remote(yb.at[chunk(c)], sc_ref.at[1, 0, chunk(c)], b_send.at[1 + c], b_recv.at[1 + c], partner)

    def yr_relay(c):
        return remote(yr.at[chunk(c)], sc_ref.at[1, 2, chunk(c)], y_send.at[c], y_recv.at[0, c], partner)

    yr_part = pl.ds(0, NR * CH)
    yr_copy = remote(sc_ref.at[0, 2, yr_part], yr, q_send, q_recv, y_early)
    yb_copy = remote(sc_ref.at[0, 0], yb, b_send.at[0], b_recv.at[0], y_early)
    x_tail = remote(o_ref.at[0, tx], sc_ref.at[0, 2, tx], v_send, v_recv, x_peer)
    u_copy = remote(sc_ref.at[0, 0, ty], sc_ref.at[1, 1, ty], u_send, u_recv, y_late)
    o_copy = remote(o_ref.at[0], o_ref.at[1], d_send.at[NC], d_recv.at[NC], partner)
    barrier = pltpu.get_barrier_semaphore()

    @pl.when(early)
    def _():
        signal(barrier, (x_peer, y_early, partner, y_late))
        pl.semaphore_wait(barrier, 2)
        for n in (0, 1, *range(NC, NX)):
            x_copy(n).start()
        yb_copy.start()
        x_copy(0).wait_recv()
        yr_copy.start()
        pl.semaphore_wait(join, 2)
        for c in range(NC):
            if c == NR:
                x_copy(1).wait_recv()
            s_copy(c).start()
            relay_copy(c).start()
            if c == 0:
                yb_copy.wait_recv()
                yb_relay(c).start()
        for c in range(NC):
            if c == 0:
                yr_copy.wait_recv()
            if c < NR:
                yr_relay(c).start()
            if c + 1 < NC:
                yb_relay(c + 1).start()
        o_copy.start()

    @pl.when(late)
    def _():
        signal(barrier, (x_peer, y_late))
        pl.semaphore_wait(barrier, 4)
        signal(join, (partner, y_early))
        x_tail.start()
        for n in range(NC, NX):
            x_copy(n).start()
        for c in range(NC - 1):
            y_copy(1, c).start()
        u_copy.start()
        for c in range(NC):
            s_copy(c).start()
            if c < NC - 1:
                relay_copy(c).start()
        o_copy.start()
        x_tail.wait_recv()
        relay_copy(NC - 1).start()
        y_copy(1, NC - 1).start()

    def rows_ready(i):
        s_copy(i).wait_recv()
        s_relay(i).wait_recv()

    def o_step(n):
        x_copy(NC + n).wait_recv()
        relay_copy(NC + n).start()

    rows_ready(0)
    row_blk = 2 * x + y
    for c in range(NC):
        if c == NC - 1:
            o_step(len(O_PARTS) - 1)

        @pl.when(early)
        def _():
            if c in (0, 2):
                y_copy(0, NR + c // 2).start()

        @pl.when(late)
        def _():
            yb_relay(c).wait_recv()
            if c == NC - 1:
                u_copy.wait_recv()
            for s in range(2):
                y_copy(s, c).wait_recv()

        if c < NC - 1:
            base = NOW.index((c, c))
            diag_tile(t_ref.at[base], sc_ref, (0,), sc_ref, (side,), c, row_blk, col)

            def body(i, _):
                if c == 0:
                    rows_ready(i)
                full_tile(t_ref.at[base + i - c], sc_ref, (0,), i, sc_ref, (side,), c)
                return 0
            lax.fori_loop(c + 1, NC, body, 0)
            o_step(c)
        if c == 1:
            o_copy.wait_recv()
            relay_copy(NC).wait_recv()
        if c == 2:
            o_step(c + 1)
        for m, (i, j) in enumerate(EXTRA):
            if c == max(j, 1):
                full_tile(t_ref.at[len(NOW) + m], o_ref, (), i, sc_ref, (side,), j)

    for n in range(1, len(O_PARTS)):
        relay_copy(NC + n).wait_recv()
    for n in range(NX):
        relay_copy(n).wait_send()
    for n in range(NC, NX):
        x_copy(n).wait_send()
    for c in range(NC):
        s_copy(c).wait_send()
        y_copy(0, c).wait_send()
    o_copy.wait_send()

    @pl.when(late)
    def _():
        u_copy.wait_send()
        x_tail.wait_send()

    @pl.when(early)
    def _():
        for n in range(2):
            x_copy(n).wait_send()
        yr_copy.wait_send()
        yb_copy.wait_send()
        for c in range(NC):
            yb_relay(c).wait_send()


def lookup(n, values):
    out = jnp.int32(values[-1])
    for m in range(len(values) - 2, -1, -1):
        out = jnp.where(n == m, jnp.int32(values[m]), out)
    return out


def write_kernel(sc_ref, o_ref, t_ref, c_in, c_ref, obuf, tsem, osem):
    y, x, k, col = positions()
    side = jnp.where(k != y, 1, 0)

    def pick(n, values):
        return [lookup(n, column) for column in zip(*values)]

    def put(src, i, j, s, sem, act):
        @pl.when(i != j)
        def _():
            act(pltpu.make_async_copy(src, c_ref.at[pl.ds(i * CH, CH), s, :, pl.ds(pl.multiple_of(j * TILE, TILE), TILE)], sem))

        @pl.when(i == j)
        def _():
            for q in range(CH):
                act(pltpu.make_async_copy(
                    src.at[pl.ds(q, CH - q), :, pl.ds(q * BLOCK, BLOCK)],
                    c_ref.at[pl.ds(i * CH + q, CH - q), s, :, pl.ds(pl.multiple_of(j * TILE + q * BLOCK, BLOCK), BLOCK)], sem))

    def put_panel(n, act):
        i, j, cls = pick(n, PANELS)
        put(t_ref.at[n], i, j, jnp.where(cls == 0, x, 1 - x), tsem, act)

    def put_job(n, act):
        i, j = pick(n, LATER)
        b = lax.rem(n, NBUF)
        put(obuf.at[b], i, j, 1 - x, osem.at[b], act)

    def start(cp):
        cp.start()

    def wait(cp):
        cp.wait()

    for n in range(LEAD):
        put_panel(jnp.int32(n), start)

    def body(n, _):
        i, j = pick(n, LATER)
        b = lax.rem(n, NBUF)

        @pl.when(n >= NBUF)
        def _():
            put_job(n - NBUF, wait)

        @pl.when(i != j)
        def _():
            full_tile(obuf.at[b], o_ref, (), i, sc_ref, (side,), j)

        @pl.when(i == j)
        def _():
            diag_tile(obuf.at[b], o_ref, (), sc_ref, (side,), j, 2 * (1 - x) + y, col)
        put_job(n, start)

        @pl.when(n + LEAD < len(PANELS))
        def _():
            put_panel(jnp.minimum(n + LEAD, len(PANELS) - 1), start)
        return 0

    lax.fori_loop(0, len(LATER), body, 0)
    last_slot = len(LATER) % NBUF
    put_job(jnp.int32(len(LATER) - NBUF), wait)
    diag_tile(obuf.at[last_slot], sc_ref, (0,), sc_ref, (side,), LAST[1], 2 * x + y, col)
    put(obuf.at[last_slot], jnp.int32(LAST[0]), jnp.int32(LAST[1]), x, osem.at[last_slot], start)

    def drain(n, _):
        put_panel(n, wait)

        @pl.when(jnp.logical_and(n > len(LATER) - NBUF, n < len(LATER)))
        def _():
            put_job(jnp.minimum(n, len(LATER) - 1), wait)
        return 0
    lax.fori_loop(0, len(PANELS), drain, 0)
    put(obuf.at[last_slot], jnp.int32(LAST[0]), jnp.int32(LAST[1]), x, osem.at[last_slot], wait)


def solution(mesh):
    def local_fn(a):
        a4 = pltpu.with_memory_space_constraint(a.reshape(NM, 2, BLOCK, PIECE), pltpu.HBM)
        any_spec = pl.BlockSpec(memory_space=pl.ANY)
        hbm = pl.BlockSpec(memory_space=pltpu.HBM)
        vmem = pl.BlockSpec(memory_space=pltpu.VMEM)
        dma = pltpu.SemaphoreType.DMA
        half_flops = 136 * 2 * BLOCK * BLOCK * K_DIM
        panels = pltpu.VMEM((2, PIECES, NM, BLOCK, PIECE), jnp.bfloat16)
        token = jax.ShapeDtypeStruct((8, 128), jnp.float32)
        sc, first = pl.pallas_call(
            first_kernel,
            out_shape=[panels, token],
            in_specs=[hbm],
            out_specs=[vmem, vmem],
            scratch_shapes=[dma(())] * 4,
            compiler_params=pltpu.CompilerParams(collective_id=0, has_side_effects=True, vmem_limit_bytes=2 * 1024 * 1024),
        )(a4)
        rest = pltpu.VMEM((PIECES, NM, BLOCK, PIECE), jnp.bfloat16)
        c, zeroed, sc, o = pl.pallas_call(
            zero_kernel,
            out_shape=[jax.ShapeDtypeStruct((NM, 2, BLOCK, NM * BLOCK), jnp.bfloat16), token, panels, rest],
            in_specs=[any_spec, hbm, vmem],
            out_specs=[any_spec, vmem, vmem, vmem],
            input_output_aliases={2: 2},
            scratch_shapes=[pltpu.VMEM((CH, BLOCK, TILE), jnp.bfloat16), dma(()), dma(())],
            compiler_params=pltpu.CompilerParams(vmem_limit_bytes=4 * 1024 * 1024),
            cost_estimate=pl.CostEstimate(flops=half_flops, bytes_accessed=30 << 20, transcendentals=0),
        )(first, a4, sc)
        sc, o, t = pl.pallas_call(
            gather_kernel,
            out_shape=[panels, rest,
                       pltpu.VMEM((len(PANELS), CH, BLOCK, TILE), jnp.bfloat16)],
            in_specs=[vmem, vmem, any_spec],
            out_specs=[vmem] * 3,
            input_output_aliases={0: 0, 1: 1},
            scratch_shapes=[pltpu.VMEM((NM, BLOCK, PIECE), jnp.bfloat16), pltpu.VMEM((NR * CH, BLOCK, PIECE), jnp.bfloat16),
                            pltpu.SemaphoreType.REGULAR,
                            dma((NC + 1,)), dma((NC + 1,)), dma((NX,)), dma((NX,)), dma((NX,)), dma((NX,)),
                            dma((NC,)), dma((2, NC)), dma((NC + 1,)), dma((NC + 1,)), dma(()), dma(())] + [dma(())] * 4,
            compiler_params=pltpu.CompilerParams(collective_id=1, has_side_effects=True, vmem_limit_bytes=8 * 1024 * 1024),
            cost_estimate=pl.CostEstimate(flops=half_flops, bytes_accessed=2 << 20, transcendentals=0),
        )(sc, o, zeroed)
        c = pl.pallas_call(
            write_kernel,
            out_shape=jax.ShapeDtypeStruct((NM, 2, BLOCK, NM * BLOCK), jnp.bfloat16),
            in_specs=[vmem] * 3 + [any_spec],
            out_specs=any_spec,
            input_output_aliases={3: 0},
            scratch_shapes=[pltpu.VMEM((NBUF, CH, BLOCK, TILE), jnp.bfloat16), dma(()), dma((NBUF,))],
            compiler_params=pltpu.CompilerParams(vmem_limit_bytes=15 * 1024 * 1024),
            cost_estimate=pl.CostEstimate(flops=half_flops, bytes_accessed=34 << 20, transcendentals=0),
        )(sc, o, t, c)
        return c.reshape(2 * NM * BLOCK, NM * BLOCK)

    spec = P(('batch', 'row'), 'col')
    return jax.shard_map(local_fn, mesh=mesh, in_specs=(spec,), out_specs=spec, check_vma=False)
```

```python
import functools
import jax
import jax.numpy as jnp
from jax import lax
from jax.experimental import pallas as pl
from jax.experimental.pallas import tpu as pltpu
from jax.sharding import PartitionSpec as P

BLOCK = 256
K_DIM = 512
PIECE = 128
PIECES = K_DIM // PIECE
NM = 16
CH = 4
NC = NM // CH
NBUF = 5
LEAD = 4
TILE = CH * BLOCK
JOBS = [(i, j) for j in range(NC) for i in range(j, NC)]
LAST = (NC - 1, NC - 1)
NOW = [job for job in JOBS if job != LAST]
NAX, NAY = 15, 15
NR = 2
O_PARTS = ((12, 4), (0, 4), (4, 4), (8, 3), (11, 1))
NX = NC + len(O_PARTS)
EXTRA = [(3, 0), (3, 1)]
LATER = [job for job in JOBS if job not in EXTRA]
PANELS = [(i, j, 0) for i, j in NOW] + [(i, j, 1) for i, j in EXTRA]


def positions():
    y = lax.axis_index('row')
    col = lax.axis_index('col')
    return y, col // 2, col % 2, col


def chunk(c):
    return pl.ds(c * CH, CH)


def panel(ref, lead, first, count):
    parts = [ref[(*lead, p, pl.ds(first, count))].reshape(count * BLOCK, PIECE) for p in range(PIECES)]
    return jnp.concatenate(parts, axis=1)


def dot_t(rows, cols):
    return lax.dot_general(rows, cols, (((1,), (1,)), ((), ())), preferred_element_type=jnp.float32)


def full_tile(out, row_ref, row_lead, i, col_ref, col_lead, j):
    prod = dot_t(panel(row_ref, row_lead, i * CH, CH), panel(col_ref, col_lead, j * CH, CH))
    out[...] = prod.astype(jnp.bfloat16).reshape(CH, BLOCK, TILE)


def diag_tile(out, row_ref, row_lead, col_ref, col_lead, j, row_blk, col_blk):
    for q in range(CH):
        prod = dot_t(panel(row_ref, row_lead, j * CH + q, CH - q), panel(col_ref, col_lead, j * CH + q, 1))
        row_id = lax.broadcasted_iota(jnp.int32, (BLOCK, BLOCK), 0) + row_blk * BLOCK
        col_id = lax.broadcasted_iota(jnp.int32, (BLOCK, BLOCK), 1) + col_blk * BLOCK
        lanes = slice(q * BLOCK, (q + 1) * BLOCK)
        out[q, :, lanes] = jnp.where(row_id >= col_id, prod[:BLOCK], 0.0).astype(jnp.bfloat16)
        if q + 1 < CH:
            out[q + 1:, :, lanes] = prod[BLOCK:].astype(jnp.bfloat16).reshape(CH - q - 1, BLOCK, BLOCK)


MESH_ID = pl.DeviceIdType.MESH


def remote(src, dst, send, recv, dev):
    return pltpu.make_async_remote_copy(src, dst, send, recv, device_id=dev, device_id_type=MESH_ID)


def signal(sem, devices):
    for dev in devices:
        pl.semaphore_signal(sem, inc=1, device_id=dev, device_id_type=MESH_ID)


def first_kernel(a_ref, sc_ref, token_ref, x_send, x_recv, y_send, y_recv):
    y, x, k, _ = positions()
    token_ref[...] = jnp.zeros_like(token_ref)

    @pl.when(k != y)
    def _():
        x_peer = (0, y, 2 * (1 - x) + k)
        y_peer = (0, 1 - y, 2 * x + y)
        barrier = pltpu.get_barrier_semaphore()
        signal(barrier, (x_peer, y_peer))
        pl.semaphore_wait(barrier, 2)
        px, py = pl.ds(0, NAX), pl.ds(0, NAY)
        xc = remote(a_ref.at[px, 1 - x], sc_ref.at[0, 2, px], x_send, x_recv, x_peer)
        yc = remote(a_ref.at[py, x], sc_ref.at[1, 1, py], y_send, y_recv, y_peer)
        xc.start()
        yc.start()
        xc.wait()
        yc.wait()


def zero_kernel(token_ref, a_ref, sc_in, c_ref, done_ref, sc_ref, o_ref, zbuf, sem, lsem):
    _, x, _, _ = positions()
    loads = [pltpu.make_async_copy(a_ref.at[:, 1 - x], o_ref.at[0], lsem),
             pltpu.make_async_copy(a_ref.at[:, x], sc_ref.at[0, 0], lsem)]
    for cp in loads:
        cp.start()
    zbuf[...] = jnp.zeros_like(zbuf)
    done_ref[...] = jnp.zeros_like(done_ref)
    copies = []
    for s in range(2):
        for i in range(NC):
            for j in range(i + 1, NC):
                copies.append(pltpu.make_async_copy(zbuf, c_ref.at[chunk(i), s, :, pl.ds(j * TILE, TILE)], sem))
            for q in range(1, CH):
                copies.append(pltpu.make_async_copy(
                    zbuf.at[pl.ds(0, q), :, pl.ds(0, BLOCK)],
                    c_ref.at[pl.ds(i * CH, q), s, :, pl.ds((i * CH + q) * BLOCK, BLOCK)], sem))
    for cp in copies:
        cp.start()
    for cp in copies + loads:
        cp.wait()


def gather_kernel(sc_in, o_in, token_ref, sc_ref, o_ref, t_ref, yb, yr, join, d_send, d_recv, x_send, x_recv, r_send, r_recv,
                  y_send, y_recv, b_send, b_recv, q_send, q_recv, u_send, u_recv, v_send, v_recv):
    y, x, k, col = positions()
    late = k != y
    early = k == y
    side = jnp.where(late, 1, 0)
    partner = (0, y, 2 * x + 1 - k)
    x_peer = (0, y, 2 * (1 - x) + k)
    y_early = (0, 1 - y, 2 * x + 1 - y)
    y_late = (0, 1 - y, 2 * x + y)
    tx, ty = pl.ds(NAX, NM - NAX), pl.ds(NAY, NM - NAY)

    def x_copy(n):
        if n < NC:
            part = pl.ds(n * NM // 2, NM // 2)
            return remote(o_ref.at[0, part], sc_ref.at[0, 2, part], x_send.at[n], x_recv.at[n], x_peer)
        part = pl.ds(*O_PARTS[n - NC])
        return remote(sc_ref.at[0, 0, part], o_ref.at[2, part], x_send.at[n], x_recv.at[n], x_peer)

    def relay_copy(n):
        if n < NC:
            return s_relay(n)
        part = pl.ds(*O_PARTS[n - NC])
        return remote(o_ref.at[2, part], o_ref.at[3, part], r_send.at[n], r_recv.at[n], partner)

    def y_copy(s, c):
        return remote(sc_ref.at[0, 2, chunk(c)], sc_ref.at[1, 2 + s, chunk(c)], y_send.at[c], y_recv.at[s, c], y_late)

    def s_relay(c):
        return remote(sc_ref.at[0, 2, chunk(c)], sc_ref.at[0, 3, chunk(c)], r_send.at[c], r_recv.at[c], partner)

    def s_copy(c):
        return remote(sc_ref.at[0, 0, chunk(c)], sc_ref.at[0, 1, chunk(c)], d_send.at[c], d_recv.at[c], partner)

    def yb_relay(c):
        return remote(yb.at[chunk(c)], sc_ref.at[1, 0, chunk(c)], b_send.at[1 + c], b_recv.at[1 + c], partner)

    def yr_relay(c):
        return remote(yr.at[chunk(c)], sc_ref.at[1, 2, chunk(c)], y_send.at[c], y_recv.at[0, c], partner)

    yr_part = pl.ds(0, NR * CH)
    yr_copy = remote(sc_ref.at[0, 2, yr_part], yr, q_send, q_recv, y_early)
    yb_copy = remote(sc_ref.at[0, 0], yb, b_send.at[0], b_recv.at[0], y_early)
    x_tail = remote(o_ref.at[0, tx], sc_ref.at[0, 2, tx], v_send, v_recv, x_peer)
    u_copy = remote(sc_ref.at[0, 0, ty], sc_ref.at[1, 1, ty], u_send, u_recv, y_late)
    o_copy = remote(o_ref.at[0], o_ref.at[1], d_send.at[NC], d_recv.at[NC], partner)
    barrier = pltpu.get_barrier_semaphore()

    @pl.when(early)
    def _():
        signal(barrier, (x_peer, y_early, partner, y_late))
        pl.semaphore_wait(barrier, 2)
        for n in (0, 1, *range(NC, NX)):
            x_copy(n).start()
        yb_copy.start()
        x_copy(0).wait_recv()
        yr_copy.start()
        pl.semaphore_wait(join, 2)
        for c in range(NC):
            if c == NR:
                x_copy(1).wait_recv()
            s_copy(c).start()
            relay_copy(c).start()
            if c == 0:
                yb_copy.wait_recv()
                yb_relay(c).start()
        for c in range(NC):
            if c == 0:
                yr_copy.wait_recv()
            if c < NR:
                yr_relay(c).start()
            if c + 1 < NC:
                yb_relay(c + 1).start()
        o_copy.start()

    @pl.when(late)
    def _():
        signal(barrier, (x_peer, y_late))
        pl.semaphore_wait(barrier, 4)
        signal(join, (partner, y_early))
        x_tail.start()
        for c in range(NC - 1):
            y_copy(1, c).start()
        u_copy.start()
        for c in range(NC):
            s_copy(c).start()
            if c < NC - 1:
                relay_copy(c).start()
        o_copy.start()
        x_tail.wait_recv()
        relay_copy(NC - 1).start()
        y_copy(1, NC - 1).start()

    def rows_ready(i):
        s_copy(i).wait_recv()
        s_relay(i).wait_recv()

    def o_step(n):
        x_copy(NC + n).wait_recv()
        relay_copy(NC + n).start()

    rows_ready(0)
    row_blk = 2 * x + y
    for c in range(NC):
        if c == NC - 1:
            o_step(len(O_PARTS) - 1)

        @pl.when(early)
        def _():
            if c in (0, 2):
                y_copy(0, NR + c // 2).start()

        @pl.when(late)
        def _():
            yb_relay(c).wait_recv()
            if c == NC - 1:
                u_copy.wait_recv()
            for s in range(2):
                y_copy(s, c).wait_recv()

        if c < NC - 1:
            base = NOW.index((c, c))
            diag_tile(t_ref.at[base], sc_ref, (0,), sc_ref, (side,), c, row_blk, col)
            if c == 0:
                @pl.when(late)
                def _():
                    for n in range(NC, NX):
                        x_copy(n).start()

            def body(i, _):
                if c == 0:
                    rows_ready(i)
                full_tile(t_ref.at[base + i - c], sc_ref, (0,), i, sc_ref, (side,), c)
                return 0
            lax.fori_loop(c + 1, NC, body, 0)
            o_step(c)
        if c == 1:
            o_copy.wait_recv()
            relay_copy(NC).wait_recv()
            for m, (i, j) in enumerate(EXTRA):
                full_tile(t_ref.at[len(NOW) + m], o_ref, (), i, sc_ref, (side,), j)
        if c == 2:
            o_step(c + 1)

    for n in range(1, len(O_PARTS)):
        relay_copy(NC + n).wait_recv()
    for n in range(NX):
        relay_copy(n).wait_send()
    for n in range(NC, NX):
        x_copy(n).wait_send()
    for c in range(NC):
        s_copy(c).wait_send()
        y_copy(0, c).wait_send()
    o_copy.wait_send()

    @pl.when(late)
    def _():
        u_copy.wait_send()
        x_tail.wait_send()

    @pl.when(early)
    def _():
        for n in range(2):
            x_copy(n).wait_send()
        yr_copy.wait_send()
        yb_copy.wait_send()
        for c in range(NC):
            yb_relay(c).wait_send()


def lookup(n, values):
    out = jnp.int32(values[-1])
    for m in range(len(values) - 2, -1, -1):
        out = jnp.where(n == m, jnp.int32(values[m]), out)
    return out


def write_kernel(sc_ref, o_ref, t_ref, c_in, c_ref, obuf, tsem, osem):
    y, x, k, col = positions()
    side = jnp.where(k != y, 1, 0)

    def pick(n, values):
        return [lookup(n, column) for column in zip(*values)]

    def put(src, i, j, s, sem, act):
        @pl.when(i != j)
        def _():
            act(pltpu.make_async_copy(src, c_ref.at[pl.ds(i * CH, CH), s, :, pl.ds(pl.multiple_of(j * TILE, TILE), TILE)], sem))

        @pl.when(i == j)
        def _():
            for q in range(CH):
                act(pltpu.make_async_copy(
                    src.at[pl.ds(q, CH - q), :, pl.ds(q * BLOCK, BLOCK)],
                    c_ref.at[pl.ds(i * CH + q, CH - q), s, :, pl.ds(pl.multiple_of(j * TILE + q * BLOCK, BLOCK), BLOCK)], sem))

    def put_panel(n, act):
        i, j, cls = pick(n, PANELS)
        put(t_ref.at[n], i, j, jnp.where(cls == 0, x, 1 - x), tsem, act)

    def put_job(n, act):
        i, j = pick(n, LATER)
        b = lax.rem(n, NBUF)
        put(obuf.at[b], i, j, 1 - x, osem.at[b], act)

    def start(cp):
        cp.start()

    def wait(cp):
        cp.wait()

    for n in range(LEAD):
        put_panel(jnp.int32(n), start)

    def body(n, _):
        i, j = pick(n, LATER)
        b = lax.rem(n, NBUF)

        @pl.when(n >= NBUF)
        def _():
            put_job(n - NBUF, wait)

        @pl.when(i != j)
        def _():
            full_tile(obuf.at[b], o_ref, (), i, sc_ref, (side,), j)

        @pl.when(i == j)
        def _():
            diag_tile(obuf.at[b], o_ref, (), sc_ref, (side,), j, 2 * (1 - x) + y, col)
        put_job(n, start)

        @pl.when(n + LEAD < len(PANELS))
        def _():
            put_panel(jnp.minimum(n + LEAD, len(PANELS) - 1), start)
        return 0

    lax.fori_loop(0, len(LATER), body, 0)
    last_slot = len(LATER) % NBUF
    put_job(jnp.int32(len(LATER) - NBUF), wait)
    diag_tile(obuf.at[last_slot], sc_ref, (0,), sc_ref, (side,), LAST[1], 2 * x + y, col)
    put(obuf.at[last_slot], jnp.int32(LAST[0]), jnp.int32(LAST[1]), x, osem.at[last_slot], start)

    def drain(n, _):
        put_panel(n, wait)

        @pl.when(jnp.logical_and(n > len(LATER) - NBUF, n < len(LATER)))
        def _():
            put_job(jnp.minimum(n, len(LATER) - 1), wait)
        return 0
    lax.fori_loop(0, len(PANELS), drain, 0)
    put(obuf.at[last_slot], jnp.int32(LAST[0]), jnp.int32(LAST[1]), x, osem.at[last_slot], wait)


def solution(mesh):
    def local_fn(a):
        a4 = pltpu.with_memory_space_constraint(a.reshape(NM, 2, BLOCK, PIECE), pltpu.HBM)
        any_spec = pl.BlockSpec(memory_space=pl.ANY)
        hbm = pl.BlockSpec(memory_space=pltpu.HBM)
        vmem = pl.BlockSpec(memory_space=pltpu.VMEM)
        dma = pltpu.SemaphoreType.DMA
        half_flops = 136 * 2 * BLOCK * BLOCK * K_DIM
        panels = pltpu.VMEM((2, PIECES, NM, BLOCK, PIECE), jnp.bfloat16)
        token = jax.ShapeDtypeStruct((8, 128), jnp.float32)
        sc, first = pl.pallas_call(
            first_kernel,
            out_shape=[panels, token],
            in_specs=[hbm],
            out_specs=[vmem, vmem],
            scratch_shapes=[dma(())] * 4,
            compiler_params=pltpu.CompilerParams(collective_id=0, has_side_effects=True, vmem_limit_bytes=2 * 1024 * 1024),
        )(a4)
        rest = pltpu.VMEM((PIECES, NM, BLOCK, PIECE), jnp.bfloat16)
        c, zeroed, sc, o = pl.pallas_call(
            zero_kernel,
            out_shape=[jax.ShapeDtypeStruct((NM, 2, BLOCK, NM * BLOCK), jnp.bfloat16), token, panels, rest],
            in_specs=[any_spec, hbm, vmem],
            out_specs=[any_spec, vmem, vmem, vmem],
            input_output_aliases={2: 2},
            scratch_shapes=[pltpu.VMEM((CH, BLOCK, TILE), jnp.bfloat16), dma(()), dma(())],
            compiler_params=pltpu.CompilerParams(vmem_limit_bytes=4 * 1024 * 1024),
            cost_estimate=pl.CostEstimate(flops=half_flops, bytes_accessed=30 << 20, transcendentals=0),
        )(first, a4, sc)
        sc, o, t = pl.pallas_call(
            gather_kernel,
            out_shape=[panels, rest,
                       pltpu.VMEM((len(PANELS), CH, BLOCK, TILE), jnp.bfloat16)],
            in_specs=[vmem, vmem, any_spec],
            out_specs=[vmem] * 3,
            input_output_aliases={0: 0, 1: 1},
            scratch_shapes=[pltpu.VMEM((NM, BLOCK, PIECE), jnp.bfloat16), pltpu.VMEM((NR * CH, BLOCK, PIECE), jnp.bfloat16),
                            pltpu.SemaphoreType.REGULAR,
                            dma((NC + 1,)), dma((NC + 1,)), dma((NX,)), dma((NX,)), dma((NX,)), dma((NX,)),
                            dma((NC,)), dma((2, NC)), dma((NC + 1,)), dma((NC + 1,)), dma(()), dma(())] + [dma(())] * 4,
            compiler_params=pltpu.CompilerParams(collective_id=1, has_side_effects=True, vmem_limit_bytes=8 * 1024 * 1024),
            cost_estimate=pl.CostEstimate(flops=half_flops, bytes_accessed=2 << 20, transcendentals=0),
        )(sc, o, zeroed)
        c = pl.pallas_call(
            write_kernel,
            out_shape=jax.ShapeDtypeStruct((NM, 2, BLOCK, NM * BLOCK), jnp.bfloat16),
            in_specs=[vmem] * 3 + [any_spec],
            out_specs=any_spec,
            input_output_aliases={3: 0},
            scratch_shapes=[pltpu.VMEM((NBUF, CH, BLOCK, TILE), jnp.bfloat16), dma(()), dma((NBUF,))],
            compiler_params=pltpu.CompilerParams(vmem_limit_bytes=15 * 1024 * 1024),
            cost_estimate=pl.CostEstimate(flops=half_flops, bytes_accessed=34 << 20, transcendentals=0),
        )(sc, o, t, c)
        return c.reshape(2 * NM * BLOCK, NM * BLOCK)

    spec = P(('batch', 'row'), 'col')
    return jax.shard_map(local_fn, mesh=mesh, in_specs=(spec,), out_specs=spec, check_vma=False)
```

```python
import functools
import jax
import jax.numpy as jnp
from jax import lax
from jax.experimental import pallas as pl
from jax.experimental.pallas import tpu as pltpu
from jax.sharding import PartitionSpec as P

BLOCK = 256
K_DIM = 512
PIECE = 128
PIECES = K_DIM // PIECE
NM = 16
CH = 4
NC = NM // CH
NBUF = 5
LEAD = 4
TILE = CH * BLOCK
JOBS = [(i, j) for j in range(NC) for i in range(j, NC)]
LAST = (NC - 1, NC - 1)
NOW = [job for job in JOBS if job != LAST]
NAX, NAY = 16, 16
NR = 2
O_PARTS = ((12, 4), (0, 4), (4, 4), (8, 3), (11, 1))
NX = NC + len(O_PARTS)
EXTRA = [(3, 0), (3, 1)]
LATER = [job for job in JOBS if job not in EXTRA]
PANELS = [(i, j, 0) for i, j in NOW] + [(i, j, 1) for i, j in EXTRA]


def positions():
    y = lax.axis_index('row')
    col = lax.axis_index('col')
    return y, col // 2, col % 2, col


def chunk(c):
    return pl.ds(c * CH, CH)


def panel(ref, lead, first, count):
    parts = [ref[(*lead, p, pl.ds(first, count))].reshape(count * BLOCK, PIECE) for p in range(PIECES)]
    return jnp.concatenate(parts, axis=1)


def dot_t(rows, cols):
    return lax.dot_general(rows, cols, (((1,), (1,)), ((), ())), preferred_element_type=jnp.float32)


def full_tile(out, row_ref, row_lead, i, col_ref, col_lead, j):
    prod = dot_t(panel(row_ref, row_lead, i * CH, CH), panel(col_ref, col_lead, j * CH, CH))
    out[...] = prod.astype(jnp.bfloat16).reshape(CH, BLOCK, TILE)


def diag_tile(out, row_ref, row_lead, col_ref, col_lead, j, row_blk, col_blk):
    for q in range(CH):
        prod = dot_t(panel(row_ref, row_lead, j * CH + q, CH - q), panel(col_ref, col_lead, j * CH + q, 1))
        row_id = lax.broadcasted_iota(jnp.int32, (BLOCK, BLOCK), 0) + row_blk * BLOCK
        col_id = lax.broadcasted_iota(jnp.int32, (BLOCK, BLOCK), 1) + col_blk * BLOCK
        lanes = slice(q * BLOCK, (q + 1) * BLOCK)
        out[q, :, lanes] = jnp.where(row_id >= col_id, prod[:BLOCK], 0.0).astype(jnp.bfloat16)
        if q + 1 < CH:
            out[q + 1:, :, lanes] = prod[BLOCK:].astype(jnp.bfloat16).reshape(CH - q - 1, BLOCK, BLOCK)


MESH_ID = pl.DeviceIdType.MESH


def remote(src, dst, send, recv, dev):
    return pltpu.make_async_remote_copy(src, dst, send, recv, device_id=dev, device_id_type=MESH_ID)


def signal(sem, devices):
    for dev in devices:
        pl.semaphore_signal(sem, inc=1, device_id=dev, device_id_type=MESH_ID)


def first_kernel(a_ref, sc_ref, token_ref, x_send, x_recv, y_send, y_recv):
    y, x, k, _ = positions()
    token_ref[...] = jnp.zeros_like(token_ref)

    @pl.when(k != y)
    def _():
        x_peer = (0, y, 2 * (1 - x) + k)
        y_peer = (0, 1 - y, 2 * x + y)
        barrier = pltpu.get_barrier_semaphore()
        signal(barrier, (x_peer, y_peer))
        pl.semaphore_wait(barrier, 2)
        px, py = pl.ds(0, NAX), pl.ds(0, NAY)
        xc = remote(a_ref.at[px, 1 - x], sc_ref.at[0, 2, px], x_send, x_recv, x_peer)
        yc = remote(a_ref.at[py, x], sc_ref.at[1, 1, py], y_send, y_recv, y_peer)
        xc.start()
        yc.start()
        xc.wait()
        yc.wait()


def zero_kernel(token_ref, a_ref, sc_in, c_ref, done_ref, sc_ref, o_ref, zbuf, sem, lsem):
    _, x, _, _ = positions()
    loads = [pltpu.make_async_copy(a_ref.at[:, 1 - x], o_ref.at[0], lsem),
             pltpu.make_async_copy(a_ref.at[:, x], sc_ref.at[0, 0], lsem)]
    for cp in loads:
        cp.start()
    zbuf[...] = jnp.zeros_like(zbuf)
    done_ref[...] = jnp.zeros_like(done_ref)
    copies = []
    for s in range(2):
        for i in range(NC):
            for j in range(i + 1, NC):
                copies.append(pltpu.make_async_copy(zbuf, c_ref.at[chunk(i), s, :, pl.ds(j * TILE, TILE)], sem))
            for q in range(1, CH):
                copies.append(pltpu.make_async_copy(
                    zbuf.at[pl.ds(0, q), :, pl.ds(0, BLOCK)],
                    c_ref.at[pl.ds(i * CH, q), s, :, pl.ds((i * CH + q) * BLOCK, BLOCK)], sem))
    for cp in copies:
        cp.start()
    for cp in copies + loads:
        cp.wait()


def gather_kernel(sc_in, o_in, token_ref, sc_ref, o_ref, t_ref, yb, yr, join, d_send, d_recv, x_send, x_recv, r_send, r_recv,
                  y_send, y_recv, b_send, b_recv, q_send, q_recv):
    y, x, k, col = positions()
    late = k != y
    early = k == y
    side = jnp.where(late, 1, 0)
    partner = (0, y, 2 * x + 1 - k)
    x_peer = (0, y, 2 * (1 - x) + k)
    y_early = (0, 1 - y, 2 * x + 1 - y)
    y_late = (0, 1 - y, 2 * x + y)

    def x_copy(n):
        if n < NC:
            part = pl.ds(n * NM // 2, NM // 2)
            return remote(o_ref.at[0, part], sc_ref.at[0, 2, part], x_send.at[n], x_recv.at[n], x_peer)
        part = pl.ds(*O_PARTS[n - NC])
        return remote(sc_ref.at[0, 0, part], o_ref.at[2, part], x_send.at[n], x_recv.at[n], x_peer)

    def relay_copy(n):
        if n < NC:
            return s_relay(n)
        part = pl.ds(*O_PARTS[n - NC])
        return remote(o_ref.at[2, part], o_ref.at[3, part], r_send.at[n], r_recv.at[n], partner)

    def y_copy(s, c):
        return remote(sc_ref.at[0, 2, chunk(c)], sc_ref.at[1, 2 + s, chunk(c)], y_send.at[c], y_recv.at[s, c], y_late)

    def s_relay(c):
        return remote(sc_ref.at[0, 2, chunk(c)], sc_ref.at[0, 3, chunk(c)], r_send.at[c], r_recv.at[c], partner)

    def s_copy(c):
        return remote(sc_ref.at[0, 0, chunk(c)], sc_ref.at[0, 1, chunk(c)], d_send.at[c], d_recv.at[c], partner)

    def yb_relay(c):
        return remote(yb.at[chunk(c)], sc_ref.at[1, 0, chunk(c)], b_send.at[1 + c], b_recv.at[1 + c], partner)

    def yr_relay(c):
        return remote(yr.at[chunk(c)], sc_ref.at[1, 2, chunk(c)], y_send.at[c], y_recv.at[0, c], partner)

    yr_part = pl.ds(0, NR * CH)
    yr_copy = remote(sc_ref.at[0, 2, yr_part], yr, q_send, q_recv, y_early)
    yb_copy = remote(sc_ref.at[0, 0], yb, b_send.at[0], b_recv.at[0], y_early)
    o_copy = remote(o_ref.at[0], o_ref.at[1], d_send.at[NC], d_recv.at[NC], partner)
    barrier = pltpu.get_barrier_semaphore()

    @pl.when(early)
    def _():
        signal(barrier, (x_peer, y_early, partner, y_late))
        pl.semaphore_wait(barrier, 2)
        for n in (0, 1, *range(NC, NX)):
            x_copy(n).start()
        yb_copy.start()
        x_copy(0).wait_recv()
        yr_copy.start()
        pl.semaphore_wait(join, 2)
        for c in range(NC):
            if c == NR:
                x_copy(1).wait_recv()
            s_copy(c).start()
            relay_copy(c).start()
            if c == 0:
                yb_copy.wait_recv()
                yb_relay(c).start()
        for c in range(NC):
            if c == 0:
                yr_copy.wait_recv()
            if c < NR:
                yr_relay(c).start()
            if c + 1 < NC:
                yb_relay(c + 1).start()
        o_copy.start()

    @pl.when(late)
    def _():
        signal(barrier, (x_peer, y_late))
        pl.semaphore_wait(barrier, 4)
        signal(join, (partner, y_early))
        for n in range(NC, NX):
            x_copy(n).start()
        for c in range(NC - 1):
            y_copy(1, c).start()
        for c in range(NC):
            s_copy(c).start()
            if c < NC - 1:
                relay_copy(c).start()
        o_copy.start()
        relay_copy(NC - 1).start()
        y_copy(1, NC - 1).start()

    def rows_ready(i):
        s_copy(i).wait_recv()
        s_relay(i).wait_recv()

    def o_step(n):
        x_copy(NC + n).wait_recv()
        relay_copy(NC + n).start()

    rows_ready(0)
    row_blk = 2 * x + y
    for c in range(NC):
        if c == NC - 1:
            o_step(len(O_PARTS) - 1)

        @pl.when(early)
        def _():
            if c in (0, 2):
                y_copy(0, NR + c // 2).start()

        @pl.when(late)
        def _():
            yb_relay(c).wait_recv()
            for s in range(2):
                y_copy(s, c).wait_recv()

        if c < NC - 1:
            base = NOW.index((c, c))
            diag_tile(t_ref.at[base], sc_ref, (0,), sc_ref, (side,), c, row_blk, col)

            def body(i, _):
                if c == 0:
                    rows_ready(i)
                full_tile(t_ref.at[base + i - c], sc_ref, (0,), i, sc_ref, (side,), c)
                return 0
            lax.fori_loop(c + 1, NC, body, 0)
            o_step(c)
        if c == 1:
            o_copy.wait_recv()
            relay_copy(NC).wait_recv()
            for m, (i, j) in enumerate(EXTRA):
                full_tile(t_ref.at[len(NOW) + m], o_ref, (), i, sc_ref, (side,), j)
        if c == 2:
            o_step(c + 1)

    for n in range(1, len(O_PARTS)):
        relay_copy(NC + n).wait_recv()
    for n in range(NX):
        relay_copy(n).wait_send()
    for n in range(NC, NX):
        x_copy(n).wait_send()
    for c in range(NC):
        s_copy(c).wait_send()
        y_copy(0, c).wait_send()
    o_copy.wait_send()

    @pl.when(early)
    def _():
        for n in range(2):
            x_copy(n).wait_send()
        yr_copy.wait_send()
        yb_copy.wait_send()
        for c in range(NC):
            yb_relay(c).wait_send()


def lookup(n, values):
    out = jnp.int32(values[-1])
    for m in range(len(values) - 2, -1, -1):
        out = jnp.where(n == m, jnp.int32(values[m]), out)
    return out


def write_kernel(sc_ref, o_ref, t_ref, c_in, c_ref, obuf, tsem, osem):
    y, x, k, col = positions()
    side = jnp.where(k != y, 1, 0)

    def pick(n, values):
        return [lookup(n, column) for column in zip(*values)]

    def put(src, i, j, s, sem, act):
        @pl.when(i != j)
        def _():
            act(pltpu.make_async_copy(src, c_ref.at[pl.ds(i * CH, CH), s, :, pl.ds(pl.multiple_of(j * TILE, TILE), TILE)], sem))

        @pl.when(i == j)
        def _():
            for q in range(CH):
                act(pltpu.make_async_copy(
                    src.at[pl.ds(q, CH - q), :, pl.ds(q * BLOCK, BLOCK)],
                    c_ref.at[pl.ds(i * CH + q, CH - q), s, :, pl.ds(pl.multiple_of(j * TILE + q * BLOCK, BLOCK), BLOCK)], sem))

    def put_panel(n, act):
        i, j, cls = pick(n, PANELS)
        put(t_ref.at[n], i, j, jnp.where(cls == 0, x, 1 - x), tsem, act)

    def put_job(n, act):
        i, j = pick(n, LATER)
        b = lax.rem(n, NBUF)
        put(obuf.at[b], i, j, 1 - x, osem.at[b], act)

    def start(cp):
        cp.start()

    def wait(cp):
        cp.wait()

    for n in range(LEAD):
        put_panel(jnp.int32(n), start)

    def body(n, _):
        i, j = pick(n, LATER)
        b = lax.rem(n, NBUF)

        @pl.when(n >= NBUF)
        def _():
            put_job(n - NBUF, wait)

        @pl.when(i != j)
        def _():
            full_tile(obuf.at[b], o_ref, (), i, sc_ref, (side,), j)

        @pl.when(i == j)
        def _():
            diag_tile(obuf.at[b], o_ref, (), sc_ref, (side,), j, 2 * (1 - x) + y, col)
        put_job(n, start)

        @pl.when(n + LEAD < len(PANELS))
        def _():
            put_panel(jnp.minimum(n + LEAD, len(PANELS) - 1), start)
        return 0

    lax.fori_loop(0, len(LATER), body, 0)
    last_slot = len(LATER) % NBUF
    put_job(jnp.int32(len(LATER) - NBUF), wait)
    diag_tile(obuf.at[last_slot], sc_ref, (0,), sc_ref, (side,), LAST[1], 2 * x + y, col)
    put(obuf.at[last_slot], jnp.int32(LAST[0]), jnp.int32(LAST[1]), x, osem.at[last_slot], start)

    def drain(n, _):
        put_panel(n, wait)

        @pl.when(jnp.logical_and(n > len(LATER) - NBUF, n < len(LATER)))
        def _():
            put_job(jnp.minimum(n, len(LATER) - 1), wait)
        return 0
    lax.fori_loop(0, len(PANELS), drain, 0)
    put(obuf.at[last_slot], jnp.int32(LAST[0]), jnp.int32(LAST[1]), x, osem.at[last_slot], wait)


def solution(mesh):
    def local_fn(a):
        a4 = pltpu.with_memory_space_constraint(a.reshape(NM, 2, BLOCK, PIECE), pltpu.HBM)
        any_spec = pl.BlockSpec(memory_space=pl.ANY)
        hbm = pl.BlockSpec(memory_space=pltpu.HBM)
        vmem = pl.BlockSpec(memory_space=pltpu.VMEM)
        dma = pltpu.SemaphoreType.DMA
        half_flops = 136 * 2 * BLOCK * BLOCK * K_DIM
        panels = pltpu.VMEM((2, PIECES, NM, BLOCK, PIECE), jnp.bfloat16)
        token = jax.ShapeDtypeStruct((8, 128), jnp.float32)
        sc, first = pl.pallas_call(
            first_kernel,
            out_shape=[panels, token],
            in_specs=[hbm],
            out_specs=[vmem, vmem],
            scratch_shapes=[dma(())] * 4,
            compiler_params=pltpu.CompilerParams(collective_id=0, has_side_effects=True, vmem_limit_bytes=2 * 1024 * 1024),
        )(a4)
        rest = pltpu.VMEM((PIECES, NM, BLOCK, PIECE), jnp.bfloat16)
        c, zeroed, sc, o = pl.pallas_call(
            zero_kernel,
            out_shape=[jax.ShapeDtypeStruct((NM, 2, BLOCK, NM * BLOCK), jnp.bfloat16), token, panels, rest],
            in_specs=[any_spec, hbm, vmem],
            out_specs=[any_spec, vmem, vmem, vmem],
            input_output_aliases={2: 2},
            scratch_shapes=[pltpu.VMEM((CH, BLOCK, TILE), jnp.bfloat16), dma(()), dma(())],
            compiler_params=pltpu.CompilerParams(vmem_limit_bytes=4 * 1024 * 1024),
            cost_estimate=pl.CostEstimate(flops=half_flops, bytes_accessed=30 << 20, transcendentals=0),
        )(first, a4, sc)
        sc, o, t = pl.pallas_call(
            gather_kernel,
            out_shape=[panels, rest,
                       pltpu.VMEM((len(PANELS), CH, BLOCK, TILE), jnp.bfloat16)],
            in_specs=[vmem, vmem, any_spec],
            out_specs=[vmem] * 3,
            input_output_aliases={0: 0, 1: 1},
            scratch_shapes=[pltpu.VMEM((NM, BLOCK, PIECE), jnp.bfloat16), pltpu.VMEM((NR * CH, BLOCK, PIECE), jnp.bfloat16),
                            pltpu.SemaphoreType.REGULAR,
                            dma((NC + 1,)), dma((NC + 1,)), dma((NX,)), dma((NX,)), dma((NX,)), dma((NX,)),
                            dma((NC,)), dma((2, NC)), dma((NC + 1,)), dma((NC + 1,)), dma(()), dma(())],
            compiler_params=pltpu.CompilerParams(collective_id=1, has_side_effects=True, vmem_limit_bytes=8 * 1024 * 1024),
            cost_estimate=pl.CostEstimate(flops=half_flops, bytes_accessed=2 << 20, transcendentals=0),
        )(sc, o, zeroed)
        c = pl.pallas_call(
            write_kernel,
            out_shape=jax.ShapeDtypeStruct((NM, 2, BLOCK, NM * BLOCK), jnp.bfloat16),
            in_specs=[vmem] * 3 + [any_spec],
            out_specs=any_spec,
            input_output_aliases={3: 0},
            scratch_shapes=[pltpu.VMEM((NBUF, CH, BLOCK, TILE), jnp.bfloat16), dma(()), dma((NBUF,))],
            compiler_params=pltpu.CompilerParams(vmem_limit_bytes=15 * 1024 * 1024),
            cost_estimate=pl.CostEstimate(flops=half_flops, bytes_accessed=34 << 20, transcendentals=0),
        )(sc, o, t, c)
        return c.reshape(2 * NM * BLOCK, NM * BLOCK)

    spec = P(('batch', 'row'), 'col')
    return jax.shard_map(local_fn, mesh=mesh, in_specs=(spec,), out_specs=spec, check_vma=False)
```

```python
import functools
import jax
import jax.numpy as jnp
from jax import lax
from jax.experimental import pallas as pl
from jax.experimental.pallas import tpu as pltpu
from jax.sharding import PartitionSpec as P

BLOCK = 256
K_DIM = 512
PIECE = 128
PIECES = K_DIM // PIECE
NM = 16
CH = 4
NC = NM // CH
NBUF = 5
LEAD = 4
TILE = CH * BLOCK
JOBS = [(i, j) for j in range(NC) for i in range(j, NC)]
LAST = (NC - 1, NC - 1)
NOW = [job for job in JOBS if job != LAST]
NAX, NAY = 14, 14
NR = 2
O_PARTS = ((12, 4), (0, 4), (4, 4), (8, 3), (11, 1))
NX = NC + len(O_PARTS)
EXTRA = [(3, 0), (3, 1)]
LATER = [job for job in JOBS if job not in EXTRA]
PANELS = [(i, j, 0) for i, j in NOW] + [(i, j, 1) for i, j in EXTRA]


def positions():
    y = lax.axis_index('row')
    col = lax.axis_index('col')
    return y, col // 2, col % 2, col


def chunk(c):
    return pl.ds(c * CH, CH)


def panel(ref, lead, first, count):
    parts = [ref[(*lead, p, pl.ds(first, count))].reshape(count * BLOCK, PIECE) for p in range(PIECES)]
    return jnp.concatenate(parts, axis=1)


def dot_t(rows, cols):
    return lax.dot_general(rows, cols, (((1,), (1,)), ((), ())), preferred_element_type=jnp.float32)


def full_tile(out, row_ref, row_lead, i, col_ref, col_lead, j):
    prod = dot_t(panel(row_ref, row_lead, i * CH, CH), panel(col_ref, col_lead, j * CH, CH))
    out[...] = prod.astype(jnp.bfloat16).reshape(CH, BLOCK, TILE)


def diag_tile(out, row_ref, row_lead, col_ref, col_lead, j, row_blk, col_blk):
    for q in range(CH):
        prod = dot_t(panel(row_ref, row_lead, j * CH + q, CH - q), panel(col_ref, col_lead, j * CH + q, 1))
        row_id = lax.broadcasted_iota(jnp.int32, (BLOCK, BLOCK), 0) + row_blk * BLOCK
        col_id = lax.broadcasted_iota(jnp.int32, (BLOCK, BLOCK), 1) + col_blk * BLOCK
        lanes = slice(q * BLOCK, (q + 1) * BLOCK)
        out[q, :, lanes] = jnp.where(row_id >= col_id, prod[:BLOCK], 0.0).astype(jnp.bfloat16)
        if q + 1 < CH:
            out[q + 1:, :, lanes] = prod[BLOCK:].astype(jnp.bfloat16).reshape(CH - q - 1, BLOCK, BLOCK)


MESH_ID = pl.DeviceIdType.MESH


def remote(src, dst, send, recv, dev):
    return pltpu.make_async_remote_copy(src, dst, send, recv, device_id=dev, device_id_type=MESH_ID)


def signal(sem, devices):
    for dev in devices:
        pl.semaphore_signal(sem, inc=1, device_id=dev, device_id_type=MESH_ID)


def first_kernel(a_ref, sc_ref, token_ref, x_send, x_recv, y_send, y_recv):
    y, x, k, _ = positions()
    token_ref[...] = jnp.zeros_like(token_ref)

    @pl.when(k != y)
    def _():
        x_peer = (0, y, 2 * (1 - x) + k)
        y_peer = (0, 1 - y, 2 * x + y)
        barrier = pltpu.get_barrier_semaphore()
        signal(barrier, (x_peer, y_peer))
        pl.semaphore_wait(barrier, 2)
        px, py = pl.ds(0, NAX), pl.ds(0, NAY)
        xc = remote(a_ref.at[px, 1 - x], sc_ref.at[0, 2, px], x_send, x_recv, x_peer)
        yc = remote(a_ref.at[py, x], sc_ref.at[1, 1, py], y_send, y_recv, y_peer)
        xc.start()
        yc.start()
        xc.wait()
        yc.wait()


def zero_kernel(token_ref, a_ref, sc_in, c_ref, done_ref, sc_ref, o_ref, zbuf, sem, lsem):
    _, x, _, _ = positions()
    loads = [pltpu.make_async_copy(a_ref.at[:, 1 - x], o_ref.at[0], lsem),
             pltpu.make_async_copy(a_ref.at[:, x], sc_ref.at[0, 0], lsem)]
    for cp in loads:
        cp.start()
    zbuf[...] = jnp.zeros_like(zbuf)
    done_ref[...] = jnp.zeros_like(done_ref)
    copies = []
    for s in range(2):
        for i in range(NC):
            for j in range(i + 1, NC):
                copies.append(pltpu.make_async_copy(zbuf, c_ref.at[chunk(i), s, :, pl.ds(j * TILE, TILE)], sem))
            for q in range(1, CH):
                copies.append(pltpu.make_async_copy(
                    zbuf.at[pl.ds(0, q), :, pl.ds(0, BLOCK)],
                    c_ref.at[pl.ds(i * CH, q), s, :, pl.ds((i * CH + q) * BLOCK, BLOCK)], sem))
    for cp in copies:
        cp.start()
    for cp in copies + loads:
        cp.wait()


def gather_kernel(sc_in, o_in, token_ref, sc_ref, o_ref, t_ref, yb, yr, join, d_send, d_recv, x_send, x_recv, r_send, r_recv,
                  y_send, y_recv, b_send, b_recv, q_send, q_recv, u_send, u_recv, v_send, v_recv):
    y, x, k, col = positions()
    late = k != y
    early = k == y
    side = jnp.where(late, 1, 0)
    partner = (0, y, 2 * x + 1 - k)
    x_peer = (0, y, 2 * (1 - x) + k)
    y_early = (0, 1 - y, 2 * x + 1 - y)
    y_late = (0, 1 - y, 2 * x + y)
    tx, ty = pl.ds(NAX, NM - NAX), pl.ds(NAY, NM - NAY)

    def x_copy(n):
        if n < NC:
            part = pl.ds(n * NM // 2, NM // 2)
            return remote(o_ref.at[0, part], sc_ref.at[0, 2, part], x_send.at[n], x_recv.at[n], x_peer)
        part = pl.ds(*O_PARTS[n - NC])
        return remote(sc_ref.at[0, 0, part], o_ref.at[2, part], x_send.at[n], x_recv.at[n], x_peer)

    def relay_copy(n):
        if n < NC:
            return s_relay(n)
        part = pl.ds(*O_PARTS[n - NC])
        return remote(o_ref.at[2, part], o_ref.at[3, part], r_send.at[n], r_recv.at[n], partner)

    def y_copy(s, c):
        return remote(sc_ref.at[0, 2, chunk(c)], sc_ref.at[1, 2 + s, chunk(c)], y_send.at[c], y_recv.at[s, c], y_late)

    def s_relay(c):
        return remote(sc_ref.at[0, 2, chunk(c)], sc_ref.at[0, 3, chunk(c)], r_send.at[c], r_recv.at[c], partner)

    def s_copy(c):
        return remote(sc_ref.at[0, 0, chunk(c)], sc_ref.at[0, 1, chunk(c)], d_send.at[c], d_recv.at[c], partner)

    def yb_relay(c):
        return remote(yb.at[chunk(c)], sc_ref.at[1, 0, chunk(c)], b_send.at[1 + c], b_recv.at[1 + c], partner)

    def yr_relay(c):
        return remote(yr.at[chunk(c)], sc_ref.at[1, 2, chunk(c)], y_send.at[c], y_recv.at[0, c], partner)

    yr_part = pl.ds(0, NR * CH)
    yr_copy = remote(sc_ref.at[0, 2, yr_part], yr, q_send, q_recv, y_early)
    yb_copy = remote(sc_ref.at[0, 0], yb, b_send.at[0], b_recv.at[0], y_early)
    x_tail = remote(o_ref.at[0, tx], sc_ref.at[0, 2, tx], v_send, v_recv, x_peer)
    u_copy = remote(sc_ref.at[0, 0, ty], sc_ref.at[1, 1, ty], u_send, u_recv, y_late)
    o_copy = remote(o_ref.at[0], o_ref.at[1], d_send.at[NC], d_recv.at[NC], partner)
    barrier = pltpu.get_barrier_semaphore()

    @pl.when(early)
    def _():
        signal(barrier, (x_peer, y_early, partner, y_late))
        pl.semaphore_wait(barrier, 2)
        for n in (0, 1, *range(NC, NX)):
            x_copy(n).start()
        yb_copy.start()
        x_copy(0).wait_recv()
        yr_copy.start()
        pl.semaphore_wait(join, 2)
        for c in range(NC):
            if c == NR:
                x_copy(1).wait_recv()
            s_copy(c).start()
            relay_copy(c).start()
            if c == 0:
                yb_copy.wait_recv()
                yb_relay(c).start()
        for c in range(NC):
            if c == 0:
                yr_copy.wait_recv()
            if c < NR:
                yr_relay(c).start()
            if c + 1 < NC:
                yb_relay(c + 1).start()
        o_copy.start()

    @pl.when(late)
    def _():
        signal(barrier, (x_peer, y_late))
        pl.semaphore_wait(barrier, 4)
        signal(join, (partner, y_early))
        x_tail.start()
        for n in range(NC, NX):
            x_copy(n).start()
        for c in range(NC - 1):
            y_copy(1, c).start()
        u_copy.start()
        for c in range(NC):
            s_copy(c).start()
            if c < NC - 1:
                relay_copy(c).start()
        o_copy.start()
        x_tail.wait_recv()
        relay_copy(NC - 1).start()
        y_copy(1, NC - 1).start()

    def rows_ready(i):
        s_copy(i).wait_recv()
        s_relay(i).wait_recv()

    def o_step(n):
        x_copy(NC + n).wait_recv()
        relay_copy(NC + n).start()

    rows_ready(0)
    row_blk = 2 * x + y
    for c in range(NC):
        if c == NC - 1:
            o_step(len(O_PARTS) - 1)

        @pl.when(early)
        def _():
            if c in (0, 2):
                y_copy(0, NR + c // 2).start()

        @pl.when(late)
        def _():
            yb_relay(c).wait_recv()
            if c == NC - 1:
                u_copy.wait_recv()
            for s in range(2):
                y_copy(s, c).wait_recv()

        if c < NC - 1:
            base = NOW.index((c, c))
            diag_tile(t_ref.at[base], sc_ref, (0,), sc_ref, (side,), c, row_blk, col)

            def body(i, _):
                if c == 0:
                    rows_ready(i)
                full_tile(t_ref.at[base + i - c], sc_ref, (0,), i, sc_ref, (side,), c)
                return 0
            lax.fori_loop(c + 1, NC, body, 0)
            o_step(c)
        if c == 1:
            o_copy.wait_recv()
            relay_copy(NC).wait_recv()
            for m, (i, j) in enumerate(EXTRA):
                full_tile(t_ref.at[len(NOW) + m], o_ref, (), i, sc_ref, (side,), j)
        if c == 2:
            o_step(c + 1)

    for n in range(1, len(O_PARTS)):
        relay_copy(NC + n).wait_recv()
    for n in range(NX):
        relay_copy(n).wait_send()
    for n in range(NC, NX):
        x_copy(n).wait_send()
    for c in range(NC):
        s_copy(c).wait_send()
        y_copy(0, c).wait_send()
    o_copy.wait_send()

    @pl.when(late)
    def _():
        u_copy.wait_send()
        x_tail.wait_send()

    @pl.when(early)
    def _():
        for n in range(2):
            x_copy(n).wait_send()
        yr_copy.wait_send()
        yb_copy.wait_send()
        for c in range(NC):
            yb_relay(c).wait_send()


def lookup(n, values):
    out = jnp.int32(values[-1])
    for m in range(len(values) - 2, -1, -1):
        out = jnp.where(n == m, jnp.int32(values[m]), out)
    return out


def write_kernel(sc_ref, o_ref, t_ref, c_in, c_ref, obuf, tsem, osem):
    y, x, k, col = positions()
    side = jnp.where(k != y, 1, 0)

    def pick(n, values):
        return [lookup(n, column) for column in zip(*values)]

    def put(src, i, j, s, sem, act):
        @pl.when(i != j)
        def _():
            act(pltpu.make_async_copy(src, c_ref.at[pl.ds(i * CH, CH), s, :, pl.ds(pl.multiple_of(j * TILE, TILE), TILE)], sem))

        @pl.when(i == j)
        def _():
            for q in range(CH):
                act(pltpu.make_async_copy(
                    src.at[pl.ds(q, CH - q), :, pl.ds(q * BLOCK, BLOCK)],
                    c_ref.at[pl.ds(i * CH + q, CH - q), s, :, pl.ds(pl.multiple_of(j * TILE + q * BLOCK, BLOCK), BLOCK)], sem))

    def put_panel(n, act):
        i, j, cls = pick(n, PANELS)
        put(t_ref.at[n], i, j, jnp.where(cls == 0, x, 1 - x), tsem, act)

    def put_job(n, act):
        i, j = pick(n, LATER)
        b = lax.rem(n, NBUF)
        put(obuf.at[b], i, j, 1 - x, osem.at[b], act)

    def start(cp):
        cp.start()

    def wait(cp):
        cp.wait()

    for n in range(LEAD):
        put_panel(jnp.int32(n), start)

    def body(n, _):
        i, j = pick(n, LATER)
        b = lax.rem(n, NBUF)

        @pl.when(n >= NBUF)
        def _():
            put_job(n - NBUF, wait)

        @pl.when(i != j)
        def _():
            full_tile(obuf.at[b], o_ref, (), i, sc_ref, (side,), j)

        @pl.when(i == j)
        def _():
            diag_tile(obuf.at[b], o_ref, (), sc_ref, (side,), j, 2 * (1 - x) + y, col)
        put_job(n, start)

        @pl.when(n + LEAD < len(PANELS))
        def _():
            put_panel(jnp.minimum(n + LEAD, len(PANELS) - 1), start)
        return 0

    lax.fori_loop(0, len(LATER), body, 0)
    last_slot = len(LATER) % NBUF
    put_job(jnp.int32(len(LATER) - NBUF), wait)
    diag_tile(obuf.at[last_slot], sc_ref, (0,), sc_ref, (side,), LAST[1], 2 * x + y, col)
    put(obuf.at[last_slot], jnp.int32(LAST[0]), jnp.int32(LAST[1]), x, osem.at[last_slot], start)

    def drain(n, _):
        put_panel(n, wait)

        @pl.when(jnp.logical_and(n > len(LATER) - NBUF, n < len(LATER)))
        def _():
            put_job(jnp.minimum(n, len(LATER) - 1), wait)
        return 0
    lax.fori_loop(0, len(PANELS), drain, 0)
    put(obuf.at[last_slot], jnp.int32(LAST[0]), jnp.int32(LAST[1]), x, osem.at[last_slot], wait)


def solution(mesh):
    def local_fn(a):
        a4 = pltpu.with_memory_space_constraint(a.reshape(NM, 2, BLOCK, PIECE), pltpu.HBM)
        any_spec = pl.BlockSpec(memory_space=pl.ANY)
        hbm = pl.BlockSpec(memory_space=pltpu.HBM)
        vmem = pl.BlockSpec(memory_space=pltpu.VMEM)
        dma = pltpu.SemaphoreType.DMA
        half_flops = 136 * 2 * BLOCK * BLOCK * K_DIM
        panels = pltpu.VMEM((2, PIECES, NM, BLOCK, PIECE), jnp.bfloat16)
        token = jax.ShapeDtypeStruct((8, 128), jnp.float32)
        sc, first = pl.pallas_call(
            first_kernel,
            out_shape=[panels, token],
            in_specs=[hbm],
            out_specs=[vmem, vmem],
            scratch_shapes=[dma(())] * 4,
            compiler_params=pltpu.CompilerParams(collective_id=0, has_side_effects=True, vmem_limit_bytes=2 * 1024 * 1024),
        )(a4)
        rest = pltpu.VMEM((PIECES, NM, BLOCK, PIECE), jnp.bfloat16)
        c, zeroed, sc, o = pl.pallas_call(
            zero_kernel,
            out_shape=[jax.ShapeDtypeStruct((NM, 2, BLOCK, NM * BLOCK), jnp.bfloat16), token, panels, rest],
            in_specs=[any_spec, hbm, vmem],
            out_specs=[any_spec, vmem, vmem, vmem],
            input_output_aliases={2: 2},
            scratch_shapes=[pltpu.VMEM((CH, BLOCK, TILE), jnp.bfloat16), dma(()), dma(())],
            compiler_params=pltpu.CompilerParams(vmem_limit_bytes=4 * 1024 * 1024),
            cost_estimate=pl.CostEstimate(flops=half_flops, bytes_accessed=30 << 20, transcendentals=0),
        )(first, a4, sc)
        sc, o, t = pl.pallas_call(
            gather_kernel,
            out_shape=[panels, rest,
                       pltpu.VMEM((len(PANELS), CH, BLOCK, TILE), jnp.bfloat16)],
            in_specs=[vmem, vmem, any_spec],
            out_specs=[vmem] * 3,
            input_output_aliases={0: 0, 1: 1},
            scratch_shapes=[pltpu.VMEM((NM, BLOCK, PIECE), jnp.bfloat16), pltpu.VMEM((NR * CH, BLOCK, PIECE), jnp.bfloat16),
                            pltpu.SemaphoreType.REGULAR,
                            dma((NC + 1,)), dma((NC + 1,)), dma((NX,)), dma((NX,)), dma((NX,)), dma((NX,)),
                            dma((NC,)), dma((2, NC)), dma((NC + 1,)), dma((NC + 1,)), dma(()), dma(())] + [dma(())] * 4,
            compiler_params=pltpu.CompilerParams(collective_id=1, has_side_effects=True, vmem_limit_bytes=8 * 1024 * 1024),
            cost_estimate=pl.CostEstimate(flops=half_flops, bytes_accessed=2 << 20, transcendentals=0),
        )(sc, o, zeroed)
        c = pl.pallas_call(
            write_kernel,
            out_shape=jax.ShapeDtypeStruct((NM, 2, BLOCK, NM * BLOCK), jnp.bfloat16),
            in_specs=[vmem] * 3 + [any_spec],
            out_specs=any_spec,
            input_output_aliases={3: 0},
            scratch_shapes=[pltpu.VMEM((NBUF, CH, BLOCK, TILE), jnp.bfloat16), dma(()), dma((NBUF,))],
            compiler_params=pltpu.CompilerParams(vmem_limit_bytes=15 * 1024 * 1024),
            cost_estimate=pl.CostEstimate(flops=half_flops, bytes_accessed=34 << 20, transcendentals=0),
        )(sc, o, t, c)
        return c.reshape(2 * NM * BLOCK, NM * BLOCK)

    spec = P(('batch', 'row'), 'col')
    return jax.shard_map(local_fn, mesh=mesh, in_specs=(spec,), out_specs=spec, check_vma=False)
```
